32 devices in a mesh: dp: 4 (over z), expert: 8 (over y, x, core).
Axes of the slice: x: 2, y: 2, z: 4, core: 2. Of those that a mesh axis runs over, the one named last changes fastest.
Arguments:
- hidden: bfloat16 [4, 1024, 2048], P('dp', 'expert'), may hold values from -6 to 6
- output_cotangent: bfloat16 [4, 1024, 2048], P('dp', 'expert'), may hold values from -6 to 6
- attention_gain: float32 [2048], replicated, may hold values from 0.5 to 1.5
- expert_norm_gain: float32 [2048], replicated, may hold values from 0.5 to 1.5
- query_key_value_weight: bfloat16 [3, 2048, 2048], P(None, None, 'expert'), may hold values from -0.125 to 0.125
- output_weight: bfloat16 [2048, 2048], P('expert'), may hold values from -0.5 to 0.5
- gate_up_weight: bfloat16 [16, 2, 2048, 1024], P('expert'), may hold values from -0.125 to 0.125
- down_weight: bfloat16 [16, 1024, 2048], P('expert'), may hold values from -0.1875 to 0.1875
- token_experts: int32 [4, 1024, 8], P('dp', 'expert'), may hold values from 0 to 15, all different within a row; in each aligned block of 128 rows (0 to 127, 128 to 255, ..., all dimensions but the last counted through in order) at most 80 rows name the same one
- expert_gate_weight: float32 [4, 1024, 8], P('dp', 'expert'), may hold values from 0.05 to 0.25
- sequence_adapter: int32 [4], replicated, may hold values from 0 to 7
- optimizer_steps: int32 [1], replicated, may hold values from 1 to 20
- adapter_attention_input: bfloat16 [3, 8, 16, 2048], replicated, may hold values from -0.125 to 0.125
- adapter_attention_output: bfloat16 [3, 8, 16, 2048], P(None, None, None, 'expert'), may hold values from -0.375 to 0.375
- adapter_projection_input: bfloat16 [8, 16, 2048], P(None, None, 'expert'), may hold values from -0.5 to 0.5
- adapter_projection_output: bfloat16 [8, 16, 2048], replicated, may hold values from -0.375 to 0.375
- adapter_hidden_input: bfloat16 [16, 2, 8, 16, 2048], P('expert'), may hold values from -0.125 to 0.125
- adapter_hidden_output: bfloat16 [16, 2, 8, 16, 1024], P('expert'), may hold values from -0.375 to 0.375
- adapter_down_input: bfloat16 [16, 8, 16, 1024], P('expert'), may hold values from -0.1875 to 0.1875
- adapter_down_output: bfloat16 [16, 8, 16, 2048], P('expert'), may hold values from -0.375 to 0.375
- moment_attention_input: float32 [3, 8, 16, 2048], P(None, None, None, ('dp', 'expert')), may hold values from -0.036 to 0.036
- moment_attention_output: float32 [3, 8, 16, 2048], P(None, None, None, ('expert', 'dp')), may hold values from -0.036 to 0.036
- moment_projection_input: float32 [8, 16, 2048], P(None, None, ('expert', 'dp')), may hold values from -0.036 to 0.036
- moment_projection_output: float32 [8, 16, 2048], P(None, None, ('dp', 'expert')), may hold values from -0.036 to 0.036
- moment_hidden_input: float32 [16, 2, 8, 16, 2048], P('expert', None, None, None, 'dp'), may hold values from -0.036 to 0.036
- moment_hidden_output: float32 [16, 2, 8, 16, 1024], P('expert', None, None, None, 'dp'), may hold values from -0.036 to 0.036
- moment_down_input: float32 [16, 8, 16, 1024], P('expert', None, None, 'dp'), may hold values from -0.036 to 0.036
- moment_down_output: float32 [16, 8, 16, 2048], P('expert', None, None, 'dp'), may hold values from -0.036 to 0.036
- squared_attention_input: float32 [3, 8, 16, 2048], P(None, None, None, ('dp', 'expert')), may hold values from 2e-05 to 0.001
- squared_attention_output: float32 [3, 8, 16, 2048], P(None, None, None, ('expert', 'dp')), may hold values from 2e-05 to 0.001
- squared_projection_input: float32 [8, 16, 2048], P(None, None, ('expert', 'dp')), may hold values from 2e-05 to 0.001
- squared_projection_output: float32 [8, 16, 2048], P(None, None, ('dp', 'expert')), may hold values from 2e-05 to 0.001
- squared_hidden_input: float32 [16, 2, 8, 16, 2048], P('expert', None, None, None, 'dp'), may hold values from 2e-05 to 0.001
- squared_hidden_output: float32 [16, 2, 8, 16, 1024], P('expert', None, None, None, 'dp'), may hold values from 2e-05 to 0.001
- squared_down_input: float32 [16, 8, 16, 1024], P('expert', None, None, 'dp'), may hold values from 2e-05 to 0.001
- squared_down_output: float32 [16, 8, 16, 2048], P('expert', None, None, 'dp'), may hold values from 2e-05 to 0.001
Outputs:
- block_out: bfloat16 [4, 1024, 2048], P('dp', 'expert')
- grad_hidden: float32 [4, 1024, 2048], P('dp', 'expert')
- global_norm: float32 [1], replicated
- grad_qkv_a: float32 [3, 8, 16, 2048], P(None, None, None, ('dp', 'expert'))
- new_first_qkv_a: float32 [3, 8, 16, 2048], P(None, None, None, ('dp', 'expert'))
- new_second_qkv_a: float32 [3, 8, 16, 2048], P(None, None, None, ('dp', 'expert'))
- update_qkv_a: float32 [3, 8, 16, 2048], P(None, None, None, ('dp', 'expert'))
- grad_qkv_b: float32 [3, 8, 16, 2048], P(None, None, None, ('expert', 'dp'))
- new_first_qkv_b: float32 [3, 8, 16, 2048], P(None, None, None, ('expert', 'dp'))
- new_second_qkv_b: float32 [3, 8, 16, 2048], P(None, None, None, ('expert', 'dp'))
- update_qkv_b: float32 [3, 8, 16, 2048], P(None, None, None, ('expert', 'dp'))
- grad_out_a: float32 [8, 16, 2048], P(None, None, ('expert', 'dp'))
- new_first_out_a: float32 [8, 16, 2048], P(None, None, ('expert', 'dp'))
- new_second_out_a: float32 [8, 16, 2048], P(None, None, ('expert', 'dp'))
- update_out_a: float32 [8, 16, 2048], P(None, None, ('expert', 'dp'))
- grad_out_b: float32 [8, 16, 2048], P(None, None, ('dp', 'expert'))
- new_first_out_b: float32 [8, 16, 2048], P(None, None, ('dp', 'expert'))
- new_second_out_b: float32 [8, 16, 2048], P(None, None, ('dp', 'expert'))
- update_out_b: float32 [8, 16, 2048], P(None, None, ('dp', 'expert'))
- grad_in_a: float32 [16, 2, 8, 16, 2048], P('expert', None, None, None, 'dp')
- new_first_in_a: float32 [16, 2, 8, 16, 2048], P('expert', None, None, None, 'dp')
- new_second_in_a: float32 [16, 2, 8, 16, 2048], P('expert', None, None, None, 'dp')
- update_in_a: float32 [16, 2, 8, 16, 2048], P('expert', None, None, None, 'dp')
- grad_mid_b: float32 [16, 2, 8, 16, 1024], P('expert', None, None, None, 'dp')
- new_first_mid_b: float32 [16, 2, 8, 16, 1024], P('expert', None, None, None, 'dp')
- new_second_mid_b: float32 [16, 2, 8, 16, 1024], P('expert', None, None, None, 'dp')
- update_mid_b: float32 [16, 2, 8, 16, 1024], P('expert', None, None, None, 'dp')
- grad_down_a: float32 [16, 8, 16, 1024], P('expert', None, None, 'dp')
- new_first_down_a: float32 [16, 8, 16, 1024], P('expert', None, None, 'dp')
- new_second_down_a: float32 [16, 8, 16, 1024], P('expert', None, None, 'dp')
- update_down_a: float32 [16, 8, 16, 1024], P('expert', None, None, 'dp')
- grad_down_b: float32 [16, 8, 16, 2048], P('expert', None, None, 'dp')
- new_first_down_b: float32 [16, 8, 16, 2048], P('expert', None, None, 'dp')
- new_second_down_b: float32 [16, 8, 16, 2048], P('expert', None, None, 'dp')
- update_down_b: float32 [16, 8, 16, 2048], P('expert', None, None, 'dp')
The draws below stay inside these ranges and needn't reach their ends.
Inputs may be any that keep to these rules, and one draw needn't show every extreme that they name: `token_experts`: in each aligned block of 128 positions (the rows of one device) no expert is named by more than 80 assignments; this bound is reached in some block.
All inputs are finite; a program needn't handle non-finite values.
Results may differ from the reference program's by a relative error of at most 0.02.
Values may be sent and summed in bfloat16 or wider, within the bound.
A program may use at most 256 MiB of HBM per device.

```python
import math
import jax
import jax.numpy as jnp
import numpy as np
from jax import lax

MODEL_WIDTH = 2048
H = 16
HEAD = 128
EXPERT_HIDDEN = 1024
TOP = 8
ADAPTER_RANK = 16
ADAPTER_COUNT = 8
LENGTH = 1024
SEQS = 4
EXPERT_COUNT = 16
TOK_DEV = 128
CAP = 80
BLK = 512
CLIP = 256
N_EXPERT = 8


def with_ends(entries, key, least, largest):
    index_at = [jax.random.randint(jax.random.fold_in(key, axis), (), 0, length) for axis, length in enumerate(entries.shape)]
    widest = entries.shape.index(max(entries.shape))
    beside = index_at[:widest] + [(index_at[widest] + 1) % entries.shape[widest]] + index_at[widest + 1:]
    return entries.at[tuple(index_at)].set(least).at[tuple(beside)].set(largest)


def shard_levels(own_key, extent, cuts, smallest, largest):
    def one(axis_at, shards_of):
        steps = jax.random.uniform(jax.random.fold_in(jax.random.fold_in(own_key, 6), axis_at), (shards_of,), jnp.float32, smallest / len(cuts), largest / len(cuts))
        return jnp.repeat(jnp.exp(steps), extent[axis_at] // shards_of).reshape((-1,) + (1,) * (len(extent) - axis_at - 1))

    factor_of = one(*cuts[0])
    for cut in cuts[1:]:
        factor_of = factor_of * one(*cut)
    return factor_of


def assign_block(own_key, own, number, rows, amount, top, reach, skew):
    sequence = jax.random.permutation(own_key, amount)
    packed, usual = shares(amount, rows * top, reach, skew, True), shares(amount, rows * top, reach, skew, False)
    places = jnp.arange(amount)

    def named(sizes, turn):
        used = int((sizes > 0).sum())
        fixed = max(1, used // 4)
        passed = fixed + (places - fixed + turn * (used - fixed)) % max(1, amount - fixed)
        return jnp.zeros((amount,), jnp.int32).at[sequence[jnp.where(places < fixed, places, passed)]].set(jnp.asarray(sizes, jnp.int32))

    sizes = jnp.where(number % 4 == 0, named(packed, number // 4), named(usual, number - number // 4 - 1))
    mixed = jax.random.permutation(jax.random.fold_in(own, 3), amount)
    giver, receiver = mixed[0:amount // 2 * 2:2], mixed[1:amount // 2 * 2:2]
    room = jnp.minimum(sizes[giver] - 1, reach - sizes[receiver]) // 2
    room = jnp.where((giver == sequence[0]) | (receiver == sequence[0]) | (sizes[receiver] == 0), 0, jnp.maximum(room, 0))
    passed = jax.random.randint(jax.random.fold_in(own, 4), (amount // 2,), 0, 1 << 20) % (room + 1)
    sizes = sizes.at[giver].add(-passed).at[receiver].add(passed)
    members = jnp.searchsorted(jnp.cumsum(sizes), jnp.arange(rows * top), side="right").astype(jnp.int32)
    grid = members.reshape(top, rows).T
    grid = grid[jax.random.permutation(jax.random.fold_in(own, 1), rows)]
    turn = jax.random.randint(jax.random.fold_in(own, 2), (rows, 1), 0, top)
    return jnp.take_along_axis(grid, (jnp.arange(top)[None, :] + turn) % top, axis=1)


def shares(amount, total, limit, lean, full):
    portions = [(1 << 20) // math.isqrt(grade ** lean) + 1 for grade in range(1, amount + 1)]
    largest = limit if full else min(limit, max(-(-total // amount), total * portions[0] // sum(portions)))
    least = 1 if total - largest >= amount - 1 else 0
    counts, spare = [largest] + [least] * (amount - 1), total - largest - least * (amount - 1)
    while spare > 0:
        candidates = [i for i in range(1, amount) if counts[i] < largest] or [i for i in range(1, amount) if counts[i] < limit]
        pool, budget = sum([portions[i] for i in candidates]), spare
        for i in candidates:
            more = min(limit - counts[i], max(1, budget * portions[i] // pool), spare)
            counts[i] = counts[i] + more
            spare = spare - more
    return np.array(counts)


def gaussian(key, dims, spread, bound, pieces=(), kind=jnp.bfloat16):
    drawn = jax.random.normal(key, dims, jnp.float32) * spread
    if len(pieces) > 0:
        drawn = shard_levels(key, dims, pieces, -0.22, 0.18) * drawn
    return jnp.clip(drawn, min=-bound, max=bound).astype(kind)


def setup_inputs(seed: int = 0) -> dict:
    key_of = jax.random.split(jax.random.key(seed), 37)
    hidden = gaussian(key_of[0], (SEQS, LENGTH, MODEL_WIDTH), 1.0, 6.0, ((0, 4), (1, 8)))
    output_cotangent = gaussian(key_of[1], (SEQS, LENGTH, MODEL_WIDTH), 1.0, 6.0, ((0, 4), (1, 8)))
    attention_gain = jnp.clip(1.0 + 0.1 * jax.random.normal(key_of[2], (MODEL_WIDTH,), jnp.float32), 0.5, 1.5)
    expert_norm_gain = jnp.clip(1.0 + 0.1 * jax.random.normal(key_of[3], (MODEL_WIDTH,), jnp.float32), 0.5, 1.5)
    query_key_value_weight = gaussian(key_of[4], (3, MODEL_WIDTH, MODEL_WIDTH), MODEL_WIDTH ** -0.5, 0.125, ((2, 8),))
    output_weight = gaussian(key_of[5], (MODEL_WIDTH, MODEL_WIDTH), (MODEL_WIDTH // 16) ** -0.5, 0.5, ((0, 8),))
    gate_up_weight = gaussian(key_of[6], (EXPERT_COUNT, 2, MODEL_WIDTH, EXPERT_HIDDEN), MODEL_WIDTH ** -0.5, 0.125, ((0, 8),))
    down_weight = gaussian(key_of[7], (EXPERT_COUNT, EXPERT_HIDDEN, MODEL_WIDTH), EXPERT_HIDDEN ** -0.5, 0.1875, ((0, 8),))
    token_experts_keys = jax.random.split(jax.random.fold_in(key_of[8], 1), SEQS * LENGTH // TOK_DEV)
    token_experts_turns = jax.random.permutation(jax.random.fold_in(key_of[8], 3), SEQS * LENGTH // TOK_DEV)
    token_experts = jax.vmap(lambda own, number: assign_block(jax.random.fold_in(key_of[8], 2), own, number, TOK_DEV, EXPERT_COUNT, TOP, CAP, 0))(token_experts_keys, token_experts_turns).reshape((SEQS, LENGTH, TOP))
    expert_gate_weight = jnp.clip(0.05 + 0.2 * jax.random.uniform(key_of[9], (SEQS, LENGTH, TOP), jnp.float32) ** shard_levels(key_of[9], (SEQS, LENGTH, TOP), ((0, 4), (1, 8)), -0.2, 0.2), 0.05, 0.25)
    sequence_adapter = with_ends(jax.random.randint(key_of[10], (SEQS,), 0, ADAPTER_COUNT), jax.random.fold_in(key_of[10], 1), 0, ADAPTER_COUNT - 1).astype(jnp.int32)
    optimizer_steps = jax.random.randint(key_of[11], (1,), 1, 21).astype(jnp.int32)
    adapter_attention_input = gaussian(key_of[12], (3, ADAPTER_COUNT, ADAPTER_RANK, MODEL_WIDTH), MODEL_WIDTH ** -0.5, 0.125)
    adapter_attention_output = gaussian(key_of[13], (3, ADAPTER_COUNT, ADAPTER_RANK, MODEL_WIDTH), (16 * ADAPTER_RANK) ** -0.5, 0.375, ((3, 8),))
    adapter_projection_input = gaussian(key_of[14], (ADAPTER_COUNT, ADAPTER_RANK, MODEL_WIDTH), (MODEL_WIDTH // 16) ** -0.5, 0.5, ((2, 8),))
    adapter_projection_output = gaussian(key_of[15], (ADAPTER_COUNT, ADAPTER_RANK, MODEL_WIDTH), (16 * ADAPTER_RANK) ** -0.5, 0.375)
    adapter_hidden_input = gaussian(key_of[16], (EXPERT_COUNT, 2, ADAPTER_COUNT, ADAPTER_RANK, MODEL_WIDTH), MODEL_WIDTH ** -0.5, 0.125, ((0, 8),))
    adapter_hidden_output = gaussian(key_of[17], (EXPERT_COUNT, 2, ADAPTER_COUNT, ADAPTER_RANK, EXPERT_HIDDEN), (16 * ADAPTER_RANK) ** -0.5, 0.375, ((0, 8),))
    adapter_down_input = gaussian(key_of[18], (EXPERT_COUNT, ADAPTER_COUNT, ADAPTER_RANK, EXPERT_HIDDEN), EXPERT_HIDDEN ** -0.5, 0.1875, ((0, 8),))
    adapter_down_output = gaussian(key_of[19], (EXPERT_COUNT, ADAPTER_COUNT, ADAPTER_RANK, MODEL_WIDTH), (16 * ADAPTER_RANK) ** -0.5, 0.375, ((0, 8),))
    moment_attention_input = gaussian(key_of[20], (3, ADAPTER_COUNT, ADAPTER_RANK, MODEL_WIDTH), 0.006, 0.036, ((3, 32),), jnp.float32)
    moment_attention_output = gaussian(key_of[21], (3, ADAPTER_COUNT, ADAPTER_RANK, MODEL_WIDTH), 0.006, 0.036, ((3, 32),), jnp.float32)
    moment_projection_input = gaussian(key_of[22], (ADAPTER_COUNT, ADAPTER_RANK, MODEL_WIDTH), 0.006, 0.036, ((2, 32),), jnp.float32)
    moment_projection_output = gaussian(key_of[23], (ADAPTER_COUNT, ADAPTER_RANK, MODEL_WIDTH), 0.006, 0.036, ((2, 32),), jnp.float32)
    moment_hidden_input = gaussian(key_of[24], (EXPERT_COUNT, 2, ADAPTER_COUNT, ADAPTER_RANK, MODEL_WIDTH), 0.006, 0.036, ((0, 8), (4, 4)), jnp.float32)
    moment_hidden_output = gaussian(key_of[25], (EXPERT_COUNT, 2, ADAPTER_COUNT, ADAPTER_RANK, EXPERT_HIDDEN), 0.006, 0.036, ((0, 8), (4, 4)), jnp.float32)
    moment_down_input = gaussian(key_of[26], (EXPERT_COUNT, ADAPTER_COUNT, ADAPTER_RANK, EXPERT_HIDDEN), 0.006, 0.036, ((0, 8), (3, 4)), jnp.float32)
    moment_down_output = gaussian(key_of[27], (EXPERT_COUNT, ADAPTER_COUNT, ADAPTER_RANK, MODEL_WIDTH), 0.006, 0.036, ((0, 8), (3, 4)), jnp.float32)
    squared_attention_input = jnp.clip(jnp.exp(math.log(0.001) - 3.912023 * jax.random.uniform(key_of[28], (3, ADAPTER_COUNT, ADAPTER_RANK, MODEL_WIDTH), jnp.float32) ** shard_levels(key_of[28], (3, ADAPTER_COUNT, ADAPTER_RANK, MODEL_WIDTH), ((3, 32),), -0.2, 0.2)), 1.9999999494757503e-05, 0.001)
    squared_attention_output = jnp.clip(jnp.exp(math.log(0.001) - 3.912023 * jax.random.uniform(key_of[29], (3, ADAPTER_COUNT, ADAPTER_RANK, MODEL_WIDTH), jnp.float32) ** shard_levels(key_of[29], (3, ADAPTER_COUNT, ADAPTER_RANK, MODEL_WIDTH), ((3, 32),), -0.2, 0.2)), 1.9999999494757503e-05, 0.001)
    squared_projection_input = jnp.clip(jnp.exp(math.log(0.001) - 3.912023 * jax.random.uniform(key_of[30], (ADAPTER_COUNT, ADAPTER_RANK, MODEL_WIDTH), jnp.float32) ** shard_levels(key_of[30], (ADAPTER_COUNT, ADAPTER_RANK, MODEL_WIDTH), ((2, 32),), -0.2, 0.2)), 1.9999999494757503e-05, 0.001)
    squared_projection_output = jnp.clip(jnp.exp(math.log(0.001) - 3.912023 * jax.random.uniform(key_of[31], (ADAPTER_COUNT, ADAPTER_RANK, MODEL_WIDTH), jnp.float32) ** shard_levels(key_of[31], (ADAPTER_COUNT, ADAPTER_RANK, MODEL_WIDTH), ((2, 32),), -0.2, 0.2)), 1.9999999494757503e-05, 0.001)
    squared_hidden_input = jnp.clip(jnp.exp(math.log(0.001) - 3.912023 * jax.random.uniform(key_of[32], (EXPERT_COUNT, 2, ADAPTER_COUNT, ADAPTER_RANK, MODEL_WIDTH), jnp.float32) ** shard_levels(key_of[32], (EXPERT_COUNT, 2, ADAPTER_COUNT, ADAPTER_RANK, MODEL_WIDTH), ((0, 8), (4, 4)), -0.2, 0.2)), 1.9999999494757503e-05, 0.001)
    squared_hidden_output = jnp.clip(jnp.exp(math.log(0.001) - 3.912023 * jax.random.uniform(key_of[33], (EXPERT_COUNT, 2, ADAPTER_COUNT, ADAPTER_RANK, EXPERT_HIDDEN), jnp.float32) ** shard_levels(key_of[33], (EXPERT_COUNT, 2, ADAPTER_COUNT, ADAPTER_RANK, EXPERT_HIDDEN), ((0, 8), (4, 4)), -0.2, 0.2)), 1.9999999494757503e-05, 0.001)
    squared_down_input = jnp.clip(jnp.exp(math.log(0.001) - 3.912023 * jax.random.uniform(key_of[34], (EXPERT_COUNT, ADAPTER_COUNT, ADAPTER_RANK, EXPERT_HIDDEN), jnp.float32) ** shard_levels(key_of[34], (EXPERT_COUNT, ADAPTER_COUNT, ADAPTER_RANK, EXPERT_HIDDEN), ((0, 8), (3, 4)), -0.2, 0.2)), 1.9999999494757503e-05, 0.001)
    squared_down_output = jnp.clip(jnp.exp(math.log(0.001) - 3.912023 * jax.random.uniform(key_of[35], (EXPERT_COUNT, ADAPTER_COUNT, ADAPTER_RANK, MODEL_WIDTH), jnp.float32) ** shard_levels(key_of[35], (EXPERT_COUNT, ADAPTER_COUNT, ADAPTER_RANK, MODEL_WIDTH), ((0, 8), (3, 4)), -0.2, 0.2)), 1.9999999494757503e-05, 0.001)
    return dict(hidden=hidden, output_cotangent=output_cotangent, attention_gain=attention_gain, expert_norm_gain=expert_norm_gain, query_key_value_weight=query_key_value_weight, output_weight=output_weight, gate_up_weight=gate_up_weight, down_weight=down_weight, token_experts=token_experts, expert_gate_weight=expert_gate_weight, sequence_adapter=sequence_adapter, optimizer_steps=optimizer_steps, adapter_attention_input=adapter_attention_input, adapter_attention_output=adapter_attention_output, adapter_projection_input=adapter_projection_input, adapter_projection_output=adapter_projection_output, adapter_hidden_input=adapter_hidden_input, adapter_hidden_output=adapter_hidden_output, adapter_down_input=adapter_down_input, adapter_down_output=adapter_down_output, moment_attention_input=moment_attention_input, moment_attention_output=moment_attention_output, moment_projection_input=moment_projection_input, moment_projection_output=moment_projection_output, moment_hidden_input=moment_hidden_input, moment_hidden_output=moment_hidden_output, moment_down_input=moment_down_input, moment_down_output=moment_down_output, squared_attention_input=squared_attention_input, squared_attention_output=squared_attention_output, squared_projection_input=squared_projection_input, squared_projection_output=squared_projection_output, squared_hidden_input=squared_hidden_input, squared_hidden_output=squared_hidden_output, squared_down_input=squared_down_input, squared_down_output=squared_down_output)


@jax.custom_vjp
def low(v):
    return lax.optimization_barrier(v.astype(jnp.bfloat16)).astype(jnp.float32)

@jax.custom_vjp
def low_back(v):
    return v

def low_keep(v):
    return (low(v), None)

def low_pass(kept, grad):
    return (grad,)

def back_keep(v):
    return (v, None)

def back_low(kept, grad):
    return (low(grad),)
low.defvjp(low_keep, low_pass)
low_back.defvjp(back_keep, back_low)
norm_eps = 1e-05
beta_one = 0.9
beta_two = 0.95
learn_rate = 0.02
weight_decay = 0.1
adam_eps = 1e-08
highest = lax.Precision.HIGHEST

def both_low(value):
    return low_back(low(value))

def rms_scale(values, gain):
    return values * lax.rsqrt(lax.optimization_barrier(jnp.mean(values * values, axis=-1, keepdims=True)) + norm_eps) * gain

def slot_table(routes):
    blocks = routes.reshape(N_EXPERT, TOK_DEV * TOP)
    onehot = (blocks[:, :, None] == jnp.arange(EXPERT_COUNT, dtype=jnp.int32)[None, None, :]).astype(jnp.int32)
    within = lax.optimization_barrier(jnp.sum((jnp.cumsum(onehot, axis=1) - 1) * onehot, axis=2))
    block_ids = jnp.arange(N_EXPERT, dtype=jnp.int32)[:, None]
    slots = blocks * (N_EXPERT * CAP) + block_ids * CAP + within
    return slots.reshape(-1).astype(jnp.int32)

def sequence_out(parameter_list, frozen, tokens, routes, route_weight, adapter_slot):
    qkv_a, qkv_b, out_a, out_b, in_a, mid_b, down_a, down_b = parameter_list
    attention_gain, expert_norm_gain, query_key_value_weight, output_weight, gate_up_weight, down_weight = frozen
    normed = low(rms_scale(tokens, attention_gain))
    low_qkv = low(jnp.einsum('ld,jrd->jlr', normed, qkv_a[:, adapter_slot], precision=highest))
    project = jnp.einsum('ld,jde->jle', normed, query_key_value_weight, precision=highest)
    project = both_low(project + jnp.einsum('jlr,jre->jle', low_qkv, qkv_b[:, adapter_slot], precision=highest))
    queries = project[0].reshape(LENGTH, H, HEAD)
    keys = project[1].reshape(LENGTH, H, HEAD)
    values = project[2].reshape(LENGTH, H, HEAD)
    scale = HEAD ** (-0.5)

    def attend(query_block):
        scores = low_back(jnp.einsum('bhd,khd->hbk', query_block, keys, precision=highest) * scale)
        probs = low(jax.nn.softmax(scores, axis=-1))
        return jnp.einsum('hbk,khd->bhd', probs, values, precision=highest)
    mixed = lax.map(jax.checkpoint(attend), queries.reshape(LENGTH // BLK, BLK, H, HEAD))
    mixed = both_low(mixed.reshape(LENGTH, MODEL_WIDTH))
    out_rank = jnp.einsum('ld,rd->lr', mixed, out_a[adapter_slot], precision=highest)
    branch = jnp.dot(mixed, output_weight, precision=highest) + jnp.dot(out_rank, out_b[adapter_slot], precision=highest)
    resid = tokens + low_back(branch)
    moe_in = low(rms_scale(resid, expert_norm_gain))
    slots = slot_table(routes)
    token_rows = jnp.repeat(jnp.arange(LENGTH, dtype=jnp.int32), TOP)
    copies = low_back(moe_in[token_rows])
    table = jnp.zeros((EXPERT_COUNT * N_EXPERT * CAP, MODEL_WIDTH), jnp.float32).at[slots].set(copies)
    table = table.reshape(EXPERT_COUNT, N_EXPERT * CAP, MODEL_WIDTH)
    in_rank = both_low(jnp.einsum('ecd,ejrd->ejcr', table, in_a[:, :, adapter_slot], precision=highest))
    gate_up = jnp.einsum('ecd,ejdf->ejcf', table, gate_up_weight, precision=highest)
    gate_up = low_back(gate_up + jnp.einsum('ejcr,ejrf->ejcf', in_rank, mid_b[:, :, adapter_slot], precision=highest))
    active = both_low(jax.nn.silu(gate_up[:, 0]) * gate_up[:, 1])
    down_rank = both_low(jnp.einsum('ecf,erf->ecr', active, down_a[:, adapter_slot], precision=highest))
    expert_out = jnp.einsum('ecf,efd->ecd', active, down_weight, precision=highest)
    expert_out = both_low(expert_out + jnp.einsum('ecr,erd->ecd', down_rank, down_b[:, adapter_slot], precision=highest))
    picked = expert_out.reshape(-1, MODEL_WIDTH)[slots].reshape(LENGTH, TOP, MODEL_WIDTH)
    return resid + lax.optimization_barrier(jnp.sum(route_weight[:, :, None] * picked, axis=1))

def adam_step(grad, weight, first, second, factor_array, step_number):
    clipped = grad * factor_array
    first_new = beta_one * first + (1.0 - beta_one) * clipped
    second_new = beta_two * second + (1.0 - beta_two) * clipped * clipped
    fix_first = 1.0 - jnp.power(beta_one, step_number)
    fix_second = 1.0 - jnp.power(beta_two, step_number)
    update = -learn_rate * (first_new / fix_first / (jnp.sqrt(second_new / fix_second) + adam_eps) + weight_decay * weight)
    return (first_new, second_new, update)

def reference(hidden, output_cotangent, attention_gain, expert_norm_gain, query_key_value_weight, output_weight, gate_up_weight, down_weight, token_experts, expert_gate_weight, sequence_adapter, optimizer_steps, adapter_attention_input, adapter_attention_output, adapter_projection_input, adapter_projection_output, adapter_hidden_input, adapter_hidden_output, adapter_down_input, adapter_down_output, moment_attention_input, moment_attention_output, moment_projection_input, moment_projection_output, moment_hidden_input, moment_hidden_output, moment_down_input, moment_down_output, squared_attention_input, squared_attention_output, squared_projection_input, squared_projection_output, squared_hidden_input, squared_hidden_output, squared_down_input, squared_down_output):
    frozen = (attention_gain.astype(jnp.float32), expert_norm_gain.astype(jnp.float32), query_key_value_weight.astype(jnp.float32), output_weight.astype(jnp.float32), gate_up_weight.astype(jnp.float32), down_weight.astype(jnp.float32))
    parameter_list = (adapter_attention_input.astype(jnp.float32), adapter_attention_output.astype(jnp.float32), adapter_projection_input.astype(jnp.float32), adapter_projection_output.astype(jnp.float32), adapter_hidden_input.astype(jnp.float32), adapter_hidden_output.astype(jnp.float32), adapter_down_input.astype(jnp.float32), adapter_down_output.astype(jnp.float32))

    def forward(params_in, tokens_in):

        def one_sequence(carry, items):
            tokens, routes, route_weight, adapter_slot = items
            return (carry, sequence_out(params_in, frozen, tokens, routes, route_weight, adapter_slot))
        unused, outputs = lax.scan(jax.checkpoint(one_sequence), jnp.zeros((), jnp.float32), (tokens_in, token_experts, expert_gate_weight, sequence_adapter))
        return outputs
    result, pullback = jax.vjp(forward, parameter_list, hidden.astype(jnp.float32))
    grads, grad_tokens = pullback(output_cotangent.astype(jnp.float32))
    total = jnp.zeros((), jnp.float32)
    for grad in grads:
        total = total + jnp.sum(grad * grad)
    norm_value = jnp.sqrt(total)
    factor_array = jnp.minimum(1.0, CLIP / norm_value)
    step_number = optimizer_steps[0].astype(jnp.float32)
    state_qkv_a = adam_step(grads[0], parameter_list[0], moment_attention_input, squared_attention_input, factor_array, step_number)
    state_qkv_b = adam_step(grads[1], parameter_list[1], moment_attention_output, squared_attention_output, factor_array, step_number)
    state_out_a = adam_step(grads[2], parameter_list[2], moment_projection_input, squared_projection_input, factor_array, step_number)
    state_out_b = adam_step(grads[3], parameter_list[3], moment_projection_output, squared_projection_output, factor_array, step_number)
    state_in_a = adam_step(grads[4], parameter_list[4], moment_hidden_input, squared_hidden_input, factor_array, step_number)
    state_mid_b = adam_step(grads[5], parameter_list[5], moment_hidden_output, squared_hidden_output, factor_array, step_number)
    state_down_a = adam_step(grads[6], parameter_list[6], moment_down_input, squared_down_input, factor_array, step_number)
    state_down_b = adam_step(grads[7], parameter_list[7], moment_down_output, squared_down_output, factor_array, step_number)
    return (result.astype(jnp.bfloat16), grad_tokens, norm_value.reshape(1), grads[0], state_qkv_a[0], state_qkv_a[1], state_qkv_a[2], grads[1], state_qkv_b[0], state_qkv_b[1], state_qkv_b[2], grads[2], state_out_a[0], state_out_a[1], state_out_a[2], grads[3], state_out_b[0], state_out_b[1], state_out_b[2], grads[4], state_in_a[0], state_in_a[1], state_in_a[2], grads[5], state_mid_b[0], state_mid_b[1], state_mid_b[2], grads[6], state_down_a[0], state_down_a[1], state_down_a[2], grads[7], state_down_b[0], state_down_b[1], state_down_b[2])
```

```python
import jax
import jax.numpy as jnp
from jax import lax
from jax.sharding import PartitionSpec as P

MODEL_WIDTH = 2048
HEAD = 128
TOP = 8
ADAPTER_COUNT = 8
EXP_DEV = 2
CLIP = 256


norm_eps = 1e-05
beta_one = 0.9
beta_two = 0.95
learn_rate = 0.02
weight_decay = 0.1
adam_eps = 1e-08
highest = lax.Precision.HIGHEST
single = jnp.float32
brain = jnp.bfloat16


def rms_scale(values, gain):
    return values * lax.rsqrt(jnp.mean(values * values, axis=-1, keepdims=True) + norm_eps) * gain


def norm_back(values, gain, grad):
    inverse = lax.rsqrt(jnp.mean(values * values, axis=-1, keepdims=True) + norm_eps)
    scaled = grad * gain
    return inverse * scaled - values * inverse * inverse * inverse * jnp.mean(
        scaled * values, axis=-1, keepdims=True
    )


def select_adapter(array, adapter_slot, axis):
    return lax.dynamic_index_in_dim(array, adapter_slot, axis, keepdims=False)


def spread_out(compact, marker, axis):
    shape = [1] * (compact.ndim + 1)
    shape[axis] = marker.shape[0]
    return jnp.expand_dims(compact, axis) * marker.reshape(shape)


def local_portion(weight, piece_index, pieces):
    width = weight.shape[-1] // pieces
    return lax.dynamic_slice_in_dim(weight, piece_index * width, width, weight.ndim - 1).astype(
        single
    )


def adam_step(grad, weight, first, second, factor_array, step_number):
    clipped = grad * factor_array
    first_new = beta_one * first + (1.0 - beta_one) * clipped
    second_new = beta_two * second + (1.0 - beta_two) * clipped * clipped
    fix_first = 1.0 - jnp.power(beta_one, step_number)
    fix_second = 1.0 - jnp.power(beta_two, step_number)
    update = -learn_rate * (
        first_new / fix_first / (jnp.sqrt(second_new / fix_second) + adam_eps)
        + weight_decay * weight
    )
    return (first_new, second_new, update)


def per_device(
    hidden,
    output_cotangent,
    attention_gain,
    expert_norm_gain,
    query_key_value_weight,
    output_weight,
    gate_up_weight,
    down_weight,
    token_experts,
    expert_gate_weight,
    sequence_adapter,
    optimizer_steps,
    adapter_attention_input,
    adapter_attention_output,
    adapter_projection_input,
    adapter_projection_output,
    adapter_hidden_input,
    adapter_hidden_output,
    adapter_down_input,
    adapter_down_output,
    moment_attention_input,
    moment_attention_output,
    moment_projection_input,
    moment_projection_output,
    moment_hidden_input,
    moment_hidden_output,
    moment_down_input,
    moment_down_output,
    squared_attention_input,
    squared_attention_output,
    squared_projection_input,
    squared_projection_output,
    squared_hidden_input,
    squared_hidden_output,
    squared_down_input,
    squared_down_output,
):
    group_list = lax.axis_size("expert")
    replica_total = lax.axis_size("dp")
    replica_index = lax.axis_index("dp")
    group_index = lax.axis_index("expert")
    adapter_slot = lax.dynamic_index_in_dim(sequence_adapter, replica_index, 0, keepdims=False)
    tok_dev = hidden.shape[1]
    length = tok_dev * group_list
    width_here = query_key_value_weight.shape[2]
    heads_here = width_here // HEAD
    block = min(512, length)
    nblocks = length // block
    scale = HEAD ** (-0.5)
    experts_all = EXP_DEV * group_list
    cap = min(tok_dev, tok_dev * TOP * 5 // (4 * experts_all))
    picked_projection_input = select_adapter(adapter_projection_input, adapter_slot, 0)
    picked_projection_output = select_adapter(adapter_projection_output, adapter_slot, 0)
    picked_attention_input = select_adapter(adapter_attention_input, adapter_slot, 1)
    picked_attention_output = select_adapter(adapter_attention_output, adapter_slot, 1)
    picked_hidden_input = select_adapter(adapter_hidden_input, adapter_slot, 2)
    picked_hidden_output = select_adapter(adapter_hidden_output, adapter_slot, 2)
    picked_down_input = select_adapter(adapter_down_input, adapter_slot, 1)
    picked_down_output = select_adapter(adapter_down_output, adapter_slot, 1)

    def mm(spec, left, right):
        return jnp.einsum(spec, left, right, preferred_element_type=single)

    tokens = hidden[0].astype(single)
    normed = rms_scale(tokens, attention_gain).astype(brain)
    sequence = lax.all_gather(normed, "expert", axis=0, tiled=True)
    top_seq = lax.all_gather(output_cotangent[0], "expert", axis=0, tiled=True)
    routes = token_experts[0]
    dense = jnp.sum(
        jnp.where(
            routes[:, :, None] == jnp.arange(experts_all, dtype=jnp.int32)[None, None, :],
            expert_gate_weight[0][:, :, None],
            0.0,
        ),
        axis=1,
    )
    dense_all = lax.all_gather(dense.T, "expert", axis=0, tiled=False)
    dense_here = lax.dynamic_slice_in_dim(dense_all, group_index * EXP_DEV, EXP_DEV, 1)
    chosen = dense_here > 0.0
    upper = (
        jnp.arange(tok_dev)[:, None] < jnp.arange(tok_dev)[None, :]
    ).astype(brain)
    place = mm("bet,tu->beu", chosen.astype(brain), upper).astype(jnp.int32)
    pick = (
        (place[:, :, None, :] == jnp.arange(cap, dtype=jnp.int32)[None, None, :, None])
        & chosen[:, :, None, :]
    ).astype(brain)
    slot_weight = jnp.sum(pick.astype(single) * dense_here[:, :, None, :], axis=-1)
    slot_weight = jnp.transpose(slot_weight, (1, 0, 2)).reshape(EXP_DEV, group_list * cap, 1)

    low_qkv = mm("ld,jrd->jlr", sequence, picked_attention_input).astype(brain)
    project = mm("ld,jde->jle", sequence, query_key_value_weight)
    project = (project + mm("jlr,jre->jle", low_qkv, picked_attention_output)).astype(brain)
    queries = project[0].reshape(length, heads_here, HEAD)
    keys = project[1].reshape(length, heads_here, HEAD)
    values = project[2].reshape(length, heads_here, HEAD)

    def attend(query_block):
        scores = mm("bhd,khd->hbk", query_block, keys) * scale
        peak = jnp.max(scores, axis=-1, keepdims=True)
        expo = jnp.exp(scores - peak)
        totals = jnp.sum(expo, axis=-1, keepdims=True)
        probs = (expo / totals).astype(brain)
        mixed_block = mm("hbk,khd->bhd", probs, values).astype(brain)
        return (mixed_block, (peak + jnp.log(totals))[..., 0])

    query_blocks = queries.reshape(nblocks, block, heads_here, HEAD)
    mixed, log_sums = lax.map(attend, query_blocks)
    mixed = mixed.reshape(length, width_here)
    out_rank = mm("le,re->lr", mixed, picked_projection_input).astype(brain)
    branch = lax.psum_scatter(
        (jnp.dot(mixed, output_weight, preferred_element_type=single)
        + jnp.dot(out_rank, picked_projection_output, preferred_element_type=single)).astype(brain),
        "expert",
        scatter_dimension=0,
        tiled=True,
    ).astype(single)
    resid = tokens + branch
    moe_in = rms_scale(resid, expert_norm_gain).astype(brain)
    moe_seq = lax.all_gather(moe_in, "expert", axis=0, tiled=True)

    def gather_rows(seq):
        rows = mm("best,btd->ebsd", pick, seq.reshape(group_list, tok_dev, -1)).astype(brain)
        return rows.reshape(EXP_DEV, group_list * cap, -1)

    def combine(rows):
        rows = rows.reshape(EXP_DEV, group_list, cap, -1)
        return mm("best,ebsd->btd", pick, rows).reshape(length, -1)

    top_rows = gather_rows(top_seq)
    arrived = gather_rows(moe_seq)
    in_rank = mm("ecd,ejrd->ejcr", arrived, picked_hidden_input).astype(brain)
    gate_up = mm("ecd,ejdf->ejcf", arrived, gate_up_weight)
    gate_up = gate_up + mm("ejcr,ejrf->ejcf", in_rank, picked_hidden_output)
    sigmoid_gate = jax.nn.sigmoid(gate_up[:, 0])
    swish_gate = gate_up[:, 0] * sigmoid_gate
    active = (swish_gate * gate_up[:, 1]).astype(brain)
    down_rank = mm("ecf,erf->ecr", active, picked_down_input).astype(brain)
    expert_out = mm("ecf,efd->ecd", active, down_weight)
    expert_out = expert_out + mm("ecr,erd->ecd", down_rank, picked_down_output)
    expert_out = (slot_weight * expert_out).astype(brain)
    moe_out = lax.psum_scatter(
        combine(expert_out).astype(brain), "expert", scatter_dimension=0, tiled=True
    ).astype(single)
    block_out = (resid + moe_out).astype(brain)
    grad_top = output_cotangent[0].astype(single)
    grad_down_rank = (slot_weight * mm("ecd,erd->ecr", top_rows, picked_down_output)).astype(brain)
    grad_active = slot_weight * mm("ecd,efd->ecf", top_rows, down_weight)
    grad_active = grad_active + mm("ecr,erf->ecf", grad_down_rank, picked_down_input)
    g_down_b = mm("ecr,ecd->erd", (slot_weight * down_rank).astype(brain), top_rows)
    g_down_a = mm("ecr,ecf->erf", grad_down_rank, active)
    grad_gate = (
        grad_active * gate_up[:, 1] * sigmoid_gate * (1.0 + gate_up[:, 0] * (1.0 - sigmoid_gate))
    )
    grad_up = grad_active * swish_gate
    grad_gate_up = jnp.stack([grad_gate, grad_up], axis=1).astype(brain)
    grad_in_rank = mm("ejcf,ejrf->ejcr", grad_gate_up, picked_hidden_output).astype(brain)
    g_mid_b = mm("ejcr,ejcf->ejrf", in_rank, grad_gate_up)
    g_in_a = mm("ejcr,ecd->ejrd", grad_in_rank, arrived)
    grad_slots = mm("ejcf,ejdf->ecd", grad_gate_up, gate_up_weight)
    grad_slots = (grad_slots + mm("ejcr,ejrd->ecd", grad_in_rank, picked_hidden_input)).astype(brain)
    grad_moe_in = lax.psum_scatter(
        combine(grad_slots).astype(brain), "expert", scatter_dimension=0, tiled=True
    ).astype(single)
    grad_resid = grad_top + norm_back(resid, expert_norm_gain, grad_moe_in)
    grad_branch = grad_resid.astype(brain)
    branch_full = lax.all_gather(grad_branch, "expert", axis=0, tiled=True)
    grad_out_rank = mm("ld,rd->lr", branch_full, picked_projection_output).astype(brain)
    grad_mixed = mm("ld,ed->le", branch_full, output_weight)
    grad_mixed = (
        grad_mixed
        + jnp.dot(grad_out_rank, picked_projection_input, preferred_element_type=single)
    ).astype(brain)
    g_out_b = mm("lr,ld->rd", out_rank, branch_full)
    g_out_a = mm("lr,le->re", grad_out_rank, mixed)

    def back_block(carry, items):
        grad_keys, grad_values = carry
        query_block, grad_block, log_block = items
        scores = mm("bhd,khd->hbk", query_block, keys) * scale
        probs = jnp.exp(scores - log_block[..., None])
        grad_probs = mm("bhd,khd->hbk", grad_block, values)
        grad_scores = (
            probs * (grad_probs - jnp.sum(grad_probs * probs, axis=-1, keepdims=True))
        ).astype(brain)
        grad_query = mm("hbk,khd->bhd", grad_scores, keys) * scale
        grad_keys = grad_keys + mm("hbk,bhd->khd", grad_scores, query_block) * scale
        grad_values = grad_values + mm("hbk,bhd->khd", probs.astype(brain), grad_block)
        return ((grad_keys, grad_values), grad_query.astype(brain))

    zeros_heads = jnp.zeros((length, heads_here, HEAD), single)
    grad_blocks = grad_mixed.reshape(nblocks, block, heads_here, HEAD)
    (grad_keys, grad_values), grad_queries = lax.scan(
        back_block, (zeros_heads, zeros_heads), (query_blocks, grad_blocks, log_sums)
    )
    grad_project = jnp.stack(
        [
            grad_queries.reshape(length, width_here),
            grad_keys.reshape(length, width_here).astype(brain),
            grad_values.reshape(length, width_here).astype(brain),
        ],
        axis=0,
    )
    g_qkv_b = mm("jlr,jle->jre", low_qkv, grad_project)
    grad_low = mm("jle,jre->jlr", grad_project, picked_attention_output).astype(brain)
    g_qkv_a = mm("jlr,ld->jrd", grad_low, sequence)
    grad_normed = lax.psum_scatter(
        (
            mm("jle,jde->ld", grad_project, query_key_value_weight)
            + mm("jlr,jrd->ld", grad_low, picked_attention_input)
        ).astype(jnp.bfloat16),
        "expert",
        scatter_dimension=0,
        tiled=True,
    ).astype(jnp.float32)
    grad_tokens = grad_resid + norm_back(tokens, attention_gain, grad_normed)

    rank = g_out_b.shape[0]
    chosen_adapters = (
        sequence_adapter[:, None] == jnp.arange(ADAPTER_COUNT, dtype=jnp.int32)[None, :]
    ).astype(single)

    def columns(grad):
        return jnp.moveaxis(
            grad.reshape(-1, replica_total, grad.shape[-1] // replica_total), 1, 0
        )

    def place_adapters(pieces, shape):
        spread = jnp.sum(
            pieces[:, :, None] * chosen_adapters[:, None, :, None, None], axis=0
        )
        return spread.reshape(shape)

    per_expert = [g_in_a, g_mid_b, g_down_a, g_down_b, g_qkv_b, g_out_a]
    split = [columns(grad.astype(brain)) for grad in per_expert]
    flat = [part.reshape(replica_total, -1, rank * part.shape[-1]) for part in split]
    joined = jnp.concatenate([part.reshape(replica_total, -1) for part in flat], axis=1)
    swapped = lax.all_to_all(
        joined.reshape(replica_total, -1, 128), "dp", split_axis=0, concat_axis=0, tiled=True
    ).reshape(replica_total, -1)
    at = 0
    placed = []
    for grad, part in zip(per_expert, split):
        size = part.shape[1] * part.shape[2]
        got = swapped[:, at : at + size].astype(single)
        at = at + size
        lead = grad.shape[:-2]
        got = got.reshape(replica_total, -1, rank, part.shape[2])
        placed.append(place_adapters(got, lead + (ADAPTER_COUNT, rank, part.shape[2])))
    summed_hidden_input, sum_mid_b, sum_down_a, sum_down_b, sum_qkv_b, sum_out_a = placed

    shared = jnp.concatenate([g_qkv_a.reshape(-1, MODEL_WIDTH), g_out_b], axis=0)
    piece = MODEL_WIDTH // (replica_total * group_list)
    shared = jnp.transpose(
        shared.reshape(-1, replica_total, group_list, piece), (2, 0, 1, 3)
    ).reshape(group_list, -1, replica_total * piece)
    shared = lax.psum_scatter(shared, "expert", scatter_dimension=0, tiled=True)[0]
    shared = jnp.moveaxis(shared.reshape(-1, replica_total, piece), 1, 0)
    shared = lax.all_to_all(shared, "dp", split_axis=0, concat_axis=0, tiled=True)
    shared = shared.reshape(replica_total, -1, rank, piece)
    shared = place_adapters(shared, (-1, ADAPTER_COUNT, rank, piece))
    sum_qkv_a, sum_out_b = shared[:3], shared[3]

    squares = jnp.zeros((), single)
    for grad in (
        sum_qkv_a,
        sum_qkv_b,
        sum_out_a,
        sum_out_b,
        summed_hidden_input,
        sum_mid_b,
        sum_down_a,
        sum_down_b,
    ):
        squares = squares + jnp.sum(grad * grad)
    norm_value = jnp.sqrt(lax.psum(squares, ("dp", "expert")))
    factor_array = jnp.minimum(1.0, CLIP / norm_value)
    step_number = optimizer_steps[0].astype(single)
    common_index = replica_index * group_list + group_index
    state_qkv_a = adam_step(
        sum_qkv_a,
        local_portion(adapter_attention_input, common_index, replica_total * group_list),
        moment_attention_input,
        squared_attention_input,
        factor_array,
        step_number,
    )
    state_qkv_b = adam_step(
        sum_qkv_b,
        local_portion(adapter_attention_output, replica_index, replica_total),
        moment_attention_output,
        squared_attention_output,
        factor_array,
        step_number,
    )
    state_out_a = adam_step(
        sum_out_a,
        local_portion(adapter_projection_input, replica_index, replica_total),
        moment_projection_input,
        squared_projection_input,
        factor_array,
        step_number,
    )
    state_out_b = adam_step(
        sum_out_b,
        local_portion(adapter_projection_output, common_index, replica_total * group_list),
        moment_projection_output,
        squared_projection_output,
        factor_array,
        step_number,
    )
    state_in_a = adam_step(
        summed_hidden_input,
        local_portion(adapter_hidden_input, replica_index, replica_total),
        moment_hidden_input,
        squared_hidden_input,
        factor_array,
        step_number,
    )
    state_mid_b = adam_step(
        sum_mid_b,
        local_portion(adapter_hidden_output, replica_index, replica_total),
        moment_hidden_output,
        squared_hidden_output,
        factor_array,
        step_number,
    )
    state_down_a = adam_step(
        sum_down_a,
        local_portion(adapter_down_input, replica_index, replica_total),
        moment_down_input,
        squared_down_input,
        factor_array,
        step_number,
    )
    state_down_b = adam_step(
        sum_down_b,
        local_portion(adapter_down_output, replica_index, replica_total),
        moment_down_output,
        squared_down_output,
        factor_array,
        step_number,
    )
    return (
        block_out.reshape(1, tok_dev, MODEL_WIDTH),
        grad_tokens.reshape(1, tok_dev, MODEL_WIDTH),
        norm_value.reshape(1),
        sum_qkv_a,
        state_qkv_a[0],
        state_qkv_a[1],
        state_qkv_a[2],
        sum_qkv_b,
        state_qkv_b[0],
        state_qkv_b[1],
        state_qkv_b[2],
        sum_out_a,
        state_out_a[0],
        state_out_a[1],
        state_out_a[2],
        sum_out_b,
        state_out_b[0],
        state_out_b[1],
        state_out_b[2],
        summed_hidden_input,
        state_in_a[0],
        state_in_a[1],
        state_in_a[2],
        sum_mid_b,
        state_mid_b[0],
        state_mid_b[1],
        state_mid_b[2],
        sum_down_a,
        state_down_a[0],
        state_down_a[1],
        state_down_a[2],
        sum_down_b,
        state_down_b[0],
        state_down_b[1],
        state_down_b[2],
    )


def solution(mesh):
    return jax.shard_map(
        per_device,
        mesh=mesh,
        in_specs=(
            P("dp", "expert", None),
            P("dp", "expert", None),
            P(),
            P(),
            P(None, None, "expert"),
            P("expert", None),
            P("expert", None, None, None),
            P("expert", None, None),
            P("dp", "expert", None),
            P("dp", "expert", None),
            P(),
            P(),
            P(),
            P(None, None, None, "expert"),
            P(None, None, "expert"),
            P(),
            P("expert", None, None, None, None),
            P("expert", None, None, None, None),
            P("expert", None, None, None),
            P("expert", None, None, None),
            P(None, None, None, ("dp", "expert")),
            P(None, None, None, ("expert", "dp")),
            P(None, None, ("expert", "dp")),
            P(None, None, ("dp", "expert")),
            P("expert", None, None, None, "dp"),
            P("expert", None, None, None, "dp"),
            P("expert", None, None, "dp"),
            P("expert", None, None, "dp"),
            P(None, None, None, ("dp", "expert")),
            P(None, None, None, ("expert", "dp")),
            P(None, None, ("expert", "dp")),
            P(None, None, ("dp", "expert")),
            P("expert", None, None, None, "dp"),
            P("expert", None, None, None, "dp"),
            P("expert", None, None, "dp"),
            P("expert", None, None, "dp"),
        ),
        out_specs=(
            P("dp", "expert", None),
            P("dp", "expert", None),
            P(),
            P(None, None, None, ("dp", "expert")),
            P(None, None, None, ("dp", "expert")),
            P(None, None, None, ("dp", "expert")),
            P(None, None, None, ("dp", "expert")),
            P(None, None, None, ("expert", "dp")),
            P(None, None, None, ("expert", "dp")),
            P(None, None, None, ("expert", "dp")),
            P(None, None, None, ("expert", "dp")),
            P(None, None, ("expert", "dp")),
            P(None, None, ("expert", "dp")),
            P(None, None, ("expert", "dp")),
            P(None, None, ("expert", "dp")),
            P(None, None, ("dp", "expert")),
            P(None, None, ("dp", "expert")),
            P(None, None, ("dp", "expert")),
            P(None, None, ("dp", "expert")),
            P("expert", None, None, None, "dp"),
            P("expert", None, None, None, "dp"),
            P("expert", None, None, None, "dp"),
            P("expert", None, None, None, "dp"),
            P("expert", None, None, None, "dp"),
            P("expert", None, None, None, "dp"),
            P("expert", None, None, None, "dp"),
            P("expert", None, None, None, "dp"),
            P("expert", None, None, "dp"),
            P("expert", None, None, "dp"),
            P("expert", None, None, "dp"),
            P("expert", None, None, "dp"),
            P("expert", None, None, "dp"),
            P("expert", None, None, "dp"),
            P("expert", None, None, "dp"),
            P("expert", None, None, "dp"),
        ),
        check_vma=False,
    )
```

```python
import functools

import jax
import jax.numpy as jnp
from jax import lax
from jax.experimental import pallas as pl
from jax.experimental.pallas import tpu as pltpu
from jax.sharding import PartitionSpec as P


single = jnp.float32
brain = jnp.bfloat16
HEAD = 128
CHUNKS = 4
GATHER_SENDS = CHUNKS * 7
SCATTER_SEMS = CHUNKS * 7
norm_eps = 1e-05
VMEM_ALL = 67043328


def dot(a, b, left=1, right=0):
    return lax.dot_general(a, b, (((left,), (right,)), ((), ())), preferred_element_type=single)


def peers():
    me = lax.axis_index("expert")
    core = me + 1 - 2 * (me % 2)
    across = me + 2 - 4 * ((me // 2) % 2)
    along = me + 4 - 8 * (me // 4)
    return me, core, across, along


def greet():
    me, core, across, along = peers()
    barrier = pltpu.get_barrier_semaphore()
    for peer in (core, across, along):
        pl.semaphore_signal(barrier, inc=1, device_id={"expert": peer})
    pl.semaphore_wait(barrier, 3)


class Mover:
    def __init__(self, send_sem, recv_sem):
        self.send_sem, self.recv_sem = send_sem, recv_sem
        self.me, self.core, self.across, self.along = peers()
        self.far = self.across + self.along - self.me
        self.pending = []
        self.waiting = []

    def go(self, src, dst, recv, peer):
        copy = pltpu.make_async_remote_copy(
            src_ref=src, dst_ref=dst, send_sem=self.send_sem.at[len(self.pending)],
            recv_sem=self.recv_sem.at[recv], device_id={"expert": peer},
        )
        copy.start()
        self.pending.append(copy)

    def later(self, *args):
        self.waiting.append(args)
        if len(self.waiting) > 1:
            self.go(*self.waiting.pop(0))

    def flush(self):
        while self.waiting:
            self.go(*self.waiting.pop(0))

    def got(self, view, recv):
        pltpu.make_async_remote_copy(
            src_ref=view, dst_ref=view, send_sem=self.send_sem.at[0], recv_sem=self.recv_sem.at[recv],
            device_id={"expert": self.core},
        ).wait_recv()

    def drain(self):
        for copy in self.pending:
            copy.wait_send()

    def beside(self, block):
        return block + 1 - 2 * (self.me % 2)


class Gather(Mover):
    def __init__(self, out, send_sem, recv_sem):
        super().__init__(send_sem, recv_sem)
        self.out = out
        self.size = out.shape[1] // CHUNKS

    def move(self, block, k, peer):
        view = self.out.at[block, pl.ds(k * self.size, self.size)]
        self.go(view, view, block * CHUNKS + k, peer)

    def arrive(self, block, k):
        self.got(self.out.at[block, pl.ds(k * self.size, self.size)], block * CHUNKS + k)

    def start(self):
        half = CHUNKS // 2
        for i in range(CHUNKS):
            self.move(self.me, i, self.across)
            self.move(self.me, (i + half) % CHUNKS, self.along)
            self.move(self.me, i, self.core)

    def relay(self, i):
        half = CHUNKS // 2
        k = (i + half) % CHUNKS
        self.arrive(self.across, i)
        if i < half:
            self.move(self.across, i, self.along)
        self.move(self.across, i, self.core)
        self.arrive(self.along, k)
        if k >= half:
            self.move(self.along, k, self.across)
        self.move(self.along, k, self.core)

    def relay_far(self, i):
        half = CHUNKS // 2
        for k in (i, i + half):
            self.arrive(self.far, k)
            self.move(self.far, k, self.core)

    def pair(self, block):
        for k in range(CHUNKS):
            self.arrive(self.beside(block), k)


class Scatter(Mover):
    def __init__(self, part, pair, half_x, half_y, from_x, from_y, send_sem, recv_sem):
        super().__init__(send_sem, recv_sem)
        self.part, self.pair = part, pair
        self.half_x, self.half_y, self.from_x, self.from_y = half_x, half_y, from_x, from_y
        self.order = (self.far, self.across, self.along, self.me)
        self.size = part.shape[1] // CHUNKS
        half = CHUNKS // 2
        self.hx = 4 * CHUNKS
        self.hy = self.hx + half
        self.fx = self.hy + half
        self.fy = self.fx + CHUNKS

    def rows(self, k):
        return pl.ds(k * self.size, self.size)

    def give(self, i):
        other = self.beside(self.order[i])
        for k in range(CHUNKS):
            r = self.rows(k)
            self.go(self.part.at[other, r], self.pair.at[i, r], i * CHUNKS + k, self.core)

    def add(self, i, k, extra=None):
        r = self.rows(k)
        self.got(self.pair.at[i, r], i * CHUNKS + k)
        total = self.part[self.order[i], r].astype(single) + self.pair[i, r].astype(single)
        if extra is not None:
            ref, recv, k2 = extra
            r2 = self.rows(k2)
            self.got(ref.at[r2], recv)
            total = total + ref[r2].astype(single)
        self.pair[i, r] = total.astype(brain)

    def steps(self):
        half = CHUNKS // 2
        out = []

        def one(k):
            self.add(0, k)
            self.later(self.pair.at[0, self.rows(k)], self.half_x.at[self.rows(k)], self.hx + k, self.across)
            k2 = k + half
            self.add(0, k2)
            self.later(self.pair.at[0, self.rows(k2)], self.half_y.at[self.rows(k)], self.hy + k, self.along)

        def two(k):
            self.add(1, k)
            self.later(self.pair.at[1, self.rows(k)], self.from_x.at[self.rows(k)], self.fx + k, self.across)
            k2 = k + half
            self.add(2, k2)
            self.later(self.pair.at[2, self.rows(k2)], self.from_y.at[self.rows(k2)], self.fy + k2, self.along)

        def three(k):
            k2 = k + half
            self.add(1, k2, (self.half_y, self.hy + k, k))
            self.later(self.pair.at[1, self.rows(k2)], self.from_x.at[self.rows(k2)], self.fx + k2, self.across)
            self.add(2, k, (self.half_x, self.hx + k, k))
            self.later(self.pair.at[2, self.rows(k)], self.from_y.at[self.rows(k)], self.fy + k, self.along)

        for fn in (one, two, three):
            for k in range(half):
                out.append(functools.partial(fn, k))
        out.append(self.flush)
        return out

    def final(self, k):
        r = self.rows(k)
        self.got(self.pair.at[3, r], 3 * CHUNKS + k)
        total = self.part[self.me, r].astype(single) + self.pair[3, r].astype(single)
        self.got(self.from_x.at[r], self.fx + k)
        total = total + self.from_x[r].astype(single)
        self.got(self.from_y.at[r], self.fy + k)
        return total + self.from_y[r].astype(single)

    def final_order(self):
        half = CHUNKS // 2
        return [k + j * half for k in range(half) for j in range(2)]


def scatter_scratch(rows, cols):
    return [
        pltpu.VMEM((4, rows, cols), brain),
        pltpu.VMEM((rows // 2, cols), brain),
        pltpu.VMEM((rows // 2, cols), brain),
        pltpu.VMEM((rows, cols), brain),
        pltpu.VMEM((rows, cols), brain),
        pltpu.SemaphoreType.DMA((SCATTER_SEMS,)),
        pltpu.SemaphoreType.DMA((SCATTER_SEMS,)),
    ]


def gather_scratch(n):
    return [pltpu.SemaphoreType.DMA((GATHER_SENDS,)), pltpu.SemaphoreType.DMA((n * CHUNKS,))]


def rms(values, gain):
    return values * lax.rsqrt(jnp.mean(values * values, axis=-1, keepdims=True) + norm_eps) * gain


def front_kernel(
    hid_ref, top_ref, dense_ref, gain_ref, gain2_ref, w_ref, a_ref, b_ref, wo_ref, pa_ref, pb_ref,
    seq_ref, low_ref, proj_ref, mixed_ref, lse_ref, topseq_ref, denseall_ref, orank_ref, resid_ref, moe_ref,
    part, *sems,
):
    toks, width = hid_ref.shape
    span = w_ref.shape[2]
    heads = span // HEAD
    length = toks * seq_ref.shape[0]
    seq_g = Gather(seq_ref, sems[0], sems[1])
    top_g = Gather(topseq_ref, sems[2], sems[3])
    moe_g = Gather(moe_ref, sems[4], sems[5])
    red = Scatter(part, *sems[6:13])
    dsend, drecv, lsem = sems[13:16]
    me = seq_g.me
    n = seq_ref.shape[0]

    local = pltpu.make_async_copy(top_ref, topseq_ref.at[me], lsem.at[0])
    local.start()
    own = pltpu.make_async_copy(dense_ref, denseall_ref.at[me], lsem.at[1])
    own.start()
    seq_ref[me] = rms(hid_ref[...].astype(single), gain_ref[...]).astype(brain)
    barrier = pltpu.get_barrier_semaphore()
    for j in range(1, n):
        pl.semaphore_signal(barrier, inc=1, device_id={"expert": (me + j) % n})
    pl.semaphore_wait(barrier, n - 1)
    seq_g.start()
    dense_copies = []
    for j in range(1, n):
        copy = pltpu.make_async_remote_copy(
            src_ref=dense_ref, dst_ref=denseall_ref.at[me], send_sem=dsend.at[j - 1], recv_sem=drecv.at[me],
            device_id={"expert": (me + j) % n},
        )
        copy.start()
        dense_copies.append(copy)

    def qkv(block):
        p = block // 2
        both = seq_ref[pl.ds(2 * p, 2)].reshape(2 * toks, width)
        at = pl.ds(pl.multiple_of(p * 2 * toks, 2 * toks), 2 * toks)
        low = dot(both, a_ref[...], 1, 1).astype(brain)
        low_ref[at, :] = low
        for j in range(3):
            out = dot(both, w_ref[j]) + dot(low[:, 16 * j : 16 * j + 16], b_ref[j])
            proj_ref[j, at, :] = out.astype(brain)

    seq_g.pair(me)
    qkv(me)
    local.wait()
    for i in range(CHUNKS):
        seq_g.relay(i)
    top_g.start()
    seq_g.pair(seq_g.across)
    qkv(seq_g.across)
    for i in range(CHUNKS // 2):
        seq_g.relay_far(i)
    seq_g.pair(seq_g.along)
    qkv(seq_g.along)
    seq_g.pair(seq_g.far)
    qkv(seq_g.far)

    scale = HEAD ** (-0.5)
    block = 256
    top_steps = [functools.partial(top_g.relay, i) for i in range(CHUNKS)]
    top_steps += [functools.partial(top_g.relay_far, i) for i in range(CHUNKS // 2)]

    for h in range(heads):
        at = slice(h * HEAD, (h + 1) * HEAD)
        for i in range(length // block):
            r = pl.ds(i * block, block)
            scores = dot(proj_ref[0, r, at], proj_ref[1, :, at], 1, 1) * scale
            peak = jnp.max(scores, axis=-1, keepdims=True)
            expo = jnp.exp(scores - peak)
            total = jnp.sum(expo, axis=-1, keepdims=True)
            probs = (expo * (1.0 / total)).astype(brain)
            mixed_ref[r, at] = dot(probs, proj_ref[2, :, at]).astype(brain)
            lse_ref[r, h : h + 1] = peak + jnp.log(total)
            if top_steps and (h * (length // block) + i) % 2 == 1:
                top_steps.pop(0)()

    for i in range(4):
        p = red.order[i] // 2
        at = pl.ds(pl.multiple_of(p * 2 * toks, 2 * toks), 2 * toks)
        rank = dot(mixed_ref[at, :], pa_ref[...], 1, 1).astype(brain)
        orank_ref[at, :] = rank
        out = dot(mixed_ref[at, :], wo_ref[...]) + dot(rank, pb_ref[...])
        part[pl.ds(2 * p, 2)] = out.astype(brain).reshape(2, toks, width)
        if i:
            red.give(i - 1)
    red.give(3)
    while top_steps:
        top_steps.pop(0)()
    for step in red.steps():
        step()
    for block_at in (me, top_g.across, top_g.along, top_g.far):
        top_g.pair(block_at)
    for k in red.final_order():
        r = red.rows(k)
        resid = hid_ref[r].astype(single) + red.final(k)
        resid_ref[r] = resid
        moe_ref[me, r] = rms(resid, gain2_ref[...]).astype(brain)
    moe_g.start()
    for j in range(1, n):
        src = (me + j) % n
        view = denseall_ref.at[src]
        pltpu.make_async_remote_copy(
            src_ref=view, dst_ref=view, send_sem=dsend.at[0], recv_sem=drecv.at[src], device_id={"expert": src}
        ).wait_recv()
    for copy in dense_copies:
        copy.wait_send()
    own.wait()
    for i in range(CHUNKS):
        moe_g.relay(i)
    for i in range(CHUNKS // 2):
        moe_g.relay_far(i)
    for block_at in (me, moe_g.across, moe_g.along, moe_g.far):
        moe_g.pair(block_at)
    for mover in (seq_g, top_g, red, moe_g):
        mover.drain()


def front(hid, top, dense, gain, gain2, w, a, b, wo, pa, pb, n, cid=0):
    toks, width = hid.shape
    span = w.shape[2]
    length = toks * n
    vm = pl.BlockSpec(memory_space=pltpu.VMEM)
    f = lambda *s: jax.ShapeDtypeStruct(s, single)
    h = lambda *s: jax.ShapeDtypeStruct(s, brain)
    return pl.pallas_call(
        front_kernel,
        out_shape=(
            h(n, toks, width), h(length, a.shape[0]), h(3, length, span), h(length, span), f(length, span // HEAD),
            h(n, toks, width), f(n, *dense.shape), h(length, pa.shape[0]), f(toks, width), h(n, toks, width),
        ),
        in_specs=[vm] * 11,
        out_specs=[vm] * 10,
        scratch_shapes=[pltpu.VMEM((n, toks, width), brain)]
        + gather_scratch(n) + gather_scratch(n) + gather_scratch(n) + scatter_scratch(toks, width)
        + [pltpu.SemaphoreType.DMA((n,)), pltpu.SemaphoreType.DMA((n,)), pltpu.SemaphoreType.DMA((2,))],
        compiler_params=pltpu.CompilerParams(collective_id=cid, has_side_effects=True, vmem_limit_bytes=VMEM_ALL),
        name="front",
    )(hid, top, dense, gain, gain2, w, a, b, wo, pa, pb)


TILE = 256


def moe_kernel(
    cap, replicas,
    dense_ref, moe_hbm, top_hbm, gu_hbm, dn_hbm, ha_ref, hb_ref, da_ref, db_ref,
    ypart_hbm, gpart_hbm, gina_ref, gmidb_ref, gdna_ref, gdnb_ref,
    gu, dn, x_rows, g_rows, y_rows, s_rows, act, gg, uu, place, weight, irank, gdr, drank, girank,
    stage, out_stage, gu_sem, dn_sem, in_sem, out_sem,
):
    experts, hidden = 2, dn.shape[1]
    width = dn.shape[2]
    blocks, toks = moe_hbm.shape[0], moe_hbm.shape[1]
    rows = blocks * cap
    for e in range(experts):
        pltpu.make_async_copy(dn_hbm.at[e], dn.at[e], dn_sem.at[e]).start()
        pltpu.make_async_copy(gu_hbm.at[e], gu.at[e], gu_sem.at[e]).start()

    def fetch(b, slot):
        pltpu.make_async_copy(moe_hbm.at[b], stage.at[slot, 0], in_sem.at[slot, 0]).start()
        pltpu.make_async_copy(top_hbm.at[b], stage.at[slot, 1], in_sem.at[slot, 1]).start()

    fetch(0, 0)
    fetch(1, 1)
    dense = dense_ref[...]
    chosen = (dense > 0.0).astype(brain)
    upper = (
        lax.broadcasted_iota(jnp.int32, (toks, toks), 0)
        < lax.broadcasted_iota(jnp.int32, (toks, toks), 1)
    ).astype(single).astype(brain)
    before = dot(chosen, upper)
    place[...] = jnp.where(dense > 0.0, before, -1.0)
    slot_iota = lax.broadcasted_iota(jnp.int32, (cap, toks), 0).astype(single)

    def picks(b):
        return [(place[pl.ds(2 * b + e, 1), :] == slot_iota) for e in range(experts)]

    def gather(b, carry):
        slot = b % 2
        for j in range(2):
            pltpu.make_async_copy(moe_hbm.at[0], stage.at[slot, j], in_sem.at[slot, j]).wait()
        sel = picks(b)
        for e in range(experts):
            w = jnp.sum(jnp.where(sel[e], dense_ref[pl.ds(2 * b + e, 1), :], 0.0), axis=1, keepdims=True)
            weight[e, pl.ds(b * cap, cap), :] = w
        both = jnp.concatenate([m.astype(single).astype(brain) for m in sel], axis=0)
        at = pl.ds(b * cap, cap)
        for j, dst in ((0, x_rows), (1, g_rows)):
            got = dot(both, stage[slot, j]).astype(brain)
            dst[0, at, :] = got[:cap]
            dst[1, at, :] = got[cap:]

        @pl.when(b + 2 < blocks)
        def _():
            fetch(b + 2, slot)

        return carry

    lax.fori_loop(0, blocks, gather, 0)

    def expert(e, carry):
        pltpu.make_async_copy(dn_hbm.at[0], dn.at[e], dn_sem.at[e]).wait()
        pltpu.make_async_copy(gu_hbm.at[0], gu.at[e], gu_sem.at[e]).wait()
        w = weight[e]
        x = x_rows[e]
        irank[...] = dot(x, ha_ref[e], 1, 1).astype(brain)
        gdr[...] = (dot(g_rows[e], db_ref[e], 1, 1) * w).astype(brain)

        def tile(f, c):
            at = pl.ds(pl.multiple_of(f * TILE, TILE), TILE)
            gate = dot(x_rows[e], gu[e, 0, :, at]) + dot(irank[:, :16], hb_ref[e, 0, :, at])
            up = dot(x_rows[e], gu[e, 1, :, at]) + dot(irank[:, 16:], hb_ref[e, 1, :, at])
            ga = dot(g_rows[e], dn[e, at, :], 1, 1) * w + dot(gdr[...], da_ref[e, :, at])
            sig = jax.nn.sigmoid(gate)
            swish = gate * sig
            act[:, at] = (swish * up).astype(brain)
            gg[:, at] = (ga * up * sig * (1.0 + gate * (1.0 - sig))).astype(brain)
            uu[:, at] = (ga * swish).astype(brain)
            return c

        lax.fori_loop(0, hidden // TILE, tile, 0)
        drank[...] = dot(act[...], da_ref[e], 1, 1).astype(brain)
        girank[:, :16] = dot(gg[...], hb_ref[e, 0], 1, 1).astype(brain)
        girank[:, 16:] = dot(uu[...], hb_ref[e, 1], 1, 1).astype(brain)

        def deal(ref, row, value):
            piece = value.shape[1] // replicas
            at = pl.ds(pl.multiple_of(row, 16), value.shape[0])
            for d in range(replicas):
                ref[d, at, :] = value[:, d * piece : (d + 1) * piece].astype(brain)

        deal(gdnb_ref, e * 16, dot((drank[...].astype(single) * w).astype(brain), g_rows[e], 0, 0))
        deal(gdna_ref, e * 16, dot(gdr[...], act[...], 0, 0))
        deal(gmidb_ref, e * 32, dot(irank[:, :16], gg[...], 0, 0))
        deal(gmidb_ref, e * 32 + 16, dot(irank[:, 16:], uu[...], 0, 0))
        deal(gina_ref, e * 32, dot(girank[...], x_rows[e], 0, 0))

        def back(d, c):
            at = pl.ds(pl.multiple_of(d * TILE, TILE), TILE)
            s = dot(gg[...], gu[e, 0, at, :], 1, 1) + dot(uu[...], gu[e, 1, at, :], 1, 1)
            s = s + dot(girank[...], ha_ref[e, :, at])
            s_rows[e, :, at] = s.astype(brain)
            y = dot(act[...], dn[e, :, at]) + dot(drank[...], db_ref[e, :, at])
            y_rows[e, :, at] = (y * w).astype(brain)
            return c

        lax.fori_loop(0, width // TILE, back, 0)
        return carry

    lax.fori_loop(0, experts, expert, 0)

    def combine(b, carry):
        slot = b % 2

        @pl.when(b >= 2)
        def _():
            for j, dst in ((0, ypart_hbm), (1, gpart_hbm)):
                pltpu.make_async_copy(out_stage.at[slot, j], dst.at[0], out_sem.at[slot, j]).wait()

        sel = picks(b)
        both = jnp.concatenate([m.astype(single).astype(brain) for m in sel], axis=0)
        at = pl.ds(b * cap, cap)
        for j, (src, dst) in enumerate(((y_rows, ypart_hbm), (s_rows, gpart_hbm))):
            pair = jnp.concatenate([src[0, at, :], src[1, at, :]], axis=0)
            out_stage[slot, j] = dot(both, pair, 0, 0).astype(brain)
            pltpu.make_async_copy(out_stage.at[slot, j], dst.at[b], out_sem.at[slot, j]).start()
        return carry

    lax.fori_loop(0, blocks, combine, 0)
    for slot in range(2):
        for j, dst in ((0, ypart_hbm), (1, gpart_hbm)):
            pltpu.make_async_copy(out_stage.at[slot, j], dst.at[0], out_sem.at[slot, j]).wait()


def moe(dense, moe_seq, top_seq, gu, dn, ha, hb, da, db, cap, replicas):
    blocks, toks, width = moe_seq.shape
    experts, hidden = dn.shape[0], dn.shape[1]
    rank = da.shape[1]
    rows = blocks * cap
    vm = pl.BlockSpec(memory_space=pltpu.VMEM)
    any_ = pl.BlockSpec(memory_space=pl.ANY)
    f = lambda *s: jax.ShapeDtypeStruct(s, single)
    h = lambda *s: jax.ShapeDtypeStruct(s, brain)
    return pl.pallas_call(
        functools.partial(moe_kernel, cap, replicas),
        out_shape=(
            h(blocks, toks, width), h(blocks, toks, width),
            h(replicas, experts * 2 * rank, width // replicas), h(replicas, experts * 2 * rank, hidden // replicas),
            h(replicas, experts * rank, hidden // replicas), h(replicas, experts * rank, width // replicas),
        ),
        in_specs=[vm, any_, any_, any_, any_, vm, vm, vm, vm],
        out_specs=[any_, any_, vm, vm, vm, vm],
        scratch_shapes=[
            pltpu.VMEM((experts, 2, width, hidden), brain),
            pltpu.VMEM((experts, hidden, width), brain),
            pltpu.VMEM((experts, rows, width), brain),
            pltpu.VMEM((experts, rows, width), brain),
            pltpu.VMEM((experts, rows, width), brain),
            pltpu.VMEM((experts, rows, width), brain),
            pltpu.VMEM((rows, hidden), brain),
            pltpu.VMEM((rows, hidden), brain),
            pltpu.VMEM((rows, hidden), brain),
            pltpu.VMEM((blocks * experts, toks), single),
            pltpu.VMEM((experts, rows, 1), single),
            pltpu.VMEM((rows, 2 * rank), brain),
            pltpu.VMEM((rows, rank), brain),
            pltpu.VMEM((rows, rank), brain),
            pltpu.VMEM((rows, 2 * rank), brain),
            pltpu.VMEM((2, 2, toks, width), brain),
            pltpu.VMEM((2, 2, toks, width), brain),
            pltpu.SemaphoreType.DMA((experts,)),
            pltpu.SemaphoreType.DMA((experts,)),
            pltpu.SemaphoreType.DMA((2, 2)),
            pltpu.SemaphoreType.DMA((2, 2)),
        ],
        compiler_params=pltpu.CompilerParams(vmem_limit_bytes=67043328),
        name="moe",
    )(dense, moe_seq, top_seq, gu, dn, ha, hb, da, db)


def norm_back(values, gain, grad):
    inverse = lax.rsqrt(jnp.mean(values * values, axis=-1, keepdims=True) + norm_eps)
    scaled = grad * gain
    return inverse * scaled - values * (
        inverse * inverse * inverse * jnp.mean(scaled * values, axis=-1, keepdims=True)
    )


def back_kernel(
    replicas,
    gpart_ref, ypart_ref, resid_ref, hid_ref, top_ref, gain_ref, gain2_ref, seq_ref, low_ref, proj_ref, mixed_ref,
    lse_ref, orank_ref, w_ref, a_ref, b_ref, wo_ref, pa_ref, pb_ref,
    out_ref, gh_ref, gqb_ref, goa_ref, shared_ref,
    bf, part, gres, gmix, grank, gproj, glow, gk, gv, *sems,
):
    toks, width = hid_ref.shape
    span = w_ref.shape[2]
    heads = span // HEAD
    n = seq_ref.shape[0]
    length = toks * n
    red = Scatter(gpart_ref, *sems[0:7])
    redy = Scatter(ypart_ref, *sems[7:14])
    redn = Scatter(part, *sems[14:21])
    bf_g = Gather(bf, *sems[21:23])
    me = red.me
    greet()
    for i in range(4):
        red.give(i)
    for i in range(4):
        redy.give(i)
    for step in red.steps():
        step()
    for k in red.final_order():
        r = red.rows(k)
        grad = top_ref[r].astype(single) + norm_back(resid_ref[r], gain2_ref[...], red.final(k))
        gres[r] = grad
        bf[me, r] = grad.astype(brain)
    bf_g.start()

    def mixed_grad(block):
        p = block // 2
        both = bf[pl.ds(2 * p, 2)].reshape(2 * toks, width)
        at = pl.ds(pl.multiple_of(p * 2 * toks, 2 * toks), 2 * toks)
        rank = dot(both, pb_ref[...], 1, 1).astype(brain)
        grank[at, :] = rank
        gmix[at, :] = (dot(both, wo_ref[...], 1, 1) + dot(rank, pa_ref[...])).astype(brain)

    bf_g.pair(me)
    mixed_grad(me)
    for i in range(CHUNKS):
        bf_g.relay(i)
    bf_g.pair(bf_g.across)
    mixed_grad(bf_g.across)
    for i in range(CHUNKS // 2):
        bf_g.relay_far(i)
    bf_g.pair(bf_g.along)
    mixed_grad(bf_g.along)
    bf_g.pair(bf_g.far)
    mixed_grad(bf_g.far)

    goa = dot(grank[...], mixed_ref[...], 0, 0)
    piece = span // replicas
    for d in range(replicas):
        goa_ref[d] = goa[:, d * piece : (d + 1) * piece].astype(brain)

    steps = redy.steps()
    scale = HEAD ** (-0.5)
    block = 256
    for h in range(heads):
        at = slice(h * HEAD, (h + 1) * HEAD)
        for i in range(length // block):
            r = pl.ds(i * block, block)
            q, do = proj_ref[0, r, at], gmix[r, at]
            delta = jnp.sum(do.astype(single) * mixed_ref[r, at].astype(single), axis=-1, keepdims=True)
            probs = jnp.exp(dot(q, proj_ref[1, :, at], 1, 1) * scale - lse_ref[r, h : h + 1])
            gp = dot(do, proj_ref[2, :, at], 1, 1)
            gs = (probs * (gp - delta)).astype(brain)
            gproj[0, r, at] = (dot(gs, proj_ref[1, :, at]) * scale).astype(brain)
            dk = dot(gs, q, 0, 0)
            dv = dot(probs.astype(brain), do, 0, 0)
            if i == 0:
                gk[...] = dk
                gv[...] = dv
            elif i < length // block - 1:
                gk[...] += dk
                gv[...] += dv
            else:
                gproj[1, :, at] = ((gk[...] + dk) * scale).astype(brain)
                gproj[2, :, at] = (gv[...] + dv).astype(brain)
            if steps:
                steps.pop(0)()
    while steps:
        steps.pop(0)()

    for i in range(4):
        p = redn.order[i] // 2
        at = pl.ds(pl.multiple_of(p * 2 * toks, 2 * toks), 2 * toks)
        for j in range(3):
            glow[at, 16 * j : 16 * j + 16] = dot(gproj[j, at, :], b_ref[j], 1, 1).astype(brain)
        out = dot(glow[at, :], a_ref[...])
        for j in range(3):
            out = out + dot(gproj[j, at, :], w_ref[j], 1, 1)
        part[pl.ds(2 * p, 2)] = out.astype(brain).reshape(2, toks, width)
        if i:
            redn.give(i - 1)
    redn.give(3)
    for k in redy.final_order():
        r = redy.rows(k)
        out_ref[r] = (resid_ref[r] + redy.final(k)).astype(brain)

    thin = width // (n * replicas)

    def share(row, value, base):
        for c in range(value.shape[1] // thin):
            d, e = (base + c) // n, (base + c) % n
            shared_ref[e, row : row + value.shape[0], d * thin : (d + 1) * thin] = value[
                :, c * thin : (c + 1) * thin
            ].astype(brain)

    nsteps = redn.steps()

    def advance():
        if nsteps:
            nsteps.pop(0)()

    advance()
    for j in range(3):
        gqb = dot(low_ref[:, 16 * j : 16 * j + 16], gproj[j], 0, 0)
        for d in range(replicas):
            gqb_ref[d, 16 * j : 16 * j + 16, :] = gqb[:, d * piece : (d + 1) * piece].astype(brain)
    advance()
    cols = 512
    for c in range(width // cols):
        s = slice(c * cols, (c + 1) * cols)
        share(0, dot(glow[...], seq_ref[:, :, s].reshape(length, cols), 0, 0), c * cols // thin)
        advance()
        share(48, dot(orank_ref[...], bf[:, :, s].reshape(length, cols), 0, 0), c * cols // thin)
    while nsteps:
        advance()
    for k in redn.final_order():
        r = redn.rows(k)
        gh_ref[r] = gres[r] + norm_back(hid_ref[r].astype(single), gain_ref[...], redn.final(k))
    for mover in (red, redy, redn, bf_g):
        mover.drain()


def back(gpart, ypart, resid, hid, top, gain, gain2, seq, low, proj, mixed, lse, orank, w, a, b, wo, pa, pb, replicas, cid=1):
    n, toks, width = seq.shape
    span = w.shape[2]
    length = toks * n
    vm = pl.BlockSpec(memory_space=pltpu.VMEM)
    f = lambda *s: jax.ShapeDtypeStruct(s, single)
    h = lambda *s: jax.ShapeDtypeStruct(s, brain)
    return pl.pallas_call(
        functools.partial(back_kernel, replicas),
        out_shape=(
            h(toks, width), f(toks, width), h(replicas, 48, span // replicas), h(replicas, 16, span // replicas),
            h(n, 64, width // n),
        ),
        in_specs=[vm] * 19,
        out_specs=[vm] * 5,
        scratch_shapes=[
            pltpu.VMEM((n, toks, width), brain), pltpu.VMEM((n, toks, width), brain), pltpu.VMEM((toks, width), single),
            pltpu.VMEM((length, span), brain), pltpu.VMEM((length, 16), brain), pltpu.VMEM((3, length, span), brain),
            pltpu.VMEM((length, 48), brain), pltpu.VMEM((length, HEAD), single), pltpu.VMEM((length, HEAD), single),
        ]
        + scatter_scratch(toks, width) * 3 + gather_scratch(n),
        compiler_params=pltpu.CompilerParams(collective_id=cid, has_side_effects=True, vmem_limit_bytes=VMEM_ALL),
        name="back",
    )(gpart, ypart, resid, hid, top, gain, gain2, seq, low, proj, mixed, lse, orank, w, a, b, wo, pa, pb)


ADAPTERS = 8
RANK = 16
CLIP = 256.0
beta_one = 0.9
beta_two = 0.95
learn_rate = 0.02
weight_decay = 0.1
adam_eps = 1e-08


def update_kernel(
    n, replicas, groups, adapter_ref, step_ref, shared_ref, *refs
):
    pieces, refs = refs[:6], refs[6:]
    weight, first, second, refs = refs[:8], refs[8:16], refs[16:24], refs[24:]
    norm_ref, grad, new_first, new_second, change, refs = (
        refs[0], refs[1:9], refs[9:17], refs[17:25], refs[25:33], refs[33:]
    )
    got, refs = refs[:6], refs[6:]
    shared_in, shared_mid, shared_got, tot_e, tot_d, mine = refs[:6]
    sh_send, sh_recv, mid_send, mid_recv, p_send, p_recv, t_send, t_recv = refs[6:]
    me = lax.axis_index("expert")
    rep = lax.axis_index("dp")
    barrier = pltpu.get_barrier_semaphore()
    for j in range(1, n):
        pl.semaphore_signal(barrier, inc=1, device_id={"expert": (me + j) % n})
    for j in range(1, replicas):
        pl.semaphore_signal(barrier, inc=1, device_id={"dp": (rep + j) % replicas})
    pl.semaphore_wait(barrier, n - 1 + replicas - 1)
    pending = []

    def go(src, dst, send, recv, where):
        copy = pltpu.make_async_remote_copy(
            src_ref=src, dst_ref=dst, send_sem=send, recv_sem=recv, device_id=where
        )
        copy.start()
        pending.append(copy)

    def wait(view, send, recv):
        pltpu.make_async_remote_copy(
            src_ref=view, dst_ref=view, send_sem=send, recv_sem=recv, device_id={"expert": (me + 1) % n}
        ).wait_recv()

    for j in range(1, n):
        peer = (me + j) % n
        go(shared_ref.at[peer], shared_in.at[me], sh_send.at[j - 1], sh_recv.at[me], {"expert": peer})
    for j in range(1, replicas):
        peer = (rep + j) % replicas
        for i in range(6):
            go(
                pieces[i].at[peer], got[i].at[rep], p_send.at[i * replicas + j], p_recv.at[i * replicas + rep],
                {"dp": peer},
            )
    for i in range(6):
        got[i][rep] = pieces[i][rep]
    shared_in[me] = shared_ref[me]
    for j in range(1, n):
        src = (me + j) % n
        wait(shared_in.at[src], sh_send.at[0], sh_recv.at[src])
    total = shared_in[0].astype(single)
    for e in range(1, n):
        total = total + shared_in[e].astype(single)
    thin = shared_mid.shape[2]
    for d in range(replicas):
        shared_mid[d] = total[:, d * thin : (d + 1) * thin].astype(brain)
    shared_got[rep] = shared_mid[rep]
    for j in range(1, replicas):
        peer = (rep + j) % replicas
        go(shared_mid.at[peer], shared_got.at[rep], mid_send.at[j], mid_recv.at[rep], {"dp": peer})

    def place(a, source, base):
        count = groups[a]

        def body(t, acc):
            i, slot = t // ADAPTERS, t % ADAPTERS
            at = pl.ds(pl.multiple_of(base + i * RANK, RANK), RANK)
            value = jnp.zeros((RANK, grad[a].shape[1]), single)
            for s in range(replicas):
                keep = jnp.where(adapter_ref[s] == slot, 1.0, 0.0)
                value = value + source[s, at, :].astype(single) * keep
            grad[a][pl.ds(pl.multiple_of(t * RANK, RANK), RANK), :] = value
            return acc + value * value

        acc = lax.fori_loop(0, count * ADAPTERS, body, jnp.zeros((RANK, grad[a].shape[1]), single))
        return jnp.sum(acc)

    squares = jnp.zeros((), single)
    for i in range(6):
        for j in range(1, replicas):
            src = (rep + j) % replicas
            wait(got[i].at[src], p_send.at[0], p_recv.at[i * replicas + src])
        squares = squares + place(i + 2, got[i], 0)
    for j in range(1, replicas):
        src = (rep + j) % replicas
        wait(shared_got.at[src], mid_send.at[0], mid_recv.at[src])
    squares = squares + place(0, shared_got, 0) + place(1, shared_got, groups[0] * RANK)

    mine[0] = jnp.full(mine.shape[1:], squares, single)
    tot_e[me] = mine[0]
    for j in range(1, n):
        peer = (me + j) % n
        go(mine.at[0], tot_e.at[me], t_send.at[j], t_recv.at[me], {"expert": peer})
    for j in range(1, n):
        src = (me + j) % n
        wait(tot_e.at[src], t_send.at[0], t_recv.at[src])
    total = tot_e[0]
    for e in range(1, n):
        total = total + tot_e[e]
    mine[1] = total
    tot_d[rep] = mine[1]
    for j in range(1, replicas):
        peer = (rep + j) % replicas
        go(mine.at[1], tot_d.at[rep], t_send.at[n + j], t_recv.at[n + rep], {"dp": peer})
    for j in range(1, replicas):
        src = (rep + j) % replicas
        wait(tot_d.at[src], t_send.at[0], t_recv.at[n + src])
    total = tot_d[0]
    for d in range(1, replicas):
        total = total + tot_d[d]
    norm = jnp.sqrt(total)
    norm_ref[...] = norm
    factor = jnp.minimum(1.0, CLIP / norm)[0:1, 0:1]
    steps = jnp.full((8, 128), step_ref[0].astype(single), single)
    fix_first = (1.0 / (1.0 - jnp.exp(steps * jnp.log(jnp.full((8, 128), beta_one, single)))))[0:1, 0:1]
    fix_second = (1.0 / (1.0 - jnp.exp(steps * jnp.log(jnp.full((8, 128), beta_two, single)))))[0:1, 0:1]
    for a in range(8):
        rows = 64

        def body(t, carry, a=a):
            at = pl.ds(pl.multiple_of(t * rows, rows), rows)
            clipped = grad[a][at, :] * factor
            f = beta_one * first[a][at, :] + (1.0 - beta_one) * clipped
            s = beta_two * second[a][at, :] + (1.0 - beta_two) * clipped * clipped
            new_first[a][at, :] = f
            new_second[a][at, :] = s
            change[a][at, :] = -learn_rate * (
                f * fix_first / (jnp.sqrt(s * fix_second) + adam_eps)
                + weight_decay * weight[a][at, :].astype(single)
            )
            return carry

        lax.fori_loop(0, grad[a].shape[0] // rows, body, 0)
    for copy in pending:
        copy.wait_send()


def update(adapters, steps, shared, pieces, weight, first, second, n, replicas, cid=2):
    groups = tuple(w.shape[0] // (ADAPTERS * RANK) for w in weight)
    vm = pl.BlockSpec(memory_space=pltpu.VMEM)
    sm = pl.BlockSpec(memory_space=pltpu.SMEM)
    f = lambda *s: jax.ShapeDtypeStruct(s, single)
    thin = shared.shape[2] // replicas
    like = tuple(f(*w.shape) for w in weight)
    dma = pltpu.SemaphoreType.DMA
    return pl.pallas_call(
        functools.partial(update_kernel, n, replicas, groups),
        out_shape=(f(8, 128),) + like * 4,
        in_specs=[sm, sm] + [vm] * 31,
        out_specs=[vm] * 33,
        scratch_shapes=[pltpu.VMEM(p.shape, brain) for p in pieces]
        + [
            pltpu.VMEM(shared.shape, brain), pltpu.VMEM((replicas, shared.shape[1], thin), brain),
            pltpu.VMEM((replicas, shared.shape[1], thin), brain), pltpu.VMEM((n, 8, 128), single),
            pltpu.VMEM((replicas, 8, 128), single), pltpu.VMEM((2, 8, 128), single),
            dma((n,)), dma((n,)), dma((replicas,)), dma((replicas,)), dma((6 * replicas,)), dma((6 * replicas,)),
            dma((n + replicas,)), dma((n + replicas,)),
        ],
        compiler_params=pltpu.CompilerParams(collective_id=cid, has_side_effects=True, vmem_limit_bytes=VMEM_ALL),
        name="update",
    )(adapters, steps, shared, *pieces, *weight, *first, *second)


def per_device(
    hidden,
    output_cotangent,
    attention_gain,
    expert_norm_gain,
    query_key_value_weight,
    output_weight,
    gate_up_weight,
    down_weight,
    token_experts,
    expert_gate_weight,
    sequence_adapter,
    optimizer_steps,
    adapter_attention_input,
    adapter_attention_output,
    adapter_projection_input,
    adapter_projection_output,
    adapter_hidden_input,
    adapter_hidden_output,
    adapter_down_input,
    adapter_down_output,
    moment_attention_input,
    moment_attention_output,
    moment_projection_input,
    moment_projection_output,
    moment_hidden_input,
    moment_hidden_output,
    moment_down_input,
    moment_down_output,
    squared_attention_input,
    squared_attention_output,
    squared_projection_input,
    squared_projection_output,
    squared_hidden_input,
    squared_hidden_output,
    squared_down_input,
    squared_down_output,
):
    n = lax.axis_size("expert")
    replicas = lax.axis_size("dp")
    rep = lax.axis_index("dp")
    me = lax.axis_index("expert")
    slot = lax.dynamic_index_in_dim(sequence_adapter, rep, 0, keepdims=False)
    toks, width = hidden.shape[1:]
    span = query_key_value_weight.shape[2]
    hidden_units = down_weight.shape[1]
    here = down_weight.shape[0]
    everyone = here * n
    top = token_experts.shape[2]
    cap = min(toks, toks * top * 5 // (4 * everyone))

    def pick(array, axis):
        return lax.dynamic_index_in_dim(array, slot, axis, keepdims=False)

    low_in = pick(adapter_attention_input, 1).reshape(3 * RANK, width)
    low_out = pick(adapter_attention_output, 1)
    proj_in = pick(adapter_projection_input, 0)
    proj_out = pick(adapter_projection_output, 0)
    hid_in = pick(adapter_hidden_input, 2).reshape(here, 2 * RANK, width)
    hid_out = pick(adapter_hidden_output, 2)
    down_in = pick(adapter_down_input, 1)
    down_out = pick(adapter_down_output, 1)

    routes = token_experts[0].T
    gates = expert_gate_weight[0].T
    dense = jnp.sum(
        jnp.where(
            routes[:, None, :] == jnp.arange(everyone, dtype=jnp.int32)[None, :, None], gates[:, None, :], 0.0
        ),
        axis=0,
    )
    gain = attention_gain[None]
    gain2 = expert_norm_gain[None]
    hid, cot = hidden[0], output_cotangent[0]
    seq, low, proj, mixed, lse, top_seq, dense_all, orank, resid, moe_seq = front(
        hid, cot, dense, gain, gain2, query_key_value_weight, low_in, low_out, output_weight, proj_in, proj_out, n
    )
    dense_here = lax.dynamic_slice_in_dim(dense_all, me * here, here, 1).reshape(n * here, toks)
    ypart, gpart, gina, gmidb, gdna, gdnb = moe(
        dense_here, moe_seq, top_seq, gate_up_weight, down_weight, hid_in, hid_out, down_in, down_out, cap, replicas
    )
    block_out, grad_hidden, gqb, goa, shared = back(
        gpart, ypart, resid, hid, cot, gain, gain2, seq, low, proj, mixed, lse, orank,
        query_key_value_weight, low_in, low_out, output_weight, proj_in, proj_out, replicas,
    )

    def flat(array):
        return array.reshape(-1, array.shape[-1])

    def part(array, index, pieces):
        piece = array.shape[-1] // pieces
        return flat(lax.dynamic_slice_in_dim(array, index * piece, piece, array.ndim - 1))

    common = rep * n + me
    weights = (
        part(adapter_attention_input, common, replicas * n), part(adapter_projection_output, common, replicas * n),
        part(adapter_attention_output, rep, replicas), part(adapter_projection_input, rep, replicas),
        part(adapter_hidden_input, rep, replicas), part(adapter_hidden_output, rep, replicas),
        part(adapter_down_input, rep, replicas), part(adapter_down_output, rep, replicas),
    )
    first = (
        moment_attention_input, moment_projection_output, moment_attention_output, moment_projection_input,
        moment_hidden_input, moment_hidden_output, moment_down_input, moment_down_output,
    )
    second = (
        squared_attention_input, squared_projection_output, squared_attention_output, squared_projection_input,
        squared_hidden_input, squared_hidden_output, squared_down_input, squared_down_output,
    )
    outs = update(
        sequence_adapter, optimizer_steps, shared, (gqb, goa, gina, gmidb, gdna, gdnb), weights,
        tuple(flat(m) for m in first), tuple(flat(s) for s in second), n, replicas,
    )
    norm = outs[0][0, :1]
    results = [block_out[None], grad_hidden[None], norm]
    for a in (0, 2, 3, 1, 4, 5, 6, 7):
        for kind in range(4):
            results.append(outs[1 + kind * 8 + a].reshape(first[a].shape))
    return tuple(results)


def solution(mesh):
    return jax.shard_map(
        per_device,
        mesh=mesh,
        in_specs=(
            P("dp", "expert", None),
            P("dp", "expert", None),
            P(),
            P(),
            P(None, None, "expert"),
            P("expert", None),
            P("expert", None, None, None),
            P("expert", None, None),
            P("dp", "expert", None),
            P("dp", "expert", None),
            P(),
            P(),
            P(),
            P(None, None, None, "expert"),
            P(None, None, "expert"),
            P(),
            P("expert", None, None, None, None),
            P("expert", None, None, None, None),
            P("expert", None, None, None),
            P("expert", None, None, None),
            P(None, None, None, ("dp", "expert")),
            P(None, None, None, ("expert", "dp")),
            P(None, None, ("expert", "dp")),
            P(None, None, ("dp", "expert")),
            P("expert", None, None, None, "dp"),
            P("expert", None, None, None, "dp"),
            P("expert", None, None, "dp"),
            P("expert", None, None, "dp"),
            P(None, None, None, ("dp", "expert")),
            P(None, None, None, ("expert", "dp")),
            P(None, None, ("expert", "dp")),
            P(None, None, ("dp", "expert")),
            P("expert", None, None, None, "dp"),
            P("expert", None, None, None, "dp"),
            P("expert", None, None, "dp"),
            P("expert", None, None, "dp"),
        ),
        out_specs=(
            P("dp", "expert", None),
            P("dp", "expert", None),
            P(),
            P(None, None, None, ("dp", "expert")),
            P(None, None, None, ("dp", "expert")),
            P(None, None, None, ("dp", "expert")),
            P(None, None, None, ("dp", "expert")),
            P(None, None, None, ("expert", "dp")),
            P(None, None, None, ("expert", "dp")),
            P(None, None, None, ("expert", "dp")),
            P(None, None, None, ("expert", "dp")),
            P(None, None, ("expert", "dp")),
            P(None, None, ("expert", "dp")),
            P(None, None, ("expert", "dp")),
            P(None, None, ("expert", "dp")),
            P(None, None, ("dp", "expert")),
            P(None, None, ("dp", "expert")),
            P(None, None, ("dp", "expert")),
            P(None, None, ("dp", "expert")),
            P("expert", None, None, None, "dp"),
            P("expert", None, None, None, "dp"),
            P("expert", None, None, None, "dp"),
            P("expert", None, None, None, "dp"),
            P("expert", None, None, None, "dp"),
            P("expert", None, None, None, "dp"),
            P("expert", None, None, None, "dp"),
            P("expert", None, None, None, "dp"),
            P("expert", None, None, "dp"),
            P("expert", None, None, "dp"),
            P("expert", None, None, "dp"),
            P("expert", None, None, "dp"),
            P("expert", None, None, "dp"),
            P("expert", None, None, "dp"),
            P("expert", None, None, "dp"),
            P("expert", None, None, "dp"),
        ),
        check_vma=False,
    )
```

```python
import functools

import jax
import jax.numpy as jnp
from jax import lax
from jax.experimental import pallas as pl
from jax.experimental.pallas import tpu as pltpu
from jax.sharding import PartitionSpec as P


single = jnp.float32
brain = jnp.bfloat16
HEAD = 128
CHUNKS = 4
GATHER_SENDS = CHUNKS * 7
SCATTER_SEMS = CHUNKS * 7
norm_eps = 1e-05
VMEM_ALL = 67043328


def dot(a, b, left=1, right=0):
    return lax.dot_general(a, b, (((left,), (right,)), ((), ())), preferred_element_type=single)


def peers():
    me = lax.axis_index("expert")
    core = me + 1 - 2 * (me % 2)
    across = me + 2 - 4 * ((me // 2) % 2)
    along = me + 4 - 8 * (me // 4)
    return me, core, across, along


def greet():
    me, core, across, along = peers()
    barrier = pltpu.get_barrier_semaphore()
    for peer in (core, across, along):
        pl.semaphore_signal(barrier, inc=1, device_id={"expert": peer})
    pl.semaphore_wait(barrier, 3)


class Mover:
    def __init__(self, send_sem, recv_sem):
        self.send_sem, self.recv_sem = send_sem, recv_sem
        self.me, self.core, self.across, self.along = peers()
        self.far = self.across + self.along - self.me
        self.pending = []
        self.waiting = []

    def go(self, src, dst, recv, peer):
        copy = pltpu.make_async_remote_copy(
            src_ref=src, dst_ref=dst, send_sem=self.send_sem.at[len(self.pending)],
            recv_sem=self.recv_sem.at[recv], device_id={"expert": peer},
        )
        copy.start()
        self.pending.append(copy)

    def later(self, *args):
        self.waiting.append(args)
        if len(self.waiting) > 1:
            self.go(*self.waiting.pop(0))

    def flush(self):
        while self.waiting:
            self.go(*self.waiting.pop(0))

    def got(self, view, recv):
        pltpu.make_async_remote_copy(
            src_ref=view, dst_ref=view, send_sem=self.send_sem.at[0], recv_sem=self.recv_sem.at[recv],
            device_id={"expert": self.core},
        ).wait_recv()

    def drain(self):
        for copy in self.pending:
            copy.wait_send()

    def beside(self, block):
        return block + 1 - 2 * (self.me % 2)


class Gather(Mover):
    def __init__(self, out, send_sem, recv_sem):
        super().__init__(send_sem, recv_sem)
        self.out = out
        self.size = out.shape[1] // CHUNKS

    def move(self, block, k, peer):
        view = self.out.at[block, pl.ds(k * self.size, self.size)]
        self.go(view, view, block * CHUNKS + k, peer)

    def arrive(self, block, k):
        self.got(self.out.at[block, pl.ds(k * self.size, self.size)], block * CHUNKS + k)

    def start(self):
        half = CHUNKS // 2
        for i in range(CHUNKS):
            self.move(self.me, i, self.across)
            self.move(self.me, (i + half) % CHUNKS, self.along)
            self.move(self.me, i, self.core)

    def relay(self, i):
        half = CHUNKS // 2
        k = (i + half) % CHUNKS
        self.arrive(self.across, i)
        if i < half:
            self.move(self.across, i, self.along)
        self.move(self.across, i, self.core)
        self.arrive(self.along, k)
        if k >= half:
            self.move(self.along, k, self.across)
        self.move(self.along, k, self.core)

    def relay_far(self, i):
        half = CHUNKS // 2
        for k in (i, i + half):
            self.arrive(self.far, k)
            self.move(self.far, k, self.core)

    def pair(self, block):
        for k in range(CHUNKS):
            self.arrive(self.beside(block), k)


class Scatter(Mover):
    def __init__(self, part, pair, half_x, half_y, from_x, from_y, send_sem, recv_sem, own=None):
        super().__init__(send_sem, recv_sem)
        self.part, self.pair, self.own = part, pair, own
        self.half_x, self.half_y, self.from_x, self.from_y = half_x, half_y, from_x, from_y
        self.order = (self.far, self.across, self.along, self.me)
        self.size = part.shape[1] // CHUNKS
        half = CHUNKS // 2
        self.hx = 4 * CHUNKS
        self.hy = self.hx + half
        self.fx = self.hy + half
        self.fy = self.fx + CHUNKS

    def rows(self, k):
        return pl.ds(k * self.size, self.size)

    def mine(self, i, r):
        return (self.part[self.order[i], r] if self.own is None else self.own[i, r]).astype(single)

    def give(self, i):
        other = self.beside(self.order[i])
        for k in range(CHUNKS):
            r = self.rows(k)
            self.go(self.part.at[other, r], self.pair.at[i, r], i * CHUNKS + k, self.core)

    def add(self, i, k, extra=None):
        r = self.rows(k)
        self.got(self.pair.at[i, r], i * CHUNKS + k)
        total = self.mine(i, r) + self.pair[i, r].astype(single)
        if extra is not None:
            ref, recv, k2 = extra
            r2 = self.rows(k2)
            self.got(ref.at[r2], recv)
            total = total + ref[r2].astype(single)
        self.pair[i, r] = total.astype(brain)

    def steps(self):
        half = CHUNKS // 2
        out = []

        def one(k):
            self.add(0, k)
            self.later(self.pair.at[0, self.rows(k)], self.half_x.at[self.rows(k)], self.hx + k, self.across)
            k2 = k + half
            self.add(0, k2)
            self.later(self.pair.at[0, self.rows(k2)], self.half_y.at[self.rows(k)], self.hy + k, self.along)

        def two(k):
            self.add(1, k)
            self.later(self.pair.at[1, self.rows(k)], self.from_x.at[self.rows(k)], self.fx + k, self.across)
            k2 = k + half
            self.add(2, k2)
            self.later(self.pair.at[2, self.rows(k2)], self.from_y.at[self.rows(k2)], self.fy + k2, self.along)

        def three(k):
            k2 = k + half
            self.add(1, k2, (self.half_y, self.hy + k, k))
            self.later(self.pair.at[1, self.rows(k2)], self.from_x.at[self.rows(k2)], self.fx + k2, self.across)
            self.add(2, k, (self.half_x, self.hx + k, k))
            self.later(self.pair.at[2, self.rows(k)], self.from_y.at[self.rows(k)], self.fy + k, self.along)

        for fn in (one, two, three):
            for k in range(half):
                out.append(functools.partial(fn, k))
        out.append(self.flush)
        return out

    def final(self, k):
        r = self.rows(k)
        self.got(self.pair.at[3, r], 3 * CHUNKS + k)
        total = self.mine(3, r) + self.pair[3, r].astype(single)
        self.got(self.from_x.at[r], self.fx + k)
        total = total + self.from_x[r].astype(single)
        self.got(self.from_y.at[r], self.fy + k)
        return total + self.from_y[r].astype(single)

    def final_order(self):
        half = CHUNKS // 2
        return [k + j * half for k in range(half) for j in range(2)]


def scatter_scratch(rows, cols):
    return [
        pltpu.VMEM((4, rows, cols), brain),
        pltpu.VMEM((rows // 2, cols), brain),
        pltpu.VMEM((rows // 2, cols), brain),
        pltpu.VMEM((rows, cols), brain),
        pltpu.VMEM((rows, cols), brain),
        pltpu.SemaphoreType.DMA((SCATTER_SEMS,)),
        pltpu.SemaphoreType.DMA((SCATTER_SEMS,)),
    ]


def gather_scratch(n):
    return [pltpu.SemaphoreType.DMA((GATHER_SENDS,)), pltpu.SemaphoreType.DMA((n * CHUNKS,))]


def rms(values, gain):
    return values * lax.rsqrt(jnp.mean(values * values, axis=-1, keepdims=True) + norm_eps) * gain


def fetch(src, dst, sem):
    copy = pltpu.make_async_copy(src, dst, sem)
    copy.start()
    return copy


def two(p, toks):
    return pl.ds(pl.multiple_of(p * 2 * toks, 2 * toks), 2 * toks)


def meet(n, replicas, with_dp):
    me, rep = lax.axis_index("expert"), lax.axis_index("dp")
    barrier = pltpu.get_barrier_semaphore()
    for j in range(1, n):
        pl.semaphore_signal(barrier, inc=1, device_id={"expert": (me + j) % n})
    if with_dp:
        for j in range(1, replicas):
            pl.semaphore_signal(barrier, inc=1, device_id={"dp": (rep + j) % replicas})
    pl.semaphore_wait(barrier, n - 1 + (replicas - 1 if with_dp else 0))


def front_kernel(
    ids_ref, hid_ref, top_ref, routes_ref, gates_ref, gain_ref, gain2_ref,
    w_hbm, a_hbm, b_hbm, wo_hbm, pa_hbm, pb_hbm,
    low_ref, lse_ref, denseall_ref, orank_ref, seq_hbm, proj_hbm, mixed_hbm, topseq_hbm, resid_hbm, moe_hbm,
    part, seq_ref, proj_ref, mixed_ref, topseq_ref, resid_ref, moe_ref,
    w_ref, a_all, b_all, wo_ref, pa_all, pb_all, a_ref, dense, load_sem, save_sem, *sems,
):
    toks, width = hid_ref.shape
    span = w_ref.shape[2]
    heads = span // HEAD
    n = seq_ref.shape[0]
    length = toks * n
    everyone = dense.shape[0]
    loads = [
        fetch(src, dst, load_sem.at[i])
        for i, (src, dst) in enumerate(
            ((w_hbm, w_ref), (a_hbm, a_all), (b_hbm, b_all), (pa_hbm, pa_all), (pb_hbm, pb_all), (wo_hbm, wo_ref))
        )
    ]
    seq_g = Gather(seq_ref, sems[0], sems[1])
    top_g = Gather(topseq_ref, sems[2], sems[3])
    moe_g = Gather(moe_ref, sems[4], sems[5])
    red = Scatter(part, *sems[6:13])
    dsend, drecv = sems[13:15]
    me = seq_g.me
    slot = ids_ref[lax.axis_index("dp")]
    saves = []

    def save(src, dst):
        saves.append(fetch(src, dst, save_sem.at[len(saves)]))

    seq_ref[me] = rms(hid_ref[...].astype(single), gain_ref[...]).astype(brain)
    topseq_ref[me] = top_ref[...]
    lanes = lax.broadcasted_iota(jnp.int32, (toks, 128), 1)
    table = jnp.zeros((toks, 128), single)
    for k in range(routes_ref.shape[1]):
        table = table + jnp.where(routes_ref[:, k : k + 1] == lanes, gates_ref[:, k : k + 1], 0.0)
    dense[...] = jnp.transpose(table)[:everyone]
    denseall_ref[me] = dense[...]
    meet(n, 1, False)
    seq_g.start()
    for j in range(1, n):
        seq_g_peer = (me + j) % n
        pltpu.make_async_remote_copy(
            src_ref=dense, dst_ref=denseall_ref.at[me], send_sem=dsend.at[j - 1], recv_sem=drecv.at[me],
            device_id={"expert": seq_g_peer},
        ).start()
    for copy in loads[:3]:
        copy.wait()
    for j in range(3):
        a_ref[16 * j : 16 * j + 16, :] = a_all[j, slot]

    def qkv(block):
        p = block // 2
        both = seq_ref[pl.ds(2 * p, 2)].reshape(2 * toks, width)
        at = two(p, toks)
        low = dot(both, a_ref[...], 1, 1).astype(brain)
        low_ref[at, :] = low
        for j in range(3):
            out = dot(both, w_ref[j]) + dot(low[:, 16 * j : 16 * j + 16], b_all[j, slot])
            proj_ref[j, at, :] = out.astype(brain)

    seq_g.pair(me)
    qkv(me)
    for i in range(CHUNKS):
        seq_g.relay(i)
    top_g.start()
    seq_g.pair(seq_g.across)
    qkv(seq_g.across)
    for i in range(CHUNKS // 2):
        seq_g.relay_far(i)
    seq_g.pair(seq_g.along)
    qkv(seq_g.along)
    seq_g.pair(seq_g.far)
    qkv(seq_g.far)
    save(seq_ref, seq_hbm)
    save(proj_ref, proj_hbm)

    scale = HEAD ** (-0.5)
    block = 256
    top_steps = [functools.partial(top_g.relay, i) for i in range(CHUNKS)]
    top_steps += [functools.partial(top_g.relay_far, i) for i in range(CHUNKS // 2)]

    for h in range(heads):
        at = slice(h * HEAD, (h + 1) * HEAD)
        for i in range(length // block):
            r = pl.ds(i * block, block)
            scores = dot(proj_ref[0, r, at], proj_ref[1, :, at], 1, 1) * scale
            peak = jnp.max(scores, axis=-1, keepdims=True)
            expo = jnp.exp(scores - peak)
            total = jnp.sum(expo, axis=-1, keepdims=True)
            probs = (expo * (1.0 / total)).astype(brain)
            mixed_ref[r, at] = dot(probs, proj_ref[2, :, at]).astype(brain)
            lse_ref[r, h : h + 1] = peak + jnp.log(total)
            if top_steps and (h * (length // block) + i) % 2 == 1:
                top_steps.pop(0)()
    for copy in loads[3:]:
        copy.wait()

    for i in range(4):
        p = red.order[i] // 2
        at = two(p, toks)
        rank = dot(mixed_ref[at, :], pa_all[slot], 1, 1).astype(brain)
        orank_ref[at, :] = rank
        out = dot(mixed_ref[at, :], wo_ref[...]) + dot(rank, pb_all[slot])
        part[pl.ds(2 * p, 2)] = out.astype(brain).reshape(2, toks, width)
        if i:
            red.give(i - 1)
    red.give(3)
    save(mixed_ref, mixed_hbm)
    while top_steps:
        top_steps.pop(0)()
    for step in red.steps():
        step()
    for block_at in (me, top_g.across, top_g.along, top_g.far):
        top_g.pair(block_at)
    save(topseq_ref, topseq_hbm)
    for k in red.final_order():
        r = red.rows(k)
        resid = hid_ref[r].astype(single) + red.final(k)
        resid_ref[r] = resid
        moe_ref[me, r] = rms(resid, gain2_ref[...]).astype(brain)
    moe_g.start()
    save(resid_ref, resid_hbm)
    for j in range(1, n):
        src = (me + j) % n
        view = denseall_ref.at[src]
        pltpu.make_async_remote_copy(
            src_ref=view, dst_ref=view, send_sem=dsend.at[0], recv_sem=drecv.at[src], device_id={"expert": src}
        ).wait_recv()
    for j in range(1, n):
        pltpu.make_async_remote_copy(
            src_ref=dense, dst_ref=denseall_ref.at[me], send_sem=dsend.at[j - 1], recv_sem=drecv.at[me],
            device_id={"expert": (me + j) % n},
        ).wait_send()
    moe_g.pair(me)

    def out_pair(block_at):
        p = block_at // 2
        save(moe_ref.at[pl.ds(2 * p, 2)], moe_hbm.at[pl.ds(2 * p, 2)])

    out_pair(me)
    for i in range(CHUNKS):
        moe_g.relay(i)
    for block_at in (moe_g.across, moe_g.along):
        moe_g.pair(block_at)
        out_pair(block_at)
    for i in range(CHUNKS // 2):
        moe_g.relay_far(i)
    moe_g.pair(moe_g.far)
    out_pair(moe_g.far)
    for mover in (seq_g, top_g, red, moe_g):
        mover.drain()
    for copy in saves:
        copy.wait()


def front(ids, hid, top, routes, gates, gain, gain2, w, a, b, wo, pa, pb, n, cid=0):
    toks, width = hid.shape
    span = w.shape[2]
    length = toks * n
    vm = pl.BlockSpec(memory_space=pltpu.VMEM)
    sm = pl.BlockSpec(memory_space=pltpu.SMEM)
    hb = pl.BlockSpec(memory_space=pl.ANY)
    f = lambda *s: jax.ShapeDtypeStruct(s, single)
    h = lambda *s: jax.ShapeDtypeStruct(s, brain)
    everyone = 2 * n
    whole = pltpu.VMEM((n, toks, width), brain)
    return pl.pallas_call(
        front_kernel,
        out_shape=(
            h(length, 48), f(length, span // HEAD), f(n, everyone, toks), h(length, 16),
            h(n, toks, width), h(3, length, span), h(length, span), h(n, toks, width), f(toks, width),
            h(n, toks, width),
        ),
        in_specs=[sm] + [vm] * 6 + [hb] * 6,
        out_specs=[vm] * 4 + [hb] * 6,
        scratch_shapes=[
            whole, whole, pltpu.VMEM((3, length, span), brain), pltpu.VMEM((length, span), brain), whole,
            pltpu.VMEM((toks, width), single), whole,
        ]
        + [pltpu.VMEM(v.shape, brain) for v in (w, a, b, wo, pa, pb)]
        + [
            pltpu.VMEM((48, width), brain), pltpu.VMEM((everyone, toks), single),
            pltpu.SemaphoreType.DMA((6,)), pltpu.SemaphoreType.DMA((10,)),
        ]
        + gather_scratch(n) + gather_scratch(n) + gather_scratch(n) + scatter_scratch(toks, width)
        + [pltpu.SemaphoreType.DMA((n,)), pltpu.SemaphoreType.DMA((n,))],
        compiler_params=pltpu.CompilerParams(collective_id=cid, has_side_effects=True, vmem_limit_bytes=VMEM_ALL),
        name="front",
    )(ids, hid, top, routes, gates, gain, gain2, w, a, b, wo, pa, pb)


TILE = 256


def moe_kernel(
    cap, replicas,
    ids_ref, denseall_ref, moe_hbm, top_hbm, gu_hbm, dn_hbm, ha_hbm, hb_hbm, da_hbm, db_hbm,
    ypart_hbm, gpart_hbm, gina_ref, gmidb_ref, gdna_ref, gdnb_ref,
    gu, dn, x_rows, g_rows, y_rows, s_rows, act, gg, uu, place, weight, irank, gdr, drank, girank,
    stage, out_stage, dense_ref, ha_ref, hb_ref, da_ref, db_ref, pick_sem, gu_sem, dn_sem, in_sem, out_sem,
):
    experts, hidden = 2, dn.shape[1]
    width = dn.shape[2]
    blocks, toks = moe_hbm.shape[0], moe_hbm.shape[1]
    rows = blocks * cap
    def bring(b, slot):
        pltpu.make_async_copy(moe_hbm.at[b], stage.at[slot, 0], in_sem.at[slot, 0]).start()
        pltpu.make_async_copy(top_hbm.at[b], stage.at[slot, 1], in_sem.at[slot, 1]).start()

    bring(0, 0)
    bring(1, 1)
    which = ids_ref[lax.axis_index("dp")]
    me = lax.axis_index("expert")
    picked = []
    for e in range(experts):
        for i in range(2):
            picked.append((ha_hbm.at[e, i, which], ha_ref.at[e, pl.ds(16 * i, 16)]))
            picked.append((hb_hbm.at[e, i, which], hb_ref.at[e, i]))
        picked.append((da_hbm.at[e, which], da_ref.at[e]))
        picked.append((db_hbm.at[e, which], db_ref.at[e]))
    picked = [pltpu.make_async_copy(s, d, pick_sem.at[i]) for i, (s, d) in enumerate(picked)]
    for copy in picked:
        copy.start()
    for e in range(experts):
        pltpu.make_async_copy(dn_hbm.at[e], dn.at[e], dn_sem.at[e]).start()
        pltpu.make_async_copy(gu_hbm.at[e], gu.at[e], gu_sem.at[e]).start()
    for b in range(blocks):
        for e in range(experts):
            dense_ref[2 * b + e : 2 * b + e + 1, :] = denseall_ref[b, pl.ds(2 * me + e, 1), :]
    dense = dense_ref[...]
    chosen = (dense > 0.0).astype(brain)
    upper = (
        lax.broadcasted_iota(jnp.int32, (toks, toks), 0)
        < lax.broadcasted_iota(jnp.int32, (toks, toks), 1)
    ).astype(single).astype(brain)
    before = dot(chosen, upper)
    place[...] = jnp.where(dense > 0.0, before, -1.0)
    slot_iota = lax.broadcasted_iota(jnp.int32, (cap, toks), 0).astype(single)

    def picks(b):
        return [(place[pl.ds(2 * b + e, 1), :] == slot_iota) for e in range(experts)]

    def gather(b, carry):
        slot = b % 2
        for j in range(2):
            pltpu.make_async_copy(moe_hbm.at[0], stage.at[slot, j], in_sem.at[slot, j]).wait()
        sel = picks(b)
        for e in range(experts):
            w = jnp.sum(jnp.where(sel[e], dense_ref[pl.ds(2 * b + e, 1), :], 0.0), axis=1, keepdims=True)
            weight[e, pl.ds(b * cap, cap), :] = w
        both = jnp.concatenate([m.astype(single).astype(brain) for m in sel], axis=0)
        at = pl.ds(b * cap, cap)
        for j, dst in ((0, x_rows), (1, g_rows)):
            got = dot(both, stage[slot, j]).astype(brain)
            dst[0, at, :] = got[:cap]
            dst[1, at, :] = got[cap:]

        @pl.when(b + 2 < blocks)
        def _():
            bring(b + 2, slot)

        return carry

    lax.fori_loop(0, blocks, gather, 0)
    for copy in picked:
        copy.wait()

    def expert(e, carry):
        pltpu.make_async_copy(dn_hbm.at[0], dn.at[e], dn_sem.at[e]).wait()
        pltpu.make_async_copy(gu_hbm.at[0], gu.at[e], gu_sem.at[e]).wait()
        w = weight[e]
        x = x_rows[e]
        irank[...] = dot(x, ha_ref[e], 1, 1).astype(brain)
        gdr[...] = (dot(g_rows[e], db_ref[e], 1, 1) * w).astype(brain)

        def tile(f, c):
            at = pl.ds(pl.multiple_of(f * TILE, TILE), TILE)
            gate = dot(x_rows[e], gu[e, 0, :, at]) + dot(irank[:, :16], hb_ref[e, 0, :, at])
            up = dot(x_rows[e], gu[e, 1, :, at]) + dot(irank[:, 16:], hb_ref[e, 1, :, at])
            ga = dot(g_rows[e], dn[e, at, :], 1, 1) * w + dot(gdr[...], da_ref[e, :, at])
            sig = jax.nn.sigmoid(gate)
            swish = gate * sig
            act[:, at] = (swish * up).astype(brain)
            gg[:, at] = (ga * up * sig * (1.0 + gate * (1.0 - sig))).astype(brain)
            uu[:, at] = (ga * swish).astype(brain)
            return c

        lax.fori_loop(0, hidden // TILE, tile, 0)
        drank[...] = dot(act[...], da_ref[e], 1, 1).astype(brain)
        girank[:, :16] = dot(gg[...], hb_ref[e, 0], 1, 1).astype(brain)
        girank[:, 16:] = dot(uu[...], hb_ref[e, 1], 1, 1).astype(brain)

        def deal(ref, row, value):
            piece = value.shape[1] // replicas
            at = pl.ds(pl.multiple_of(row, 16), value.shape[0])
            for d in range(replicas):
                ref[d, at, :] = value[:, d * piece : (d + 1) * piece].astype(brain)

        deal(gdnb_ref, e * 16, dot((drank[...].astype(single) * w).astype(brain), g_rows[e], 0, 0))
        deal(gdna_ref, e * 16, dot(gdr[...], act[...], 0, 0))
        deal(gmidb_ref, e * 32, dot(irank[:, :16], gg[...], 0, 0))
        deal(gmidb_ref, e * 32 + 16, dot(irank[:, 16:], uu[...], 0, 0))
        deal(gina_ref, e * 32, dot(girank[...], x_rows[e], 0, 0))

        def back(d, c):
            at = pl.ds(pl.multiple_of(d * TILE, TILE), TILE)
            s = dot(gg[...], gu[e, 0, at, :], 1, 1) + dot(uu[...], gu[e, 1, at, :], 1, 1)
            s = s + dot(girank[...], ha_ref[e, :, at])
            s_rows[e, :, at] = s.astype(brain)
            y = dot(act[...], dn[e, :, at]) + dot(drank[...], db_ref[e, :, at])
            y_rows[e, :, at] = (y * w).astype(brain)
            return c

        lax.fori_loop(0, width // TILE, back, 0)
        return carry

    lax.fori_loop(0, experts, expert, 0)

    def combine(b, carry):
        slot = b % 2

        @pl.when(b >= 2)
        def _():
            for j, dst in ((0, ypart_hbm), (1, gpart_hbm)):
                pltpu.make_async_copy(out_stage.at[slot, j], dst.at[0], out_sem.at[slot, j]).wait()

        sel = picks(b)
        both = jnp.concatenate([m.astype(single).astype(brain) for m in sel], axis=0)
        at = pl.ds(b * cap, cap)
        for j, (src, dst) in enumerate(((y_rows, ypart_hbm), (s_rows, gpart_hbm))):
            pair = jnp.concatenate([src[0, at, :], src[1, at, :]], axis=0)
            out_stage[slot, j] = dot(both, pair, 0, 0).astype(brain)
            pltpu.make_async_copy(out_stage.at[slot, j], dst.at[b], out_sem.at[slot, j]).start()
        return carry

    lax.fori_loop(0, blocks, combine, 0)
    for slot in range(2):
        for j, dst in ((0, ypart_hbm), (1, gpart_hbm)):
            pltpu.make_async_copy(out_stage.at[slot, j], dst.at[0], out_sem.at[slot, j]).wait()


def moe(ids, dense, moe_seq, top_seq, gu, dn, ha, hb, da, db, cap, replicas):
    blocks, toks, width = moe_seq.shape
    experts, hidden = dn.shape[0], dn.shape[1]
    rank = da.shape[2]
    rows = blocks * cap
    vm = pl.BlockSpec(memory_space=pltpu.VMEM)
    sm = pl.BlockSpec(memory_space=pltpu.SMEM)
    any_ = pl.BlockSpec(memory_space=pl.ANY)
    f = lambda *s: jax.ShapeDtypeStruct(s, single)
    h = lambda *s: jax.ShapeDtypeStruct(s, brain)
    return pl.pallas_call(
        functools.partial(moe_kernel, cap, replicas),
        out_shape=(
            h(blocks, toks, width), h(blocks, toks, width),
            h(replicas, experts * 2 * rank, width // replicas), h(replicas, experts * 2 * rank, hidden // replicas),
            h(replicas, experts * rank, hidden // replicas), h(replicas, experts * rank, width // replicas),
        ),
        in_specs=[sm, vm] + [any_] * 8,
        out_specs=[any_, any_, vm, vm, vm, vm],
        scratch_shapes=[
            pltpu.VMEM((experts, 2, width, hidden), brain),
            pltpu.VMEM((experts, hidden, width), brain),
            pltpu.VMEM((experts, rows, width), brain),
            pltpu.VMEM((experts, rows, width), brain),
            pltpu.VMEM((experts, rows, width), brain),
            pltpu.VMEM((experts, rows, width), brain),
            pltpu.VMEM((rows, hidden), brain),
            pltpu.VMEM((rows, hidden), brain),
            pltpu.VMEM((rows, hidden), brain),
            pltpu.VMEM((blocks * experts, toks), single),
            pltpu.VMEM((experts, rows, 1), single),
            pltpu.VMEM((rows, 2 * rank), brain),
            pltpu.VMEM((rows, rank), brain),
            pltpu.VMEM((rows, rank), brain),
            pltpu.VMEM((rows, 2 * rank), brain),
            pltpu.VMEM((2, 2, toks, width), brain),
            pltpu.VMEM((2, 2, toks, width), brain),
            pltpu.VMEM((blocks * experts, toks), single),
            pltpu.VMEM((experts, 2 * rank, width), brain),
            pltpu.VMEM((experts, 2, rank, hidden), brain),
            pltpu.VMEM((experts, rank, hidden), brain),
            pltpu.VMEM((experts, rank, width), brain),
            pltpu.SemaphoreType.DMA((6 * experts,)),
            pltpu.SemaphoreType.DMA((experts,)),
            pltpu.SemaphoreType.DMA((experts,)),
            pltpu.SemaphoreType.DMA((2, 2)),
            pltpu.SemaphoreType.DMA((2, 2)),
        ],
        compiler_params=pltpu.CompilerParams(vmem_limit_bytes=67043328),
        name="moe",
    )(ids, dense, moe_seq, top_seq, gu, dn, ha, hb, da, db)


ADAPTERS = 8
RANK = 16
CLIP = 256.0
beta_one = 0.9
beta_two = 0.95
learn_rate = 0.02
weight_decay = 0.1
adam_eps = 1e-08


def norm_back(values, gain, grad):
    inverse = lax.rsqrt(jnp.mean(values * values, axis=-1, keepdims=True) + norm_eps)
    scaled = grad * gain
    return inverse * scaled - values * (
        inverse * inverse * inverse * jnp.mean(scaled * values, axis=-1, keepdims=True)
    )


def back_kernel(
    replicas,
    ids_ref, hid_ref, top_ref, gain_ref, gain2_ref, low_ref, lse_ref, orank_ref,
    resid_hbm, seq_hbm, proj_hbm, mixed_hbm, gpart_hbm, ypart_hbm,
    w_hbm, a_hbm, b_hbm, wo_hbm, pa_hbm, pb_hbm, gina_hbm, gmidb_hbm, gdna_hbm, gdnb_hbm,
    out_ref, gh_ref, norm_ref, shared_got, got_qb, got_oa, got_ina, got_midb, got_dna, got_dnb,
    resid_ref, seq_ref, proj_ref, mixed_ref, own_g, own_y,
    w_ref, a_all, b_all, wo_ref, pa_all, pb_all, a_ref,
    bf, part, gres, gmix, grank, gproj, glow, gk, gv,
    gqb_ref, goa_ref, shared_ref, shared_in, shared_mid, tot_e, tot_d, mine, load_sem, own_sem,
    sh_send, sh_recv, mid_send, mid_recv, p_send, p_recv, t_send, t_recv, *sems,
):
    toks, width = hid_ref.shape
    span = w_ref.shape[2]
    heads = span // HEAD
    n = seq_ref.shape[0]
    length = toks * n
    red = Scatter(gpart_hbm, *sems[0:7], own=own_g)
    redy = Scatter(ypart_hbm, *sems[7:14], own=own_y)
    redn = Scatter(part, *sems[14:21])
    bf_g = Gather(bf, *sems[21:23])
    me = red.me
    rep = lax.axis_index("dp")
    slot = ids_ref[rep]
    owns = [fetch(gpart_hbm.at[red.order[i]], own_g.at[i], own_sem.at[i]) for i in range(4)]
    loads = {}
    for i, (name, src, dst) in enumerate(
        (
            ("resid", resid_hbm, resid_ref), ("wo", wo_hbm, wo_ref), ("pb", pb_hbm, pb_all), ("pa", pa_hbm, pa_all),
            ("mixed", mixed_hbm, mixed_ref), ("proj", proj_hbm, proj_ref), ("b", b_hbm, b_all), ("a", a_hbm, a_all),
            ("w", w_hbm, w_ref), ("seq", seq_hbm, seq_ref), ("ina", gina_hbm.at[rep], got_ina.at[rep]),
            ("midb", gmidb_hbm.at[rep], got_midb.at[rep]), ("dna", gdna_hbm.at[rep], got_dna.at[rep]),
            ("dnb", gdnb_hbm.at[rep], got_dnb.at[rep]),
        )
    ):
        loads[name] = fetch(src, dst, load_sem.at[i])

    def need(*names):
        for name in names:
            loads.pop(name).wait()

    meet(n, replicas, True)
    for i in range(4):
        red.give(i)
    for i in range(4):
        owns.append(fetch(ypart_hbm.at[red.order[i]], own_y.at[i], own_sem.at[4 + i]))
    pending = []

    def go(src, dst, send_sem, recv_sem, where):
        copy = pltpu.make_async_remote_copy(
            src_ref=src, dst_ref=dst, send_sem=send_sem, recv_sem=recv_sem, device_id=where
        )
        copy.start()
        pending.append(copy)

    def wait(view, recv_sem):
        pltpu.make_async_remote_copy(
            src_ref=view, dst_ref=view, send_sem=t_send.at[0], recv_sem=recv_sem, device_id={"expert": (me + 1) % n}
        ).wait_recv()

    got = (got_qb, got_oa, got_ina, got_midb, got_dna, got_dnb)

    def swap(i, source):
        for j in range(1, replicas):
            peer = (rep + j) % replicas
            go(
                source.at[peer], got[i].at[rep], p_send.at[i * replicas + j], p_recv.at[i * replicas + rep],
                {"dp": peer},
            )

    def swapped(i):
        for j in range(1, replicas):
            src = (rep + j) % replicas
            wait(got[i].at[src], p_recv.at[i * replicas + src])

    for copy in owns[:4]:
        copy.wait()
    steps = red.steps()
    for step in steps[:4]:
        step()
    for i, source in enumerate((gina_hbm, gmidb_hbm, gdna_hbm, gdnb_hbm)):
        swap(i + 2, source)
    for i in range(4):
        redy.give(i)
    for step in steps[4:]:
        step()
    need("resid")
    for k in red.final_order():
        r = red.rows(k)
        grad = top_ref[r].astype(single) + norm_back(resid_ref[r], gain2_ref[...], red.final(k))
        gres[r] = grad
        bf[me, r] = grad.astype(brain)
    bf_g.start()
    need("wo", "pb", "pa", "mixed")

    def mixed_grad(block):
        p = block // 2
        both = bf[pl.ds(2 * p, 2)].reshape(2 * toks, width)
        at = two(p, toks)
        rank = dot(both, pb_all[slot], 1, 1).astype(brain)
        grank[at, :] = rank
        gmix[at, :] = (dot(both, wo_ref[...], 1, 1) + dot(rank, pa_all[slot])).astype(brain)

    bf_g.pair(me)
    mixed_grad(me)
    for i in range(CHUNKS):
        bf_g.relay(i)
    bf_g.pair(bf_g.across)
    mixed_grad(bf_g.across)
    for i in range(CHUNKS // 2):
        bf_g.relay_far(i)
    bf_g.pair(bf_g.along)
    mixed_grad(bf_g.along)
    bf_g.pair(bf_g.far)
    mixed_grad(bf_g.far)

    piece = span // replicas
    goa = dot(grank[...], mixed_ref[...], 0, 0)
    for d in range(replicas):
        goa_ref[d] = goa[:, d * piece : (d + 1) * piece].astype(brain)
    got_oa[rep] = goa_ref[rep]
    swap(1, goa_ref)

    for copy in owns[4:]:
        copy.wait()
    need("proj")
    steps = redy.steps()
    scale = HEAD ** (-0.5)
    block = 256
    for h in range(heads):
        at = slice(h * HEAD, (h + 1) * HEAD)
        for i in range(length // block):
            r = pl.ds(i * block, block)
            q, do = proj_ref[0, r, at], gmix[r, at]
            delta = jnp.sum(do.astype(single) * mixed_ref[r, at].astype(single), axis=-1, keepdims=True)
            probs = jnp.exp(dot(q, proj_ref[1, :, at], 1, 1) * scale - lse_ref[r, h : h + 1])
            gp = dot(do, proj_ref[2, :, at], 1, 1)
            gs = (probs * (gp - delta)).astype(brain)
            gproj[0, r, at] = (dot(gs, proj_ref[1, :, at]) * scale).astype(brain)
            dk = dot(gs, q, 0, 0)
            dv = dot(probs.astype(brain), do, 0, 0)
            if i == 0:
                gk[...] = dk
                gv[...] = dv
            elif i < length // block - 1:
                gk[...] += dk
                gv[...] += dv
            else:
                gproj[1, :, at] = ((gk[...] + dk) * scale).astype(brain)
                gproj[2, :, at] = (gv[...] + dv).astype(brain)
            if steps:
                steps.pop(0)()
    while steps:
        steps.pop(0)()

    need("a", "b", "w")
    for j in range(3):
        a_ref[16 * j : 16 * j + 16, :] = a_all[j, slot]
    for i in range(4):
        p = redn.order[i] // 2
        at = two(p, toks)
        for j in range(3):
            glow[at, 16 * j : 16 * j + 16] = dot(gproj[j, at, :], b_all[j, slot], 1, 1).astype(brain)
        out = dot(glow[at, :], a_ref[...])
        for j in range(3):
            out = out + dot(gproj[j, at, :], w_ref[j], 1, 1)
        part[pl.ds(2 * p, 2)] = out.astype(brain).reshape(2, toks, width)
        if i:
            redn.give(i - 1)
    redn.give(3)

    thin = width // (n * replicas)

    def share(row, value, base):
        for c in range(value.shape[1] // thin):
            d, e = (base + c) // n, (base + c) % n
            shared_ref[e, row : row + value.shape[0], d * thin : (d + 1) * thin] = value[
                :, c * thin : (c + 1) * thin
            ].astype(brain)

    nsteps = redn.steps()

    def advance():
        if nsteps:
            nsteps.pop(0)()

    for j in range(3):
        gqb = dot(low_ref[:, 16 * j : 16 * j + 16], gproj[j], 0, 0)
        for d in range(replicas):
            gqb_ref[d, 16 * j : 16 * j + 16, :] = gqb[:, d * piece : (d + 1) * piece].astype(brain)
    advance()
    got_qb[rep] = gqb_ref[rep]
    swap(0, gqb_ref)
    need("seq")
    cols = 512
    for c in range(width // cols):
        s = slice(c * cols, (c + 1) * cols)
        share(0, dot(glow[...], seq_ref[:, :, s].reshape(length, cols), 0, 0), c * cols // thin)
        share(48, dot(orank_ref[...], bf[:, :, s].reshape(length, cols), 0, 0), c * cols // thin)
        advance()
    shared_in[me] = shared_ref[me]
    for j in range(1, n):
        peer = (me + j) % n
        go(shared_ref.at[peer], shared_in.at[me], sh_send.at[j - 1], sh_recv.at[me], {"expert": peer})
    while nsteps:
        advance()

    def squares(i, source):
        rows = source.shape[1] // RANK

        def body(t, acc):
            at = pl.ds(pl.multiple_of(t // ADAPTERS * RANK, RANK), RANK)
            value = jnp.zeros((RANK, source.shape[2]), single)
            for s in range(replicas):
                value = value + source[s, at, :].astype(single) * jnp.where(ids_ref[s] == t % ADAPTERS, 1.0, 0.0)
            return acc + value * value

        return jnp.sum(
            lax.fori_loop(0, rows * ADAPTERS, body, jnp.zeros((RANK, source.shape[2]), single))
        )

    need("ina", "midb", "dna", "dnb")
    total = jnp.zeros((), single)
    for i in range(2, 6):
        swapped(i)
        total = total + squares(i, got[i])
    for j in range(1, n):
        src = (me + j) % n
        wait(shared_in.at[src], sh_recv.at[src])
    summed = shared_in[0].astype(single)
    for e in range(1, n):
        summed = summed + shared_in[e].astype(single)
    for d in range(replicas):
        shared_mid[d] = summed[:, d * thin : (d + 1) * thin].astype(brain)
    shared_got[rep] = shared_mid[rep]
    for j in range(1, replicas):
        peer = (rep + j) % replicas
        go(shared_mid.at[peer], shared_got.at[rep], mid_send.at[j], mid_recv.at[rep], {"dp": peer})
    for k in redy.final_order():
        r = redy.rows(k)
        out_ref[r] = (resid_ref[r] + redy.final(k)).astype(brain)
    for i in range(2):
        swapped(i)
        total = total + squares(i, got[i])
    for j in range(1, replicas):
        src = (rep + j) % replicas
        wait(shared_got.at[src], mid_recv.at[src])
    total = total + squares(0, shared_got)

    mine[0] = jnp.full(mine.shape[1:], total, single)
    tot_e[me] = mine[0]
    for j in range(1, n):
        go(mine.at[0], tot_e.at[me], t_send.at[j], t_recv.at[me], {"expert": (me + j) % n})
    for j in range(1, n):
        src = (me + j) % n
        wait(tot_e.at[src], t_recv.at[src])
    total = tot_e[0]
    for e in range(1, n):
        total = total + tot_e[e]
    mine[1] = total
    tot_d[rep] = mine[1]
    for j in range(1, replicas):
        go(mine.at[1], tot_d.at[rep], t_send.at[n + j], t_recv.at[n + rep], {"dp": (rep + j) % replicas})
    for k in redn.final_order():
        r = redn.rows(k)
        gh_ref[r] = gres[r] + norm_back(hid_ref[r].astype(single), gain_ref[...], redn.final(k))
    for j in range(1, replicas):
        src = (rep + j) % replicas
        wait(tot_d.at[src], t_recv.at[n + src])
    total = tot_d[0]
    for d in range(1, replicas):
        total = total + tot_d[d]
    norm_ref[...] = jnp.sqrt(total)
    for mover in (red, redy, redn, bf_g):
        mover.drain()
    for copy in pending:
        copy.wait_send()


def back(
    ids, hid, top, gain, gain2, low, lse, orank, resid, seq, proj, mixed, gpart, ypart, w, a, b, wo, pa, pb,
    pieces, replicas, cid=1,
):
    n, toks, width = seq.shape
    span = w.shape[2]
    length = toks * n
    vm = pl.BlockSpec(memory_space=pltpu.VMEM)
    sm = pl.BlockSpec(memory_space=pltpu.SMEM)
    hb = pl.BlockSpec(memory_space=pl.ANY)
    f = lambda *s: jax.ShapeDtypeStruct(s, single)
    h = lambda *s: jax.ShapeDtypeStruct(s, brain)
    bv = lambda *s: pltpu.VMEM(s, brain)
    fv = lambda *s: pltpu.VMEM(s, single)
    dma = pltpu.SemaphoreType.DMA
    thin = width // (n * replicas)
    piece = span // replicas
    return pl.pallas_call(
        functools.partial(back_kernel, replicas),
        out_shape=(
            h(toks, width), f(toks, width), f(8, 128), h(replicas, 64, thin), h(replicas, 48, piece),
            h(replicas, 16, piece),
        ) + tuple(h(*p.shape) for p in pieces),
        in_specs=[sm] + [vm] * 7 + [hb] * 16,
        out_specs=[vm] * 10,
        scratch_shapes=[
            fv(toks, width), bv(n, toks, width), bv(3, length, span), bv(length, span), bv(4, toks, width),
            bv(4, toks, width),
        ]
        + [pltpu.VMEM(v.shape, brain) for v in (w, a, b, wo, pa, pb)]
        + [
            bv(48, width), bv(n, toks, width), bv(n, toks, width), fv(toks, width), bv(length, span), bv(length, 16),
            bv(3, length, span), bv(length, 48), fv(length, HEAD), fv(length, HEAD),
            bv(replicas, 48, piece), bv(replicas, 16, piece), bv(n, 64, replicas * thin), bv(n, 64, replicas * thin),
            bv(replicas, 64, thin), fv(n, 8, 128), fv(replicas, 8, 128), fv(2, 8, 128), dma((14,)), dma((8,)),
            dma((n,)), dma((n,)), dma((replicas,)), dma((replicas,)), dma((6 * replicas,)), dma((6 * replicas,)),
            dma((n + replicas,)), dma((n + replicas,)),
        ]
        + scatter_scratch(toks, width) * 3 + gather_scratch(n),
        compiler_params=pltpu.CompilerParams(collective_id=cid, has_side_effects=True, vmem_limit_bytes=VMEM_ALL),
        name="back",
    )(ids, hid, top, gain, gain2, low, lse, orank, resid, seq, proj, mixed, gpart, ypart, w, a, b, wo, pa, pb, *pieces)


def adam_kernel(n, replicas, groups, spans, adapter_ref, step_ref, norm_in, out_in, gh_in, *refs):
    got, refs = refs[:7], refs[7:]
    weight_hbm, first_hbm, second_hbm, refs = refs[:8], refs[8:16], refs[16:24], refs[24:]
    out_hbm, gh_hbm, norm_ref, result, refs = refs[0], refs[1], refs[2], refs[3:35], refs[35:]
    weight, first, second, kept, refs = refs[:8], refs[8:16], refs[16:24], refs[24:56], refs[56:]
    load_sem, save_sem = refs
    me, rep = lax.axis_index("expert"), lax.axis_index("dp")
    common = rep * n + me
    loads, saves = [], []
    for a in range(8):
        size, pieces = spans[a]
        index = common if pieces == n * replicas else rep
        start = index * size // weight[a].shape[1] * weight[a].shape[1]
        view = weight_hbm[a].at[:, pl.ds(pl.multiple_of(start, 128), weight[a].shape[1])]
        loads.append(
            [
                fetch(src, dst, load_sem.at[3 * a + k])
                for k, (src, dst) in enumerate(((view, weight[a]), (first_hbm[a], first[a]), (second_hbm[a], second[a])))
            ]
        )
    saves.append(fetch(out_in, out_hbm, save_sem.at[32]))
    saves.append(fetch(gh_in, gh_hbm, save_sem.at[33]))
    norm_ref[...] = norm_in[...]
    factor = jnp.minimum(1.0, CLIP / norm_in[...])[0:1, 0:1]
    steps = jnp.full((8, 128), step_ref[0].astype(single), single)
    fix_first = (1.0 / (1.0 - jnp.exp(steps * jnp.log(jnp.full((8, 128), beta_one, single)))))[0:1, 0:1]
    fix_second = (1.0 / (1.0 - jnp.exp(steps * jnp.log(jnp.full((8, 128), beta_two, single)))))[0:1, 0:1]
    for a in (4, 7, 5, 6, 0, 2, 1, 3):
        for copy in loads[a]:
            copy.wait()
        source = got[max(a - 1, 0)]
        base = groups[0] if a == 1 else 0
        size, pieces = spans[a]
        window = weight[a].shape[1]
        index = common if pieces == n * replicas else rep

        def body(t, carry, a=a, source=source, base=base, size=size, window=window, index=index):
            at = pl.ds(pl.multiple_of(t * RANK, RANK), RANK)
            rows = pl.ds(pl.multiple_of((base + t // ADAPTERS) * RANK, RANK), RANK)
            grad = jnp.zeros((RANK, size), single)
            for s in range(replicas):
                keep = jnp.where(adapter_ref[s] == t % ADAPTERS, 1.0, 0.0)
                grad = grad + source[s, rows, :].astype(single) * keep
            held = weight[a][at, :].astype(single)
            w = held[:, :size]
            for c in range(1, window // size):
                w = jnp.where(index % (window // size) == c, held[:, c * size : (c + 1) * size], w)
            clipped = grad * factor
            f = beta_one * first[a][at, :] + (1.0 - beta_one) * clipped
            s = beta_two * second[a][at, :] + (1.0 - beta_two) * clipped * clipped
            kept[4 * a][at, :] = grad
            kept[4 * a + 1][at, :] = f
            kept[4 * a + 2][at, :] = s
            kept[4 * a + 3][at, :] = -learn_rate * (
                f * fix_first / (jnp.sqrt(s * fix_second) + adam_eps) + weight_decay * w
            )
            return carry

        lax.fori_loop(0, groups[a] * ADAPTERS, body, 0)
        for k in range(4):
            saves.append(fetch(kept[4 * a + k], result[4 * a + k], save_sem.at[4 * a + k]))
    for copy in saves:
        copy.wait()


def adam(adapters, steps, norm, block_out, gh, got, weight, pieces, first, second, n, replicas):
    spans = tuple((f.shape[1], p) for f, p in zip(first, pieces))
    groups = tuple(f.shape[0] // (ADAPTERS * RANK) for f in first)
    vm = pl.BlockSpec(memory_space=pltpu.VMEM)
    sm = pl.BlockSpec(memory_space=pltpu.SMEM)
    hb = pl.BlockSpec(memory_space=pl.ANY)
    f = lambda s: jax.ShapeDtypeStruct(s, single)
    dma = pltpu.SemaphoreType.DMA
    shapes = [t.shape for t in first]
    return pl.pallas_call(
        functools.partial(adam_kernel, n, replicas, groups, spans),
        out_shape=(jax.ShapeDtypeStruct(block_out.shape, brain), f(gh.shape), f((8, 128)))
        + tuple(f(s) for s in shapes for _ in range(4)),
        in_specs=[sm, sm, vm, vm, vm] + [vm] * 7 + [hb] * 24,
        out_specs=[hb, hb, vm] + [hb] * 32,
        scratch_shapes=[pltpu.VMEM((s[0], max(s[1], 128)), brain) for s in shapes]
        + [pltpu.VMEM(s, single) for s in shapes] * 2
        + [pltpu.VMEM(s, single) for s in shapes for _ in range(4)]
        + [dma((24,)), dma((34,))],
        compiler_params=pltpu.CompilerParams(vmem_limit_bytes=VMEM_ALL),
        name="adam",
    )(adapters, steps, norm, block_out, gh, *got, *weight, *first, *second)


def per_device(
    hidden,
    output_cotangent,
    attention_gain,
    expert_norm_gain,
    query_key_value_weight,
    output_weight,
    gate_up_weight,
    down_weight,
    token_experts,
    expert_gate_weight,
    sequence_adapter,
    optimizer_steps,
    adapter_attention_input,
    adapter_attention_output,
    adapter_projection_input,
    adapter_projection_output,
    adapter_hidden_input,
    adapter_hidden_output,
    adapter_down_input,
    adapter_down_output,
    moment_attention_input,
    moment_attention_output,
    moment_projection_input,
    moment_projection_output,
    moment_hidden_input,
    moment_hidden_output,
    moment_down_input,
    moment_down_output,
    squared_attention_input,
    squared_attention_output,
    squared_projection_input,
    squared_projection_output,
    squared_hidden_input,
    squared_hidden_output,
    squared_down_input,
    squared_down_output,
):
    n = lax.axis_size("expert")
    replicas = lax.axis_size("dp")
    toks, width = hidden.shape[1:]
    here = down_weight.shape[0]
    cap = min(toks, toks * token_experts.shape[2] * 5 // (4 * here * n))
    gain = attention_gain[None]
    gain2 = expert_norm_gain[None]
    hid, cot = hidden[0], output_cotangent[0]
    low, lse, dense_all, orank, seq, proj, mixed, top_seq, resid, moe_seq = front(
        sequence_adapter, hid, cot, token_experts[0], expert_gate_weight[0], gain, gain2, query_key_value_weight,
        adapter_attention_input, adapter_attention_output, output_weight, adapter_projection_input,
        adapter_projection_output, n,
    )
    ypart, gpart, *pieces = moe(
        sequence_adapter, dense_all, moe_seq, top_seq, gate_up_weight, down_weight, adapter_hidden_input,
        adapter_hidden_output, adapter_down_input, adapter_down_output, cap, replicas,
    )
    block_out, grad_hidden, norm, *got = back(
        sequence_adapter, hid, cot, gain, gain2, low, lse, orank, resid, seq, proj, mixed, gpart, ypart,
        query_key_value_weight, adapter_attention_input, adapter_attention_output, output_weight,
        adapter_projection_input, adapter_projection_output, tuple(pieces), replicas,
    )

    def flat(array):
        return array.reshape(-1, array.shape[-1])

    weights = (
        adapter_attention_input, adapter_projection_output, adapter_attention_output, adapter_projection_input,
        adapter_hidden_input, adapter_hidden_output, adapter_down_input, adapter_down_output,
    )
    first = (
        moment_attention_input, moment_projection_output, moment_attention_output, moment_projection_input,
        moment_hidden_input, moment_hidden_output, moment_down_input, moment_down_output,
    )
    second = (
        squared_attention_input, squared_projection_output, squared_attention_output, squared_projection_input,
        squared_hidden_input, squared_hidden_output, squared_down_input, squared_down_output,
    )
    outs = adam(
        sequence_adapter, optimizer_steps, norm, block_out, grad_hidden, got, tuple(flat(w) for w in weights),
        (n * replicas,) * 2 + (replicas,) * 6, tuple(flat(m) for m in first), tuple(flat(s) for s in second),
        n, replicas,
    )
    results = [outs[0][None], outs[1][None], outs[2][0, :1]]
    for a in (0, 2, 3, 1, 4, 5, 6, 7):
        for kind in range(4):
            results.append(outs[3 + 4 * a + kind].reshape(first[a].shape))
    return tuple(results)


def solution(mesh):
    return jax.shard_map(
        per_device,
        mesh=mesh,
        in_specs=(
            P("dp", "expert", None),
            P("dp", "expert", None),
            P(),
            P(),
            P(None, None, "expert"),
            P("expert", None),
            P("expert", None, None, None),
            P("expert", None, None),
            P("dp", "expert", None),
            P("dp", "expert", None),
            P(),
            P(),
            P(),
            P(None, None, None, "expert"),
            P(None, None, "expert"),
            P(),
            P("expert", None, None, None, None),
            P("expert", None, None, None, None),
            P("expert", None, None, None),
            P("expert", None, None, None),
            P(None, None, None, ("dp", "expert")),
            P(None, None, None, ("expert", "dp")),
            P(None, None, ("expert", "dp")),
            P(None, None, ("dp", "expert")),
            P("expert", None, None, None, "dp"),
            P("expert", None, None, None, "dp"),
            P("expert", None, None, "dp"),
            P("expert", None, None, "dp"),
            P(None, None, None, ("dp", "expert")),
            P(None, None, None, ("expert", "dp")),
            P(None, None, ("expert", "dp")),
            P(None, None, ("dp", "expert")),
            P("expert", None, None, None, "dp"),
            P("expert", None, None, None, "dp"),
            P("expert", None, None, "dp"),
            P("expert", None, None, "dp"),
        ),
        out_specs=(
            P("dp", "expert", None),
            P("dp", "expert", None),
            P(),
            P(None, None, None, ("dp", "expert")),
            P(None, None, None, ("dp", "expert")),
            P(None, None, None, ("dp", "expert")),
            P(None, None, None, ("dp", "expert")),
            P(None, None, None, ("expert", "dp")),
            P(None, None, None, ("expert", "dp")),
            P(None, None, None, ("expert", "dp")),
            P(None, None, None, ("expert", "dp")),
            P(None, None, ("expert", "dp")),
            P(None, None, ("expert", "dp")),
            P(None, None, ("expert", "dp")),
            P(None, None, ("expert", "dp")),
            P(None, None, ("dp", "expert")),
            P(None, None, ("dp", "expert")),
            P(None, None, ("dp", "expert")),
            P(None, None, ("dp", "expert")),
            P("expert", None, None, None, "dp"),
            P("expert", None, None, None, "dp"),
            P("expert", None, None, None, "dp"),
            P("expert", None, None, None, "dp"),
            P("expert", None, None, None, "dp"),
            P("expert", None, None, None, "dp"),
            P("expert", None, None, None, "dp"),
            P("expert", None, None, None, "dp"),
            P("expert", None, None, "dp"),
            P("expert", None, None, "dp"),
            P("expert", None, None, "dp"),
            P("expert", None, None, "dp"),
            P("expert", None, None, "dp"),
            P("expert", None, None, "dp"),
            P("expert", None, None, "dp"),
            P("expert", None, None, "dp"),
        ),
        check_vma=False,
    )
```

```python
import functools

import jax
import jax.numpy as jnp
from jax import lax
from jax.experimental import pallas as pl
from jax.experimental.pallas import tpu as pltpu
from jax.sharding import PartitionSpec as P


single = jnp.float32
brain = jnp.bfloat16
HEAD = 128
TILE = 256
CHUNKS = 4
ORDER = [k + j * (CHUNKS // 2) for k in range(CHUNKS // 2) for j in range(2)]
GATHER_SENDS = CHUNKS * 7
SCATTER_SEMS = CHUNKS * 7
norm_eps = 1e-05
VMEM_ALL = 67043328


def dot(a, b, left=1, right=0):
    return lax.dot_general(a, b, (((left,), (right,)), ((), ())), preferred_element_type=single)


def peers():
    me = lax.axis_index("expert")
    core = me + 1 - 2 * (me % 2)
    across = me + 2 - 4 * ((me // 2) % 2)
    along = me + 4 - 8 * (me // 4)
    return me, core, across, along


def greet():
    me, core, across, along = peers()
    barrier = pltpu.get_barrier_semaphore()
    for peer in (core, across, along):
        pl.semaphore_signal(barrier, inc=1, device_id={"expert": peer})
    pl.semaphore_wait(barrier, 3)


class Mover:
    def __init__(self, send_sem, recv_sem):
        self.send_sem, self.recv_sem = send_sem, recv_sem
        self.me, self.core, self.across, self.along = peers()
        self.far = self.across + self.along - self.me
        self.count = 0
        self.waiting = []

    def go(self, src, dst, recv, peer):
        pltpu.make_async_remote_copy(
            src_ref=src, dst_ref=dst, send_sem=self.send_sem.at[self.count],
            recv_sem=self.recv_sem.at[recv], device_id={"expert": peer},
        ).start()
        self.count += 1

    def later(self, args):
        self.waiting.append(args)
        if len(self.waiting) > 1:
            self.waiting.pop(0)()

    def flush(self):
        while self.waiting:
            self.waiting.pop(0)()

    def got(self, view, recv):
        pltpu.make_async_remote_copy(
            src_ref=view, dst_ref=view, send_sem=self.send_sem.at[0], recv_sem=self.recv_sem.at[recv],
            device_id={"expert": self.core},
        ).wait_recv()

    def drain(self):
        view = self.sample()
        for i in range(self.count):
            pltpu.make_async_remote_copy(
                src_ref=view, dst_ref=view, send_sem=self.send_sem.at[i], recv_sem=self.recv_sem.at[0],
                device_id={"expert": self.core},
            ).wait_send()

    def beside(self, block):
        return block + 1 - 2 * (self.me % 2)


class Gather(Mover):
    def __init__(self, out, send_sem, recv_sem):
        super().__init__(send_sem, recv_sem)
        self.out = out
        self.size = out.shape[1] // CHUNKS

    def sample(self):
        return self.out.at[0, pl.ds(0, self.size)]

    def move(self, block, k, peer):
        view = self.out.at[block, pl.ds(k * self.size, self.size)]
        self.go(view, view, block * CHUNKS + k, peer)

    def arrive(self, block, k):
        self.got(self.out.at[block, pl.ds(k * self.size, self.size)], block * CHUNKS + k)

    def start_own(self, k):
        for peer in (self.across, self.along, self.core):
            self.move(self.me, k, peer)

    def start(self):
        for k in ORDER:
            self.start_own(k)

    def relay(self, i):
        k = ORDER[i]
        first_half = k < CHUNKS // 2
        self.arrive(self.across, k)
        if first_half:
            self.move(self.across, k, self.along)
        self.move(self.across, k, self.core)
        self.arrive(self.along, k)
        if not first_half:
            self.move(self.along, k, self.across)
        self.move(self.along, k, self.core)

    def relay_far(self, i):
        half = CHUNKS // 2
        for k in (i, i + half):
            self.arrive(self.far, k)
            self.move(self.far, k, self.core)

    def pair(self, block):
        for k in range(CHUNKS):
            self.arrive(self.beside(block), k)


class Scatter(Mover):
    def __init__(self, part, pair, half_x, half_y, from_x, from_y, send_sem, recv_sem, own=None):
        super().__init__(send_sem, recv_sem)
        self.part, self.pair, self.own = part, pair, own
        self.half_x, self.half_y, self.from_x, self.from_y = half_x, half_y, from_x, from_y
        self.order = (self.far, self.across, self.along, self.me)
        self.toks = pair.shape[1]
        self.size = self.toks // CHUNKS
        half = CHUNKS // 2
        self.hx = 4 * CHUNKS
        self.hy = self.hx + half
        self.fx = self.hy + half
        self.fy = self.fx + CHUNKS

    def sample(self):
        return self.pair.at[0, self.rows(0)]

    def rows(self, k):
        return pl.ds(k * self.size, self.size)

    def chunk(self, block, k):
        if len(self.part.shape) == 3:
            return self.part.at[block, self.rows(k)]
        return self.part.at[pl.ds(pl.multiple_of(block * self.toks + k * self.size, self.size), self.size)]

    def mine(self, i, k):
        view = self.chunk(self.order[i], k) if self.own is None else self.own.at[i, self.rows(k)]
        return view[...].astype(single)

    def give(self, i):
        other = self.beside(self.order[i])
        for k in range(CHUNKS):
            r = self.rows(k)
            self.go(self.chunk(other, k), self.pair.at[i, r], i * CHUNKS + k, self.core)

    def add(self, i, k, extra=None):
        r = self.rows(k)
        self.got(self.pair.at[i, r], i * CHUNKS + k)
        total = self.mine(i, k) + self.pair[i, r].astype(single)
        if extra is not None:
            ref, recv, k2 = extra
            r2 = self.rows(k2)
            self.got(ref.at[r2], recv)
            total = total + ref[r2].astype(single)
        self.pair[i, r] = total.astype(brain)

    def steps(self):
        half = CHUNKS // 2
        out = []

        def relay(i, k, to, row, recv, peer):
            self.later(lambda: self.go(self.pair.at[i, self.rows(k)], to.at[self.rows(row)], recv, peer))

        def one(k):
            self.add(0, k)
            relay(0, k, self.half_x, k, self.hx + k, self.across)
            self.add(0, k + half)
            relay(0, k + half, self.half_y, k, self.hy + k, self.along)

        def two(k):
            self.add(1, k)
            relay(1, k, self.from_x, k, self.fx + k, self.across)
            self.add(2, k + half)
            relay(2, k + half, self.from_y, k + half, self.fy + k + half, self.along)

        def three(k):
            self.add(1, k + half, (self.half_y, self.hy + k, k))
            relay(1, k + half, self.from_x, k + half, self.fx + k + half, self.across)
            self.add(2, k, (self.half_x, self.hx + k, k))
            relay(2, k, self.from_y, k, self.fy + k, self.along)

        for fn in (one, two, three):
            for k in range(half):
                out.append(functools.partial(fn, k))
        out.append(self.flush)
        return out

    def final(self, k):
        r = self.rows(k)
        self.got(self.pair.at[3, r], 3 * CHUNKS + k)
        total = self.mine(3, k) + self.pair[3, r].astype(single)
        self.got(self.from_x.at[r], self.fx + k)
        total = total + self.from_x[r].astype(single)
        self.got(self.from_y.at[r], self.fy + k)
        return total + self.from_y[r].astype(single)


def scatter_scratch(rows, cols):
    return [
        pltpu.VMEM((4, rows, cols), brain),
        pltpu.VMEM((rows // 2, cols), brain),
        pltpu.VMEM((rows // 2, cols), brain),
        pltpu.VMEM((rows, cols), brain),
        pltpu.VMEM((rows, cols), brain),
        pltpu.SemaphoreType.DMA((SCATTER_SEMS,)),
        pltpu.SemaphoreType.DMA((SCATTER_SEMS,)),
    ]


def gather_scratch(n):
    return [pltpu.SemaphoreType.DMA((GATHER_SENDS,)), pltpu.SemaphoreType.DMA((n * CHUNKS,))]


def rms(values, gain):
    return values * lax.rsqrt(jnp.mean(values * values, axis=-1, keepdims=True) + norm_eps) * gain


def fetch(src, dst, sem):
    copy = pltpu.make_async_copy(src, dst, sem)
    copy.start()
    return copy


def drive(count, body, events):
    def step(i, carry):
        body(i)
        for at, actions in events.items():

            @pl.when(i == at)
            def _(actions=actions):
                for action in actions:
                    action()

        return carry

    lax.fori_loop(0, count, step, 0)


def slots_of(denseall_ref, me, experts, dense, place):
    blocks, toks = denseall_ref.shape[0], denseall_ref.shape[2]
    for b in range(blocks):
        for e in range(experts):
            at = experts * b + e
            dense[at : at + 1, :] = denseall_ref[b, pl.ds(experts * me + e, 1), :]
    upper = (
        lax.broadcasted_iota(jnp.int32, (toks, toks), 0) < lax.broadcasted_iota(jnp.int32, (toks, toks), 1)
    ).astype(single).astype(brain)
    chosen = dense[...] > 0.0
    before = dot(chosen.astype(single).astype(brain), upper)
    place[...] = jnp.where(chosen, before, -1.0)


def picks(place, b, cap, experts):
    rows = lax.broadcasted_iota(jnp.int32, (cap, place.shape[1]), 0).astype(single)
    return [(place[pl.ds(experts * b + e, 1), :] == rows).astype(single) for e in range(experts)]


def weigh(place, dense, weight, b, cap, experts):
    for e, sel in enumerate(picks(place, b, cap, experts)):
        w = jnp.sum(sel * dense[pl.ds(experts * b + e, 1), :], axis=1, keepdims=True)
        weight[e, pl.ds(pl.multiple_of(b * cap, 16), cap), :] = w


def take(place, block, rows, b, cap):
    experts = rows.shape[0]
    both = jnp.concatenate([s.astype(brain) for s in picks(place, b, cap, experts)], axis=0)
    got = dot(both, block).astype(brain)
    at = pl.ds(pl.multiple_of(b * cap, 16), cap)
    for e in range(experts):
        rows[e, at, :] = got[e * cap : (e + 1) * cap]


def combined(place, rows, b, cap, apart):
    experts = rows.shape[0] // apart
    both = jnp.concatenate([s.astype(brain) for s in picks(place, b, cap, experts)], axis=0)
    parts = [rows[pl.ds(pl.multiple_of(e * apart + b * cap, 16), cap), :] for e in range(experts)]
    return dot(both, jnp.concatenate(parts, axis=0), 0, 0).astype(brain)


def two(p, toks):
    return pl.ds(pl.multiple_of(p * 2 * toks, 2 * toks), 2 * toks)


def meet(n, replicas, with_dp):
    me, rep = lax.axis_index("expert"), lax.axis_index("dp")
    barrier = pltpu.get_barrier_semaphore()
    for j in range(1, n):
        pl.semaphore_signal(barrier, inc=1, device_id={"expert": (me + j) % n})
    if with_dp:
        for j in range(1, replicas):
            pl.semaphore_signal(barrier, inc=1, device_id={"dp": (rep + j) % replicas})
    pl.semaphore_wait(barrier, n - 1 + (replicas - 1 if with_dp else 0))


def front_kernel(
    cap, ids_ref, hid_ref, top_ref, routes_ref, gates_ref, gain_ref, gain2_ref,
    w_hbm, a_hbm, b_hbm, wo_hbm, pa_hbm, pb_hbm, dn_hbm, da_hbm, db_hbm,
    low_ref, lse_ref, denseall_ref, orank_ref, gdr_ref, seq_hbm, proj_hbm, mixed_hbm, resid_hbm, x_hbm, g_hbm, ga_hbm,
    part, seq_ref, proj_ref, mixed_ref, topseq_ref, resid_ref, moe_ref, x_rows, g_rows, ga,
    w_ref, a_all, b_all, wo_ref, pa_all, pb_all, dn, da_all, db_all, a_ref, b_ref, mydense, dense, place, weight,
    load_sem, save_sem, *sems,
):
    toks, width = hid_ref.shape
    span = w_ref.shape[2]
    heads = span // HEAD
    n = seq_ref.shape[0]
    length = toks * n
    experts, hidden = dn.shape[0], dn.shape[1]
    loads = [
        fetch(src, dst, load_sem.at[i])
        for i, (src, dst) in enumerate(
            (
                (w_hbm, w_ref), (a_hbm, a_all), (b_hbm, b_all), (pa_hbm, pa_all), (pb_hbm, pb_all), (wo_hbm, wo_ref),
                (da_hbm, da_all), (db_hbm, db_all), (dn_hbm, dn),
            )
        )
    ]
    seq_g = Gather(seq_ref, sems[0], sems[1])
    top_g = Gather(topseq_ref, sems[2], sems[3])
    moe_g = Gather(moe_ref, sems[4], sems[5])
    red = Scatter(part, *sems[6:13])
    dsend, drecv = sems[13:15]
    me = seq_g.me
    slot = ids_ref[lax.axis_index("dp")]
    saves = []

    def save(src, dst):
        saves.append(fetch(src, dst, save_sem.at[len(saves)]))

    seq_ref[me] = rms(hid_ref[...].astype(single), gain_ref[...]).astype(brain)
    topseq_ref[me] = top_ref[...]
    choices = lax.broadcasted_iota(jnp.int32, (mydense.shape[0], toks), 0)
    table = jnp.zeros(mydense.shape, single)
    for k in range(routes_ref.shape[0]):
        table = table + jnp.where(routes_ref[k : k + 1, :] == choices, gates_ref[k : k + 1, :], 0.0)
    mydense[...] = table
    denseall_ref[me] = table
    meet(n, 1, False)
    seq_g.start()

    def dense_copy(j):
        return pltpu.make_async_remote_copy(
            src_ref=mydense, dst_ref=denseall_ref.at[me], send_sem=dsend.at[j - 1], recv_sem=drecv.at[me],
            device_id={"expert": (me + j) % n},
        )

    for j in range(1, n):
        dense_copy(j).start()
    for copy in loads[:3]:
        copy.wait()
    b_ref[...] = jnp.zeros_like(b_ref)
    for j in range(3):
        a_ref[16 * j : 16 * j + 16, :] = a_all[j, slot]
        b_ref[j, 16 * j : 16 * j + 16, :] = b_all[j, slot]

    def qkv(block):
        p = block // 2
        at = two(p, toks)
        low_ref[at, :] = dot(seq_ref[pl.ds(2 * p, 2)].reshape(2 * toks, width), a_ref[...], 1, 1).astype(brain)

        def third(j, carry):
            both = seq_ref[pl.ds(2 * p, 2)].reshape(2 * toks, width)
            proj_ref[j, at, :] = (dot(both, w_ref[j]) + dot(low_ref[at, :], b_ref[j])).astype(brain)
            return carry

        lax.fori_loop(0, 3, third, 0)

    seq_g.pair(me)
    qkv(me)
    for i in range(CHUNKS):
        seq_g.relay(i)
    top_g.start()
    seq_g.pair(seq_g.across)
    qkv(seq_g.across)
    for i in range(CHUNKS // 2):
        seq_g.relay_far(i)
    seq_g.pair(seq_g.along)
    qkv(seq_g.along)
    seq_g.pair(seq_g.far)
    qkv(seq_g.far)
    save(seq_ref, seq_hbm)
    save(proj_ref, proj_hbm)

    scale = HEAD ** (-0.5)
    block = 256
    top_steps = [functools.partial(top_g.relay, i) for i in range(CHUNKS)]
    top_steps += [functools.partial(top_g.relay_far, i) for i in range(CHUNKS // 2)]

    for h in range(heads):
        at = slice(h * HEAD, (h + 1) * HEAD)

        def attend(i, h=h, at=at):
            r = pl.ds(pl.multiple_of(i * block, block), block)
            scores = dot(proj_ref[0, r, at], proj_ref[1, :, at], 1, 1) * scale
            peak = jnp.max(scores, axis=-1, keepdims=True)
            expo = jnp.exp(scores - peak)
            total = jnp.sum(expo, axis=-1, keepdims=True)
            probs = (expo * (1.0 / total)).astype(brain)
            mixed_ref[r, at] = dot(probs, proj_ref[2, :, at]).astype(brain)
            lse_ref[r, h : h + 1] = peak + jnp.log(total)

        drive(length // block, attend, {1: top_steps[3 * h : 3 * h + 1], 3: top_steps[3 * h + 1 : 3 * h + 3]})
    del top_steps[: 3 * heads]
    for copy in loads[3:6]:
        copy.wait()

    for i in range(4):
        p = red.order[i] // 2
        at = two(p, toks)
        rank = dot(mixed_ref[at, :], pa_all[slot], 1, 1).astype(brain)
        orank_ref[at, :] = rank
        cols = min(1024, width)

        def project(c, carry, p=p, at=at):
            s = pl.ds(pl.multiple_of(c * cols, cols), cols)
            out = dot(mixed_ref[at, :], wo_ref[:, s]) + dot(orank_ref[at, :], pb_all[slot, :, s])
            part[pl.ds(2 * p, 2), :, s] = out.astype(brain).reshape(2, toks, cols)
            return carry

        lax.fori_loop(0, width // cols, project, 0)
        if i:
            red.give(i - 1)
    red.give(3)
    save(mixed_ref, mixed_hbm)
    for step in top_steps:
        step()
    for block_at in (me, top_g.across, top_g.along, top_g.far):
        top_g.pair(block_at)
    for j in range(1, n):
        src = (me + j) % n
        view = denseall_ref.at[src]
        pltpu.make_async_remote_copy(
            src_ref=view, dst_ref=view, send_sem=dsend.at[0], recv_sem=drecv.at[src], device_id={"expert": src}
        ).wait_recv()
    for j in range(1, n):
        dense_copy(j).wait_send()
    slots_of(denseall_ref, me, experts, dense, place)
    steps = red.steps()

    def top_rows(b):
        weigh(place, dense, weight, b, cap, experts)
        take(place, topseq_ref[b], g_rows, b, cap)

    drive(n, top_rows, {1: steps[0:1], 2: steps[1:2], 3: steps[2:3], 4: steps[3:4]})
    for copy in loads[6:]:
        copy.wait()

    def top_rank(e):
        gdr_ref[e] = (dot(g_rows[e], db_all[e, slot], 1, 1) * weight[e]).astype(brain)

    drive(experts, top_rank, {})
    half = n * cap // 2
    tiles = hidden // TILE

    def top_tile(t):
        e, f, m = t // (2 * tiles), t // 2 % tiles, t % 2
        at = pl.ds(pl.multiple_of(f * TILE, TILE), TILE)
        r = pl.ds(pl.multiple_of(m * half, 16), half)
        out = dot(g_rows[e, r, :], dn[e, at, :], 1, 1) * weight[e, r, :]
        ga[e, r, at] = (out + dot(gdr_ref[e, r, :], da_all[e, slot, :, at])).astype(brain)

    drive(2 * experts * tiles, top_tile, {2: steps[4:5], 4: steps[5:6], 5: steps[6:7]})
    save(g_rows, g_hbm)
    save(ga, ga_hbm)
    for k in ORDER:
        r = red.rows(k)
        resid = hid_ref[r].astype(single) + red.final(k)
        resid_ref[r] = resid
        moe_ref[me, r] = rms(resid, gain2_ref[...]).astype(brain)
        if k != ORDER[0]:
            moe_g.start_own(ORDER[ORDER.index(k) - 1])
    save(resid_ref, resid_hbm)
    moe_g.start_own(ORDER[-1])

    def moe_rows(block_at):
        p = block_at // 2

        def one(i, carry):
            take(place, moe_ref[2 * p + i], x_rows, 2 * p + i, cap)
            return carry

        lax.fori_loop(0, 2, one, 0)

    moe_g.pair(me)
    moe_rows(me)
    for i in range(CHUNKS):
        moe_g.relay(i)
    moe_g.pair(moe_g.across)
    moe_rows(moe_g.across)
    for i in range(CHUNKS // 2):
        moe_g.relay_far(i)
    moe_g.pair(moe_g.along)
    moe_rows(moe_g.along)
    moe_g.pair(moe_g.far)
    moe_rows(moe_g.far)
    save(x_rows, x_hbm)
    for mover in (seq_g, top_g, red, moe_g):
        mover.drain()
    for copy in saves:
        copy.wait()


def front(ids, hid, top, routes, gates, gain, gain2, w, a, b, wo, pa, pb, dn, da, db, n, cap, cid=0):
    toks, width = hid.shape
    span = w.shape[2]
    length = toks * n
    experts, hidden = dn.shape[0], dn.shape[1]
    rows = n * cap
    vm = pl.BlockSpec(memory_space=pltpu.VMEM)
    sm = pl.BlockSpec(memory_space=pltpu.SMEM)
    hb = pl.BlockSpec(memory_space=pl.ANY)
    f = lambda *s: jax.ShapeDtypeStruct(s, single)
    h = lambda *s: jax.ShapeDtypeStruct(s, brain)
    bv = lambda *s: pltpu.VMEM(s, brain)
    fv = lambda *s: pltpu.VMEM(s, single)
    whole = bv(n, toks, width)
    return pl.pallas_call(
        functools.partial(front_kernel, cap),
        out_shape=(
            h(length, 48), f(length, span // HEAD), f(n, experts * n, toks), h(length, 16), h(experts, rows, 16),
            h(n, toks, width), h(3, length, span), h(length, span), f(toks, width),
            h(experts, rows, width), h(experts, rows, width), h(experts, rows, hidden),
        ),
        in_specs=[sm] + [vm] * 6 + [hb] * 9,
        out_specs=[vm] * 5 + [hb] * 7,
        scratch_shapes=[
            whole, whole, bv(3, length, span), bv(length, span), whole, fv(toks, width), whole,
            bv(experts, rows, width), bv(experts, rows, width), bv(experts, rows, hidden),
        ]
        + [pltpu.VMEM(v.shape, brain) for v in (w, a, b, wo, pa, pb, dn, da, db)]
        + [
            bv(48, width), bv(3, 48, span), fv(experts * n, toks), fv(n * experts, toks), fv(n * experts, toks),
            fv(experts, rows, 1), pltpu.SemaphoreType.DMA((9,)), pltpu.SemaphoreType.DMA((7,)),
        ]
        + gather_scratch(n) + gather_scratch(n) + gather_scratch(n) + scatter_scratch(toks, width)
        + [pltpu.SemaphoreType.DMA((n,)), pltpu.SemaphoreType.DMA((n,))],
        compiler_params=pltpu.CompilerParams(collective_id=cid, has_side_effects=True, vmem_limit_bytes=VMEM_ALL),
        name="front",
    )(ids, hid, top, routes, gates, gain, gain2, w, a, b, wo, pa, pb, dn, da, db)


def moe_kernel(
    cap, replicas, ids_ref, denseall_ref, gdr_ref, x_hbm, g_hbm, ga_hbm, gu_hbm, ha_hbm, hb_hbm, da_hbm,
    drank_ref, gina_ref, gmidb_ref, gdna_ref, gdnb_ref, gpart_hbm, act_hbm,
    gu, x_rows, g_rows, ga, s_rows, act, gg, uu, dense, place, weight, irank, girank, ha_ref, hb_ref, da_ref,
    out_stage, pick_sem, x_sem, g_sem, ga_sem, gu_sem, act_sem, out_sem,
):
    experts, width, hidden = gu.shape[0], gu.shape[2], gu.shape[3]
    blocks = denseall_ref.shape[0]
    rows = x_rows.shape[1]
    tiles = hidden // TILE
    me = lax.axis_index("expert")
    which = ids_ref[lax.axis_index("dp")]
    picked = []
    for e in range(experts):
        for i in range(2):
            picked.append((ha_hbm.at[e, i, which], ha_ref.at[e, pl.ds(16 * i, 16)]))
            picked.append((hb_hbm.at[e, i, which], hb_ref.at[e, i]))
        picked.append((da_hbm.at[e, which], da_ref.at[e]))

    def cols(f):
        return pl.ds(pl.multiple_of(f * TILE, TILE), TILE)

    x_copy = lambda e: pltpu.make_async_copy(x_hbm.at[e], x_rows.at[e], x_sem.at[e])
    g_copy = lambda e: pltpu.make_async_copy(g_hbm.at[e], g_rows.at[e], g_sem.at[e])
    ga_copy = lambda e: pltpu.make_async_copy(ga_hbm.at[e], ga.at[e], ga_sem.at[e])
    gu_copy = lambda e, f: pltpu.make_async_copy(
        gu_hbm.at[e, :, :, cols(f)], gu.at[e, :, :, cols(f)], gu_sem.at[e, f]
    )
    act_copy = lambda e: pltpu.make_async_copy(act.at[e], act_hbm.at[e], act_sem.at[e])
    x_copy(0).start()
    picked = [fetch(s, d, pick_sem.at[i]) for i, (s, d) in enumerate(picked)]
    for e in range(experts):
        for f in range(tiles):
            gu_copy(e, f).start()
            if f == 0:
                ga_copy(e).start()
        if e + 1 < experts:
            x_copy(e + 1).start()
        g_copy(e).start()
    slots_of(denseall_ref, me, experts, dense, place)

    def weighed(b, carry):
        weigh(place, dense, weight, b, cap, experts)
        return carry

    lax.fori_loop(0, blocks, weighed, 0)
    for copy in picked:
        copy.wait()

    def expert(e, carry):
        x_copy(e).wait()
        irank[...] = dot(x_rows[e], ha_ref[e], 1, 1).astype(brain)
        ga_copy(e).wait()

        def tile(f, c):
            at = cols(f)
            gu_copy(e, f).wait()
            gate = dot(x_rows[e], gu[e, 0, :, at]) + dot(irank[:, :16], hb_ref[e, 0, :, at])
            up = dot(x_rows[e], gu[e, 1, :, at]) + dot(irank[:, 16:], hb_ref[e, 1, :, at])
            back = ga[e, :, at].astype(single)
            sig = jax.nn.sigmoid(gate)
            swish = gate * sig
            act[e, :, at] = (swish * up).astype(brain)
            gg[:, at] = (back * up * sig * (1.0 + gate * (1.0 - sig))).astype(brain)
            uu[:, at] = (back * swish).astype(brain)
            return c

        lax.fori_loop(0, tiles, tile, 0)
        act_copy(e).start()
        drank_ref[e] = dot(act[e], da_ref[e], 1, 1).astype(brain)
        girank[:, :16] = dot(gg[...], hb_ref[e, 0], 1, 1).astype(brain)
        girank[:, 16:] = dot(uu[...], hb_ref[e, 1], 1, 1).astype(brain)

        def deal(ref, row, value):
            piece = value.shape[1] // replicas
            at = pl.ds(pl.multiple_of(row, 16), value.shape[0])
            for d in range(replicas):
                ref[d, at, :] = value[:, d * piece : (d + 1) * piece].astype(brain)

        deal(gdna_ref, e * 16, dot(gdr_ref[e], act[e], 0, 0))
        deal(gmidb_ref, e * 32, dot(irank[:, :16], gg[...], 0, 0))
        deal(gmidb_ref, e * 32 + 16, dot(irank[:, 16:], uu[...], 0, 0))
        deal(gina_ref, e * 32, dot(girank[...], x_rows[e], 0, 0))
        g_copy(e).wait()
        deal(gdnb_ref, e * 16, dot((drank_ref[e].astype(single) * weight[e]).astype(brain), g_rows[e], 0, 0))

        def slots(d, c):
            at = cols(d)
            s = dot(gg[...], gu[e, 0, at, :], 1, 1) + dot(uu[...], gu[e, 1, at, :], 1, 1)
            s_rows[pl.ds(pl.multiple_of(e * rows, 16), rows), at] = (s + dot(girank[...], ha_ref[e, :, at])).astype(brain)
            return c

        lax.fori_loop(0, width // TILE, slots, 0)
        return carry

    lax.fori_loop(0, experts, expert, 0)
    out_copy = lambda b: pltpu.make_async_copy(out_stage.at[b % 2], gpart_hbm.at[b], out_sem.at[b % 2])

    def combine(b, carry):
        @pl.when(b >= 2)
        def _():
            out_copy(b - 2).wait()

        out_stage[b % 2] = combined(place, s_rows, b, cap, rows)
        out_copy(b).start()
        return carry

    lax.fori_loop(0, blocks, combine, 0)
    for b in (blocks - 2, blocks - 1):
        out_copy(b).wait()
    for e in range(experts):
        act_copy(e).wait()


def moe(ids, dense, gdr, x, g, ga, gu, ha, hb, da, cap, replicas):
    experts, rows, width = x.shape
    blocks, toks = dense.shape[0], dense.shape[2]
    hidden = gu.shape[3]
    rank = da.shape[2]
    vm = pl.BlockSpec(memory_space=pltpu.VMEM)
    sm = pl.BlockSpec(memory_space=pltpu.SMEM)
    hb_ = pl.BlockSpec(memory_space=pl.ANY)
    h = lambda *s: jax.ShapeDtypeStruct(s, brain)
    bv = lambda *s: pltpu.VMEM(s, brain)
    fv = lambda *s: pltpu.VMEM(s, single)
    dma = pltpu.SemaphoreType.DMA
    return pl.pallas_call(
        functools.partial(moe_kernel, cap, replicas),
        out_shape=(
            h(experts, rows, rank),
            h(replicas, experts * 2 * rank, width // replicas), h(replicas, experts * 2 * rank, hidden // replicas),
            h(replicas, experts * rank, hidden // replicas), h(replicas, experts * rank, width // replicas),
            h(blocks, toks, width), h(experts, rows, hidden),
        ),
        in_specs=[sm, vm, vm] + [hb_] * 7,
        out_specs=[vm] * 5 + [hb_] * 2,
        scratch_shapes=[
            bv(*gu.shape), bv(*x.shape), bv(*x.shape), bv(*ga.shape), bv(experts * rows, width), bv(*ga.shape),
            bv(rows, hidden), bv(rows, hidden), fv(blocks * experts, toks), fv(blocks * experts, toks),
            fv(experts, rows, 1), bv(rows, 2 * rank), bv(rows, 2 * rank), bv(experts, 2 * rank, width),
            bv(experts, 2, rank, hidden), bv(experts, rank, hidden), bv(2, toks, width),
            dma((5 * experts,)), dma((experts,)), dma((experts,)), dma((experts,)), dma((experts, hidden // TILE)),
            dma((experts,)), dma((2,)),
        ],
        compiler_params=pltpu.CompilerParams(vmem_limit_bytes=VMEM_ALL),
        name="moe",
    )(ids, dense, gdr, x, g, ga, gu, ha, hb, da)


ADAPTERS = 8
RANK = 16
CLIP = 256.0
beta_one = 0.9
beta_two = 0.95
learn_rate = 0.02
weight_decay = 0.1
adam_eps = 1e-08


def norm_back(values, gain, grad):
    inverse = lax.rsqrt(jnp.mean(values * values, axis=-1, keepdims=True) + norm_eps)
    scaled = grad * gain
    return inverse * scaled - values * (
        inverse * inverse * inverse * jnp.mean(scaled * values, axis=-1, keepdims=True)
    )


def back_kernel(
    cap, replicas,
    ids_ref, hid_ref, top_ref, gain_ref, gain2_ref, low_ref, lse_ref, orank_ref, denseall_ref, drank_ref,
    resid_hbm, seq_hbm, proj_hbm, mixed_hbm, gpart_hbm, act_hbm, dn_hbm, db_hbm,
    w_hbm, a_hbm, b_hbm, wo_hbm, pa_hbm, pb_hbm, gina_hbm, gmidb_hbm, gdna_hbm, gdnb_hbm,
    out_ref, gh_ref, norm_ref, shared_got, got_qb, got_oa, got_ina, got_midb, got_dna, got_dnb,
    resid_ref, proj_ref, mixed_ref, own_g, ypart, act, dn, db_all, part, dense, place, weight,
    w_ref, a_all, b_all, wo_ref, pa_all, pb_all, a_ref,
    bf, gres, gmix, grank, gproj, glow, gk, gv,
    gqb_ref, goa_ref, shared_ref, shared_in, shared_mid, tot_e, tot_d, mine, load_sem, own_sem,
    sh_send, sh_recv, mid_send, mid_recv, p_send, p_recv, t_send, t_recv, *sems,
):
    toks, width = hid_ref.shape
    span = w_ref.shape[2]
    heads = span // HEAD
    n = denseall_ref.shape[0]
    experts = dn.shape[0]
    length = toks * n
    red = Scatter(gpart_hbm, *sems[0:7], own=own_g)
    redy = Scatter(ypart, *sems[7:14])
    redn = Scatter(part, *sems[14:21])
    bf_g = Gather(bf, *sems[21:23])
    me = red.me
    rep = lax.axis_index("dp")
    slot = ids_ref[rep]
    owns = [fetch(gpart_hbm.at[red.order[i]], own_g.at[i], own_sem.at[i]) for i in range(4)]
    loads = {}
    for i, (name, src, dst) in enumerate(
        (
            ("act", act_hbm, act), ("db", db_hbm, db_all), ("dn", dn_hbm, dn), ("resid", resid_hbm, resid_ref), ("wo", wo_hbm, wo_ref), ("pb", pb_hbm, pb_all), ("pa", pa_hbm, pa_all),
            ("mixed", mixed_hbm, mixed_ref), ("proj", proj_hbm, proj_ref), ("b", b_hbm, b_all), ("a", a_hbm, a_all),
            ("w", w_hbm, w_ref), ("ina", gina_hbm.at[rep], got_ina.at[rep]),
            ("midb", gmidb_hbm.at[rep], got_midb.at[rep]), ("dna", gdna_hbm.at[rep], got_dna.at[rep]),
            ("dnb", gdnb_hbm.at[rep], got_dnb.at[rep]),
        )
    ):
        loads[name] = fetch(src, dst, load_sem.at[i])

    def need(*names):
        for name in names:
            loads.pop(name).wait()

    meet(n, replicas, True)
    for i in range(4):
        red.give(i)
    pending = []

    def go(src, dst, send_sem, recv_sem, where):
        copy = pltpu.make_async_remote_copy(
            src_ref=src, dst_ref=dst, send_sem=send_sem, recv_sem=recv_sem, device_id=where
        )
        copy.start()
        pending.append(copy)

    def wait(view, recv_sem):
        pltpu.make_async_remote_copy(
            src_ref=view, dst_ref=view, send_sem=t_send.at[0], recv_sem=recv_sem, device_id={"expert": (me + 1) % n}
        ).wait_recv()

    got = (got_qb, got_oa, got_ina, got_midb, got_dna, got_dnb)

    def swap(i, source):
        for j in range(1, replicas):
            peer = (rep + j) % replicas
            go(
                source.at[peer], got[i].at[rep], p_send.at[i * replicas + j], p_recv.at[i * replicas + rep],
                {"dp": peer},
            )

    def swapped(i):
        for j in range(1, replicas):
            src = (rep + j) % replicas
            wait(got[i].at[src], p_recv.at[i * replicas + src])

    for i, source in enumerate((gina_hbm, gmidb_hbm, gdna_hbm, gdnb_hbm)):
        swap(i + 2, source)
    slots_of(denseall_ref, me, experts, dense, place)

    def weighed(block_at):
        weigh(place, dense, weight, block_at, cap, experts)

    drive(n, weighed, {})
    for copy in owns:
        copy.wait()
    need("act", "db", "dn")
    tiles = width // TILE

    def y_tile(t):
        e = t // tiles
        s = pl.ds(pl.multiple_of(t % tiles * TILE, TILE), TILE)
        y = dot(act[e], dn[e, :, s]) + dot(drank_ref[e], db_all[e, slot, :, s])
        part[pl.ds(pl.multiple_of(e * n * cap, 16), n * cap), s] = (y * weight[e]).astype(brain)

    steps = red.steps()
    drive(
        experts * tiles, y_tile,
        {0: steps[0:1], 1: steps[1:2], 2: steps[2:3], 3: steps[3:4], 6: steps[4:5], 8: steps[5:6], 9: steps[6:7]},
    )
    seq_ref = dn.at[0]
    loads["seq"] = fetch(seq_hbm, seq_ref, load_sem.at[len(loads) + 4])
    need("resid")
    for k in ORDER:
        r = red.rows(k)
        grad = top_ref[r].astype(single) + norm_back(resid_ref[r], gain2_ref[...], red.final(k))
        gres[r] = grad
        bf[me, r] = grad.astype(brain)
        if k != ORDER[0]:
            bf_g.start_own(ORDER[ORDER.index(k) - 1])
    bf_g.start_own(ORDER[-1])
    need("wo", "pb", "pa", "mixed")

    def mixed_grad(block):
        p = block // 2
        both = bf[pl.ds(2 * p, 2)].reshape(2 * toks, width)
        at = two(p, toks)
        rank = dot(both, pb_all[slot], 1, 1).astype(brain)
        grank[at, :] = rank
        gmix[at, :] = (dot(both, wo_ref[...], 1, 1) + dot(rank, pa_all[slot])).astype(brain)

    def y_block(block_at):
        ypart[block_at] = combined(place, part, block_at, cap, n * cap)

    bf_g.pair(me)
    mixed_grad(me)
    drive(
        n, y_block, {2: [functools.partial(bf_g.relay, 0)], 6: [functools.partial(bf_g.relay, 1)]},
    )
    for i in range(2, CHUNKS):
        bf_g.relay(i)
    for i in range(4):
        redy.give(i)
    bf_g.pair(bf_g.across)
    mixed_grad(bf_g.across)
    for i in range(CHUNKS // 2):
        bf_g.relay_far(i)
    bf_g.pair(bf_g.along)
    mixed_grad(bf_g.along)
    bf_g.pair(bf_g.far)
    mixed_grad(bf_g.far)

    piece = span // replicas
    goa = dot(grank[...], mixed_ref[...], 0, 0)
    for d in range(replicas):
        goa_ref[d] = goa[:, d * piece : (d + 1) * piece].astype(brain)
    got_oa[rep] = goa_ref[rep]
    swap(1, goa_ref)

    need("proj")
    steps = redy.steps()
    scale = HEAD ** (-0.5)
    block = 256
    for h in range(heads):
        at = slice(h * HEAD, (h + 1) * HEAD)
        gk[...] = jnp.zeros_like(gk)
        gv[...] = jnp.zeros_like(gv)

        def attend(i, h=h, at=at):
            r = pl.ds(pl.multiple_of(i * block, block), block)
            q, do = proj_ref[0, r, at], gmix[r, at]
            delta = jnp.sum(do.astype(single) * mixed_ref[r, at].astype(single), axis=-1, keepdims=True)
            probs = jnp.exp(dot(q, proj_ref[1, :, at], 1, 1) * scale - lse_ref[r, h : h + 1])
            gp = dot(do, proj_ref[2, :, at], 1, 1)
            gs = (probs * (gp - delta)).astype(brain)
            gproj[0, r, at] = (dot(gs, proj_ref[1, :, at]) * scale).astype(brain)
            gk[...] += dot(gs, q, 0, 0)
            gv[...] += dot(probs.astype(brain), do, 0, 0)

        count = (len(steps) + heads - 1) // heads
        mine_now = steps[h * count : (h + 1) * count]
        drive(length // block, attend, {i: mine_now[i : i + 1] for i in range(len(mine_now))})
        gproj[1, :, at] = (gk[...] * scale).astype(brain)
        gproj[2, :, at] = gv[...].astype(brain)

    need("a", "b", "w")
    for j in range(3):
        a_ref[16 * j : 16 * j + 16, :] = a_all[j, slot]
    for i in range(4):
        p = redn.order[i] // 2
        at = two(p, toks)
        for j in range(3):
            glow[at, 16 * j : 16 * j + 16] = dot(gproj[j, at, :], b_all[j, slot], 1, 1).astype(brain)
        wide = min(1024, width)

        def normed_grad(c, carry, p=p, at=at):
            s = pl.ds(pl.multiple_of(c * wide, wide), wide)
            out = dot(glow[at, :], a_ref[:, s])
            for j in range(3):
                out = out + dot(gproj[j, at, :], w_ref[j, s, :], 1, 1)
            part[at, s] = out.astype(brain)
            return carry

        lax.fori_loop(0, width // wide, normed_grad, 0)
        if i:
            redn.give(i - 1)
    redn.give(3)

    thin = width // (n * replicas)

    def share(row, value, base):
        for c in range(value.shape[1] // thin):
            d, e = (base + c) // n, (base + c) % n
            shared_ref[e, row : row + value.shape[0], d * thin : (d + 1) * thin] = value[
                :, c * thin : (c + 1) * thin
            ].astype(brain)

    nsteps = redn.steps()

    def advance():
        if nsteps:
            nsteps.pop(0)()

    for j in range(3):
        gqb = dot(low_ref[:, 16 * j : 16 * j + 16], gproj[j], 0, 0)
        for d in range(replicas):
            gqb_ref[d, 16 * j : 16 * j + 16, :] = gqb[:, d * piece : (d + 1) * piece].astype(brain)
    advance()
    got_qb[rep] = gqb_ref[rep]
    swap(0, gqb_ref)
    need("seq")
    cols = 512
    for c in range(width // cols):
        s = slice(c * cols, (c + 1) * cols)
        share(0, dot(glow[...], seq_ref[:, s], 0, 0), c * cols // thin)
        share(48, dot(orank_ref[...], bf[:, :, s].reshape(length, cols), 0, 0), c * cols // thin)
        advance()
    shared_in[me] = shared_ref[me]
    for j in range(1, n):
        peer = (me + j) % n
        go(shared_ref.at[peer], shared_in.at[me], sh_send.at[j - 1], sh_recv.at[me], {"expert": peer})
    while nsteps:
        advance()

    def squares(i, source):
        rows = source.shape[1] // RANK

        def body(t, acc):
            at = pl.ds(pl.multiple_of(t // ADAPTERS * RANK, RANK), RANK)
            value = jnp.zeros((RANK, source.shape[2]), single)
            for s in range(replicas):
                value = value + source[s, at, :].astype(single) * jnp.where(ids_ref[s] == t % ADAPTERS, 1.0, 0.0)
            return acc + value * value

        return jnp.sum(
            lax.fori_loop(0, rows * ADAPTERS, body, jnp.zeros((RANK, source.shape[2]), single))
        )

    need("ina", "midb", "dna", "dnb")
    total = jnp.zeros((), single)
    for i in range(2, 6):
        swapped(i)
        total = total + squares(i, got[i])
    for j in range(1, n):
        src = (me + j) % n
        wait(shared_in.at[src], sh_recv.at[src])
    summed = shared_in[0].astype(single)
    for e in range(1, n):
        summed = summed + shared_in[e].astype(single)
    for d in range(replicas):
        shared_mid[d] = summed[:, d * thin : (d + 1) * thin].astype(brain)
    shared_got[rep] = shared_mid[rep]
    for j in range(1, replicas):
        peer = (rep + j) % replicas
        go(shared_mid.at[peer], shared_got.at[rep], mid_send.at[j], mid_recv.at[rep], {"dp": peer})
    for k in ORDER:
        r = redy.rows(k)
        out_ref[r] = (resid_ref[r] + redy.final(k)).astype(brain)
    for i in range(2):
        swapped(i)
        total = total + squares(i, got[i])
    for j in range(1, replicas):
        src = (rep + j) % replicas
        wait(shared_got.at[src], mid_recv.at[src])
    total = total + squares(0, shared_got)

    mine[0] = jnp.full(mine.shape[1:], total, single)
    tot_e[me] = mine[0]
    for j in range(1, n):
        go(mine.at[0], tot_e.at[me], t_send.at[j], t_recv.at[me], {"expert": (me + j) % n})
    for j in range(1, n):
        src = (me + j) % n
        wait(tot_e.at[src], t_recv.at[src])
    total = tot_e[0]
    for e in range(1, n):
        total = total + tot_e[e]
    mine[1] = total
    tot_d[rep] = mine[1]
    for j in range(1, replicas):
        go(mine.at[1], tot_d.at[rep], t_send.at[n + j], t_recv.at[n + rep], {"dp": (rep + j) % replicas})
    for k in ORDER:
        r = redn.rows(k)
        gh_ref[r] = gres[r] + norm_back(hid_ref[r].astype(single), gain_ref[...], redn.final(k))
    for j in range(1, replicas):
        src = (rep + j) % replicas
        wait(tot_d.at[src], t_recv.at[n + src])
    total = tot_d[0]
    for d in range(1, replicas):
        total = total + tot_d[d]
    norm_ref[...] = jnp.sqrt(total)
    for mover in (red, redy, redn, bf_g):
        mover.drain()
    for copy in pending:
        copy.wait_send()


def back(
    ids, hid, top, gain, gain2, low, lse, orank, dense, drank, resid, seq, proj, mixed, gpart, act, dn, db,
    w, a, b, wo, pa, pb, pieces, cap, replicas, cid=1,
):
    n, toks, width = seq.shape
    seq = seq.reshape(n * toks, width)
    experts, rows = act.shape[:2]
    span = w.shape[2]
    length = toks * n
    vm = pl.BlockSpec(memory_space=pltpu.VMEM)
    sm = pl.BlockSpec(memory_space=pltpu.SMEM)
    hb = pl.BlockSpec(memory_space=pl.ANY)
    f = lambda *s: jax.ShapeDtypeStruct(s, single)
    h = lambda *s: jax.ShapeDtypeStruct(s, brain)
    bv = lambda *s: pltpu.VMEM(s, brain)
    fv = lambda *s: pltpu.VMEM(s, single)
    dma = pltpu.SemaphoreType.DMA
    thin = width // (n * replicas)
    piece = span // replicas
    return pl.pallas_call(
        functools.partial(back_kernel, cap, replicas),
        out_shape=(
            h(toks, width), f(toks, width), f(8, 128), h(replicas, 64, thin), h(replicas, 48, piece),
            h(replicas, 16, piece),
        ) + tuple(h(*p.shape) for p in pieces),
        in_specs=[sm] + [vm] * 9 + [hb] * 18,
        out_specs=[vm] * 10,
        scratch_shapes=[
            fv(toks, width), bv(3, length, span), bv(length, span), bv(4, toks, width), bv(n, toks, width),
            bv(*act.shape), bv(*dn.shape), bv(*db.shape), bv(experts * rows, width), fv(n * experts, toks),
            fv(n * experts, toks), fv(experts, rows, 1),
        ]
        + [pltpu.VMEM(v.shape, brain) for v in (w, a, b, wo, pa, pb)]
        + [
            bv(48, width), bv(n, toks, width), fv(toks, width), bv(length, span), bv(length, 16),
            bv(3, length, span), bv(length, 48), fv(length, HEAD), fv(length, HEAD),
            bv(replicas, 48, piece), bv(replicas, 16, piece), bv(n, 64, replicas * thin), bv(n, 64, replicas * thin),
            bv(replicas, 64, thin), fv(n, 8, 128), fv(replicas, 8, 128), fv(2, 8, 128), dma((20,)), dma((4,)),
            dma((n,)), dma((n,)), dma((replicas,)), dma((replicas,)), dma((6 * replicas,)), dma((6 * replicas,)),
            dma((n + replicas,)), dma((n + replicas,)),
        ]
        + scatter_scratch(toks, width) * 3 + gather_scratch(n),
        compiler_params=pltpu.CompilerParams(collective_id=cid, has_side_effects=True, vmem_limit_bytes=VMEM_ALL),
        name="back",
    )(
        ids, hid, top, gain, gain2, low, lse, orank, dense, drank, resid, seq, proj, mixed, gpart, act, dn, db,
        w, a, b, wo, pa, pb, *pieces,
    )


def adam_kernel(n, replicas, groups, spans, adapter_ref, step_ref, norm_in, out_in, gh_in, *refs):
    got, refs = refs[:7], refs[7:]
    weight_hbm, first_hbm, second_hbm, refs = refs[:8], refs[8:16], refs[16:24], refs[24:]
    out_hbm, gh_hbm, norm_ref, result, refs = refs[0], refs[1], refs[2], refs[3:35], refs[35:]
    weight, first, second, kept, refs = refs[:8], refs[8:16], refs[16:24], refs[24:56], refs[56:]
    load_sem, save_sem = refs
    me, rep = lax.axis_index("expert"), lax.axis_index("dp")
    common = rep * n + me
    loads, saves = [], []
    for a in range(8):
        size, pieces = spans[a]
        index = common if pieces == n * replicas else rep
        start = index * size // weight[a].shape[1] * weight[a].shape[1]
        view = weight_hbm[a].at[:, pl.ds(pl.multiple_of(start, 128), weight[a].shape[1])]
        loads.append(
            [
                fetch(src, dst, load_sem.at[3 * a + k])
                for k, (src, dst) in enumerate(((view, weight[a]), (first_hbm[a], first[a]), (second_hbm[a], second[a])))
            ]
        )
    saves.append(fetch(out_in, out_hbm, save_sem.at[32]))
    saves.append(fetch(gh_in, gh_hbm, save_sem.at[33]))
    norm_ref[0] = norm_in[0, 0]
    factor = jnp.minimum(1.0, CLIP / norm_in[...])[0:1, 0:1]
    steps = jnp.full((8, 128), step_ref[0].astype(single), single)
    fix_first = (1.0 / (1.0 - jnp.exp(steps * jnp.log(jnp.full((8, 128), beta_one, single)))))[0:1, 0:1]
    fix_second = (1.0 / (1.0 - jnp.exp(steps * jnp.log(jnp.full((8, 128), beta_two, single)))))[0:1, 0:1]
    for a in (4, 7, 5, 6, 0, 2, 1, 3):
        for copy in loads[a]:
            copy.wait()
        source = got[max(a - 1, 0)]
        base = groups[0] if a == 1 else 0
        size, pieces = spans[a]
        window = weight[a].shape[1]
        index = common if pieces == n * replicas else rep

        def body(t, carry, a=a, source=source, base=base, size=size, window=window, index=index):
            rows = pl.ds(pl.multiple_of((base + t) * RANK, RANK), RANK)
            parts = [source[s, rows, :].astype(single) for s in range(replicas)]
            for adapter in range(ADAPTERS):
                at = pl.ds(pl.multiple_of((t * ADAPTERS + adapter) * RANK, RANK), RANK)
                grad = jnp.zeros((RANK, size), single)
                for s in range(replicas):
                    grad = grad + parts[s] * jnp.where(adapter_ref[s] == adapter, 1.0, 0.0)
                held = weight[a][at, :].astype(single)
                w = held[:, :size]
                for c in range(1, window // size):
                    w = jnp.where(index % (window // size) == c, held[:, c * size : (c + 1) * size], w)
                clipped = grad * factor
                f = beta_one * first[a][at, :] + (1.0 - beta_one) * clipped
                s = beta_two * second[a][at, :] + (1.0 - beta_two) * clipped * clipped
                kept[4 * a][at, :] = grad
                kept[4 * a + 1][at, :] = f
                kept[4 * a + 2][at, :] = s
                kept[4 * a + 3][at, :] = -learn_rate * (
                    f * fix_first / (jnp.sqrt(s * fix_second) + adam_eps) + weight_decay * w
                )
            return carry

        lax.fori_loop(0, groups[a], body, 0)
        for k in range(4):
            saves.append(fetch(kept[4 * a + k], result[4 * a + k], save_sem.at[4 * a + k]))
    for copy in saves:
        copy.wait()


def adam(adapters, steps, norm, block_out, gh, got, weight, pieces, first, second, n, replicas):
    spans = tuple((f.shape[1], p) for f, p in zip(first, pieces))
    groups = tuple(f.shape[0] // (ADAPTERS * RANK) for f in first)
    vm = pl.BlockSpec(memory_space=pltpu.VMEM)
    sm = pl.BlockSpec(memory_space=pltpu.SMEM)
    hb = pl.BlockSpec(memory_space=pl.ANY)
    f = lambda s: jax.ShapeDtypeStruct(s, single)
    dma = pltpu.SemaphoreType.DMA
    shapes = [t.shape for t in first]
    return pl.pallas_call(
        functools.partial(adam_kernel, n, replicas, groups, spans),
        out_shape=(jax.ShapeDtypeStruct(block_out.shape, brain), f(gh.shape), f((1,)))
        + tuple(f(s) for s in shapes for _ in range(4)),
        in_specs=[sm, sm, vm, vm, vm] + [vm] * 7 + [hb] * 24,
        out_specs=[hb, hb, sm] + [hb] * 32,
        scratch_shapes=[pltpu.VMEM((s[0], max(s[1], 128)), brain) for s in shapes]
        + [pltpu.VMEM(s, single) for s in shapes] * 2
        + [pltpu.VMEM(s, single) for s in shapes for _ in range(4)]
        + [dma((24,)), dma((34,))],
        compiler_params=pltpu.CompilerParams(vmem_limit_bytes=VMEM_ALL),
        name="adam",
    )(adapters, steps, norm, block_out, gh, *got, *weight, *first, *second)


def per_device(
    hidden,
    output_cotangent,
    attention_gain,
    expert_norm_gain,
    query_key_value_weight,
    output_weight,
    gate_up_weight,
    down_weight,
    token_experts,
    expert_gate_weight,
    sequence_adapter,
    optimizer_steps,
    adapter_attention_input,
    adapter_attention_output,
    adapter_projection_input,
    adapter_projection_output,
    adapter_hidden_input,
    adapter_hidden_output,
    adapter_down_input,
    adapter_down_output,
    moment_attention_input,
    moment_attention_output,
    moment_projection_input,
    moment_projection_output,
    moment_hidden_input,
    moment_hidden_output,
    moment_down_input,
    moment_down_output,
    squared_attention_input,
    squared_attention_output,
    squared_projection_input,
    squared_projection_output,
    squared_hidden_input,
    squared_hidden_output,
    squared_down_input,
    squared_down_output,
):
    n = lax.axis_size("expert")
    replicas = lax.axis_size("dp")
    toks, width = hidden.shape[1:]
    here = down_weight.shape[0]
    cap = min(toks, toks * token_experts.shape[2] * 5 // (4 * here * n))
    gain = attention_gain[None]
    gain2 = expert_norm_gain[None]
    hid, cot = hidden[0], output_cotangent[0]
    low, lse, dense_all, orank, gdr, seq, proj, mixed, resid, x_rows, g_rows, ga = front(
        sequence_adapter, hid, cot, token_experts[0].T, expert_gate_weight[0].T, gain, gain2, query_key_value_weight,
        adapter_attention_input, adapter_attention_output, output_weight, adapter_projection_input,
        adapter_projection_output, down_weight, adapter_down_input, adapter_down_output, n, cap,
    )
    drank, *pieces, gpart, act = moe(
        sequence_adapter, dense_all, gdr, x_rows, g_rows, ga, gate_up_weight, adapter_hidden_input,
        adapter_hidden_output, adapter_down_input, cap, replicas,
    )
    block_out, grad_hidden, norm, *got = back(
        sequence_adapter, hid, cot, gain, gain2, low, lse, orank, dense_all, drank, resid, seq, proj, mixed, gpart,
        act, down_weight, adapter_down_output,
        query_key_value_weight, adapter_attention_input, adapter_attention_output, output_weight,
        adapter_projection_input, adapter_projection_output, tuple(pieces), cap, replicas,
    )

    def flat(array):
        return array.reshape(-1, array.shape[-1])

    weights = (
        adapter_attention_input, adapter_projection_output, adapter_attention_output, adapter_projection_input,
        adapter_hidden_input, adapter_hidden_output, adapter_down_input, adapter_down_output,
    )
    first = (
        moment_attention_input, moment_projection_output, moment_attention_output, moment_projection_input,
        moment_hidden_input, moment_hidden_output, moment_down_input, moment_down_output,
    )
    second = (
        squared_attention_input, squared_projection_output, squared_attention_output, squared_projection_input,
        squared_hidden_input, squared_hidden_output, squared_down_input, squared_down_output,
    )
    outs = adam(
        sequence_adapter, optimizer_steps, norm, block_out, grad_hidden, got, tuple(flat(w) for w in weights),
        (n * replicas,) * 2 + (replicas,) * 6, tuple(flat(m) for m in first), tuple(flat(s) for s in second),
        n, replicas,
    )
    results = [outs[0][None], outs[1][None], outs[2]]
    for a in (0, 2, 3, 1, 4, 5, 6, 7):
        for kind in range(4):
            results.append(outs[3 + 4 * a + kind].reshape(first[a].shape))
    return tuple(results)


def solution(mesh):
    return jax.shard_map(
        per_device,
        mesh=mesh,
        in_specs=(
            P("dp", "expert", None),
            P("dp", "expert", None),
            P(),
            P(),
            P(None, None, "expert"),
            P("expert", None),
            P("expert", None, None, None),
            P("expert", None, None),
            P("dp", "expert", None),
            P("dp", "expert", None),
            P(),
            P(),
            P(),
            P(None, None, None, "expert"),
            P(None, None, "expert"),
            P(),
            P("expert", None, None, None, None),
            P("expert", None, None, None, None),
            P("expert", None, None, None),
            P("expert", None, None, None),
            P(None, None, None, ("dp", "expert")),
            P(None, None, None, ("expert", "dp")),
            P(None, None, ("expert", "dp")),
            P(None, None, ("dp", "expert")),
            P("expert", None, None, None, "dp"),
            P("expert", None, None, None, "dp"),
            P("expert", None, None, "dp"),
            P("expert", None, None, "dp"),
            P(None, None, None, ("dp", "expert")),
            P(None, None, None, ("expert", "dp")),
            P(None, None, ("expert", "dp")),
            P(None, None, ("dp", "expert")),
            P("expert", None, None, None, "dp"),
            P("expert", None, None, None, "dp"),
            P("expert", None, None, "dp"),
            P("expert", None, None, "dp"),
        ),
        out_specs=(
            P("dp", "expert", None),
            P("dp", "expert", None),
            P(),
            P(None, None, None, ("dp", "expert")),
            P(None, None, None, ("dp", "expert")),
            P(None, None, None, ("dp", "expert")),
            P(None, None, None, ("dp", "expert")),
            P(None, None, None, ("expert", "dp")),
            P(None, None, None, ("expert", "dp")),
            P(None, None, None, ("expert", "dp")),
            P(None, None, None, ("expert", "dp")),
            P(None, None, ("expert", "dp")),
            P(None, None, ("expert", "dp")),
            P(None, None, ("expert", "dp")),
            P(None, None, ("expert", "dp")),
            P(None, None, ("dp", "expert")),
            P(None, None, ("dp", "expert")),
            P(None, None, ("dp", "expert")),
            P(None, None, ("dp", "expert")),
            P("expert", None, None, None, "dp"),
            P("expert", None, None, None, "dp"),
            P("expert", None, None, None, "dp"),
            P("expert", None, None, None, "dp"),
            P("expert", None, None, None, "dp"),
            P("expert", None, None, None, "dp"),
            P("expert", None, None, None, "dp"),
            P("expert", None, None, None, "dp"),
            P("expert", None, None, "dp"),
            P("expert", None, None, "dp"),
            P("expert", None, None, "dp"),
            P("expert", None, None, "dp"),
            P("expert", None, None, "dp"),
            P("expert", None, None, "dp"),
            P("expert", None, None, "dp"),
            P("expert", None, None, "dp"),
        ),
        check_vma=False,
    )
```

```python
import functools

import jax
import jax.numpy as jnp
from jax import lax
from jax.experimental import pallas as pl
from jax.experimental.pallas import tpu as pltpu
from jax.sharding import PartitionSpec as P


single = jnp.float32
brain = jnp.bfloat16
HEAD = 128
TILE = 256
CHUNKS = 4
ORDER = [k + j * (CHUNKS // 2) for k in range(CHUNKS // 2) for j in range(2)]
GATHER_SENDS = CHUNKS * 7
SCATTER_SEMS = CHUNKS * 7
norm_eps = 1e-05
VMEM_ALL = 67043328


def dot(a, b, left=1, right=0):
    return lax.dot_general(a, b, (((left,), (right,)), ((), ())), preferred_element_type=single)


def peers():
    me = lax.axis_index("expert")
    core = me + 1 - 2 * (me % 2)
    across = me + 2 - 4 * ((me // 2) % 2)
    along = me + 4 - 8 * (me // 4)
    return me, core, across, along


def greet():
    me, core, across, along = peers()
    barrier = pltpu.get_barrier_semaphore()
    for peer in (core, across, along):
        pl.semaphore_signal(barrier, inc=1, device_id={"expert": peer})
    pl.semaphore_wait(barrier, 3)


class Mover:
    def __init__(self, send_sem, recv_sem):
        self.send_sem, self.recv_sem = send_sem, recv_sem
        self.me, self.core, self.across, self.along = peers()
        self.far = self.across + self.along - self.me
        self.count = 0
        self.waiting = []

    def go(self, src, dst, recv, peer):
        pltpu.make_async_remote_copy(
            src_ref=src, dst_ref=dst, send_sem=self.send_sem.at[self.count],
            recv_sem=self.recv_sem.at[recv], device_id={"expert": peer},
        ).start()
        self.count += 1

    def later(self, args):
        self.waiting.append(args)
        if len(self.waiting) > 1:
            self.waiting.pop(0)()

    def flush(self):
        while self.waiting:
            self.waiting.pop(0)()

    def got(self, view, recv):
        pltpu.make_async_remote_copy(
            src_ref=view, dst_ref=view, send_sem=self.send_sem.at[0], recv_sem=self.recv_sem.at[recv],
            device_id={"expert": self.core},
        ).wait_recv()

    def drain(self):
        view = self.sample()
        for i in range(self.count):
            pltpu.make_async_remote_copy(
                src_ref=view, dst_ref=view, send_sem=self.send_sem.at[i], recv_sem=self.recv_sem.at[0],
                device_id={"expert": self.core},
            ).wait_send()

    def beside(self, block):
        return block + 1 - 2 * (self.me % 2)


class Gather(Mover):
    def __init__(self, out, send_sem, recv_sem):
        super().__init__(send_sem, recv_sem)
        self.out = out
        self.size = out.shape[1] // CHUNKS

    def sample(self):
        return self.out.at[0, pl.ds(0, self.size)]

    def move(self, block, k, peer):
        view = self.out.at[block, pl.ds(k * self.size, self.size)]
        self.go(view, view, block * CHUNKS + k, peer)

    def arrive(self, block, k):
        self.got(self.out.at[block, pl.ds(k * self.size, self.size)], block * CHUNKS + k)

    def start_own(self, k):
        for peer in (self.across, self.along, self.core):
            self.move(self.me, k, peer)

    def start(self):
        for k in ORDER:
            self.start_own(k)

    def relay(self, i):
        k = ORDER[i]
        first_half = k < CHUNKS // 2
        self.arrive(self.across, k)
        if first_half:
            self.move(self.across, k, self.along)
        self.move(self.across, k, self.core)
        self.arrive(self.along, k)
        if not first_half:
            self.move(self.along, k, self.across)
        self.move(self.along, k, self.core)

    def relay_far(self, i):
        half = CHUNKS // 2
        for k in (i, i + half):
            self.arrive(self.far, k)
            self.move(self.far, k, self.core)

    def pair(self, block):
        for k in range(CHUNKS):
            self.arrive(self.beside(block), k)


class Scatter(Mover):
    def __init__(self, part, pair, half_x, half_y, from_x, from_y, send_sem, recv_sem, own=None):
        super().__init__(send_sem, recv_sem)
        self.part, self.pair, self.own = part, pair, own
        self.half_x, self.half_y, self.from_x, self.from_y = half_x, half_y, from_x, from_y
        self.order = (self.far, self.across, self.along, self.me)
        self.toks = pair.shape[1]
        self.size = self.toks // CHUNKS
        half = CHUNKS // 2
        self.hx = 4 * CHUNKS
        self.hy = self.hx + half
        self.fx = self.hy + half
        self.fy = self.fx + CHUNKS

    def sample(self):
        return self.pair.at[0, self.rows(0)]

    def rows(self, k):
        return pl.ds(k * self.size, self.size)

    def chunk(self, block, k):
        if len(self.part.shape) == 3:
            return self.part.at[block, self.rows(k)]
        return self.part.at[pl.ds(pl.multiple_of(block * self.toks + k * self.size, self.size), self.size)]

    def mine(self, i, k):
        view = self.chunk(self.order[i], k) if self.own is None else self.own.at[i, self.rows(k)]
        return view[...].astype(single)

    def give(self, i):
        other = self.beside(self.order[i])
        for k in range(CHUNKS):
            r = self.rows(k)
            self.go(self.chunk(other, k), self.pair.at[i, r], i * CHUNKS + k, self.core)

    def add(self, i, k, extra=None):
        r = self.rows(k)
        self.got(self.pair.at[i, r], i * CHUNKS + k)
        total = self.mine(i, k) + self.pair[i, r].astype(single)
        if extra is not None:
            ref, recv, k2 = extra
            r2 = self.rows(k2)
            self.got(ref.at[r2], recv)
            total = total + ref[r2].astype(single)
        self.pair[i, r] = total.astype(brain)

    def steps(self):
        half = CHUNKS // 2
        out = []

        def relay(i, k, to, row, recv, peer):
            self.later(lambda: self.go(self.pair.at[i, self.rows(k)], to.at[self.rows(row)], recv, peer))

        def one(k):
            self.add(0, k)
            relay(0, k, self.half_x, k, self.hx + k, self.across)
            self.add(0, k + half)
            relay(0, k + half, self.half_y, k, self.hy + k, self.along)

        def two(k):
            self.add(1, k)
            relay(1, k, self.from_x, k, self.fx + k, self.across)
            self.add(2, k + half)
            relay(2, k + half, self.from_y, k + half, self.fy + k + half, self.along)

        def three(k):
            self.add(1, k + half, (self.half_y, self.hy + k, k))
            relay(1, k + half, self.from_x, k + half, self.fx + k + half, self.across)
            self.add(2, k, (self.half_x, self.hx + k, k))
            relay(2, k, self.from_y, k, self.fy + k, self.along)

        for fn in (one, two, three):
            for k in range(half):
                out.append(functools.partial(fn, k))
        out.append(self.flush)
        return out

    def final(self, k):
        r = self.rows(k)
        self.got(self.pair.at[3, r], 3 * CHUNKS + k)
        total = self.mine(3, k) + self.pair[3, r].astype(single)
        self.got(self.from_x.at[r], self.fx + k)
        total = total + self.from_x[r].astype(single)
        self.got(self.from_y.at[r], self.fy + k)
        return total + self.from_y[r].astype(single)


def scatter_scratch(rows, cols):
    return [
        pltpu.VMEM((4, rows, cols), brain),
        pltpu.VMEM((rows // 2, cols), brain),
        pltpu.VMEM((rows // 2, cols), brain),
        pltpu.VMEM((rows, cols), brain),
        pltpu.VMEM((rows, cols), brain),
        pltpu.SemaphoreType.DMA((SCATTER_SEMS,)),
        pltpu.SemaphoreType.DMA((SCATTER_SEMS,)),
    ]


def gather_scratch(n):
    return [pltpu.SemaphoreType.DMA((GATHER_SENDS,)), pltpu.SemaphoreType.DMA((n * CHUNKS,))]


def rms(values, gain):
    return values * lax.rsqrt(jnp.mean(values * values, axis=-1, keepdims=True) + norm_eps) * gain


def fetch(src, dst, sem):
    copy = pltpu.make_async_copy(src, dst, sem)
    copy.start()
    return copy


def drive(count, body, events):
    def step(i, carry):
        body(i)
        for at, actions in events.items():

            @pl.when(i == at)
            def _(actions=actions):
                for action in actions:
                    action()

        return carry

    lax.fori_loop(0, count, step, 0)


def slots_of(denseall_ref, me, experts, dense, place):
    blocks, toks = denseall_ref.shape[0], denseall_ref.shape[2]
    for b in range(blocks):
        for e in range(experts):
            at = experts * b + e
            dense[at : at + 1, :] = denseall_ref[b, pl.ds(experts * me + e, 1), :]
    upper = (
        lax.broadcasted_iota(jnp.int32, (toks, toks), 0) < lax.broadcasted_iota(jnp.int32, (toks, toks), 1)
    ).astype(single).astype(brain)
    chosen = dense[...] > 0.0
    before = dot(chosen.astype(single).astype(brain), upper)
    place[...] = jnp.where(chosen, before, -1.0)


def picks(place, b, cap, experts):
    rows = lax.broadcasted_iota(jnp.int32, (cap, place.shape[1]), 0).astype(single)
    return [(place[pl.ds(experts * b + e, 1), :] == rows).astype(single) for e in range(experts)]


def weigh(place, dense, weight, b, cap, experts):
    for e, sel in enumerate(picks(place, b, cap, experts)):
        w = jnp.sum(sel * dense[pl.ds(experts * b + e, 1), :], axis=1, keepdims=True)
        weight[e, pl.ds(pl.multiple_of(b * cap, 16), cap), :] = w


def take(place, block, rows, b, cap):
    experts = rows.shape[0]
    both = jnp.concatenate([s.astype(brain) for s in picks(place, b, cap, experts)], axis=0)
    got = dot(both, block).astype(brain)
    at = pl.ds(pl.multiple_of(b * cap, 16), cap)
    for e in range(experts):
        rows[e, at, :] = got[e * cap : (e + 1) * cap]


def combined(place, rows, b, cap, apart):
    experts = rows.shape[0] // apart
    both = jnp.concatenate([s.astype(brain) for s in picks(place, b, cap, experts)], axis=0)
    parts = [rows[pl.ds(pl.multiple_of(e * apart + b * cap, 16), cap), :] for e in range(experts)]
    return dot(both, jnp.concatenate(parts, axis=0), 0, 0).astype(brain)


def two(p, toks):
    return pl.ds(pl.multiple_of(p * 2 * toks, 2 * toks), 2 * toks)


def meet(n, replicas, with_dp):
    me, rep = lax.axis_index("expert"), lax.axis_index("dp")
    barrier = pltpu.get_barrier_semaphore()
    for j in range(1, n):
        pl.semaphore_signal(barrier, inc=1, device_id={"expert": (me + j) % n})
    if with_dp:
        for j in range(1, replicas):
            pl.semaphore_signal(barrier, inc=1, device_id={"dp": (rep + j) % replicas})
    pl.semaphore_wait(barrier, n - 1 + (replicas - 1 if with_dp else 0))


def front_kernel(
    cap, ids_ref, hid_ref, top_ref, routes_ref, gates_ref, gain_ref, gain2_ref,
    w_hbm, a_hbm, b_hbm, wo_hbm, pa_hbm, pb_hbm, dn_hbm, da_hbm, db_hbm,
    low_ref, lse_ref, orank_ref, gdr_ref, place, weight, seq_hbm, proj_hbm, mixed_hbm, resid_hbm, x_hbm, g_hbm, ga_hbm,
    part, seq_ref, proj_ref, mixed_ref, topseq_ref, resid_ref, moe_ref, x_rows, g_rows, ga,
    w_ref, a_all, b_all, wo_ref, pa_all, pb_all, dn, da_all, db_all, a_ref, b_ref, mydense, dense, denseall_ref,
    load_sem, save_sem, *sems,
):
    toks, width = hid_ref.shape
    span = w_ref.shape[2]
    heads = span // HEAD
    n = seq_ref.shape[0]
    length = toks * n
    experts, hidden = dn.shape[0], dn.shape[1]
    loads = [
        fetch(src, dst, load_sem.at[i])
        for i, (src, dst) in enumerate(
            (
                (w_hbm, w_ref), (a_hbm, a_all), (b_hbm, b_all), (pa_hbm, pa_all), (pb_hbm, pb_all), (wo_hbm, wo_ref),
                (da_hbm, da_all), (db_hbm, db_all), (dn_hbm, dn),
            )
        )
    ]
    seq_g = Gather(seq_ref, sems[0], sems[1])
    top_g = Gather(topseq_ref, sems[2], sems[3])
    moe_g = Gather(moe_ref, sems[4], sems[5])
    red = Scatter(part, *sems[6:13])
    dsend, drecv = sems[13:15]
    me = seq_g.me
    slot = ids_ref[lax.axis_index("dp")]
    saves = []

    def save(src, dst):
        saves.append(fetch(src, dst, save_sem.at[len(saves)]))

    seq_ref[me] = rms(hid_ref[...].astype(single), gain_ref[...]).astype(brain)
    topseq_ref[me] = top_ref[...]
    choices = lax.broadcasted_iota(jnp.int32, (mydense.shape[0], toks), 0)
    table = jnp.zeros(mydense.shape, single)
    for k in range(routes_ref.shape[0]):
        table = table + jnp.where(routes_ref[k : k + 1, :] == choices, gates_ref[k : k + 1, :], 0.0)
    mydense[...] = table
    denseall_ref[me] = table
    meet(n, 1, False)
    seq_g.start()

    def dense_copy(j):
        return pltpu.make_async_remote_copy(
            src_ref=mydense, dst_ref=denseall_ref.at[me], send_sem=dsend.at[j - 1], recv_sem=drecv.at[me],
            device_id={"expert": (me + j) % n},
        )

    for j in range(1, n):
        dense_copy(j).start()
    for copy in loads[:3]:
        copy.wait()
    b_ref[...] = jnp.zeros_like(b_ref)
    for j in range(3):
        a_ref[16 * j : 16 * j + 16, :] = a_all[j, slot]
        b_ref[j, 16 * j : 16 * j + 16, :] = b_all[j, slot]

    def qkv(block):
        p = block // 2
        at = two(p, toks)
        low_ref[at, :] = dot(seq_ref[pl.ds(2 * p, 2)].reshape(2 * toks, width), a_ref[...], 1, 1).astype(brain)

        def third(j, carry):
            both = seq_ref[pl.ds(2 * p, 2)].reshape(2 * toks, width)
            proj_ref[j, at, :] = (dot(both, w_ref[j]) + dot(low_ref[at, :], b_ref[j])).astype(brain)
            return carry

        lax.fori_loop(0, 3, third, 0)

    seq_g.pair(me)
    qkv(me)
    for i in range(CHUNKS):
        seq_g.relay(i)
    top_g.start()
    seq_g.pair(seq_g.across)
    qkv(seq_g.across)
    seq_g.relay_far(0)
    seq_g.pair(seq_g.along)
    qkv(seq_g.along)
    for i in range(1, CHUNKS // 2):
        seq_g.relay_far(i)
    seq_g.pair(seq_g.far)
    qkv(seq_g.far)
    save(seq_ref, seq_hbm)
    save(proj_ref, proj_hbm)

    scale = HEAD ** (-0.5)
    block = 256
    top_steps = [functools.partial(top_g.relay, i) for i in range(CHUNKS)]
    top_steps += [functools.partial(top_g.relay_far, i) for i in range(CHUNKS // 2)]

    for h in range(heads):
        at = slice(h * HEAD, (h + 1) * HEAD)

        def attend(i, h=h, at=at):
            r = pl.ds(pl.multiple_of(i * block, block), block)
            scores = dot(proj_ref[0, r, at], proj_ref[1, :, at], 1, 1) * scale
            peak = jnp.max(scores, axis=-1, keepdims=True)
            expo = jnp.exp(scores - peak)
            total = jnp.sum(expo, axis=-1, keepdims=True)
            probs = (expo * (1.0 / total)).astype(brain)
            mixed_ref[r, at] = dot(probs, proj_ref[2, :, at]).astype(brain)
            lse_ref[r, h : h + 1] = peak + jnp.log(total)

        now, top_steps = top_steps[:3], top_steps[3:]
        last = length // block - 1
        drive(length // block, attend, {0: now[:1], last - 1: now[1:2], last: now[2:]} if h == 0 else {1: now[:1]})
        if h:
            top_steps = now[1:] + top_steps
    for copy in loads[3:6]:
        copy.wait()

    for i in range(4):
        p = red.order[i] // 2
        at = two(p, toks)
        rank = dot(mixed_ref[at, :], pa_all[slot], 1, 1).astype(brain)
        orank_ref[at, :] = rank
        cols = min(1024, width)

        def project(c, carry, p=p, at=at):
            s = pl.ds(pl.multiple_of(c * cols, cols), cols)
            out = dot(mixed_ref[at, :], wo_ref[:, s]) + dot(orank_ref[at, :], pb_all[slot, :, s])
            part[pl.ds(2 * p, 2), :, s] = out.astype(brain).reshape(2, toks, cols)
            return carry

        lax.fori_loop(0, width // cols, project, 0)
        if i:
            red.give(i - 1)
    red.give(3)
    save(mixed_ref, mixed_hbm)
    steps = red.steps()
    for step in steps[:4]:
        step()
    top_steps.pop(0)()
    red.flush()
    for step in top_steps:
        step()
    for block_at in (me, top_g.across, top_g.along, top_g.far):
        top_g.pair(block_at)
    for j in range(1, n):
        src = (me + j) % n
        view = denseall_ref.at[src]
        pltpu.make_async_remote_copy(
            src_ref=view, dst_ref=view, send_sem=dsend.at[0], recv_sem=drecv.at[src], device_id={"expert": src}
        ).wait_recv()
    for j in range(1, n):
        dense_copy(j).wait_send()
    slots_of(denseall_ref, me, experts, dense, place)

    def top_rows(b):
        weigh(place, dense, weight, b, cap, experts)
        take(place, topseq_ref[b], g_rows, b, cap)

    drive(n, top_rows, {5: steps[4:5]})
    for copy in loads[6:]:
        copy.wait()

    def top_rank(e):
        gdr_ref[e] = (dot(g_rows[e], db_all[e, slot], 1, 1) * weight[e]).astype(brain)

    drive(experts, top_rank, {})
    half = n * cap // 2
    tiles = hidden // TILE

    def top_tile(t):
        e, f, m = t // (2 * tiles), t // 2 % tiles, t % 2
        at = pl.ds(pl.multiple_of(f * TILE, TILE), TILE)
        r = pl.ds(pl.multiple_of(m * half, 16), half)
        out = dot(g_rows[e, r, :], dn[e, at, :], 1, 1) * weight[e, r, :]
        ga[e, r, at] = (out + dot(gdr_ref[e, r, :], da_all[e, slot, :, at])).astype(brain)

    drive(2 * experts * tiles, top_tile, {0: steps[5:6], 1: steps[6:7]})
    save(g_rows, g_hbm)
    save(ga, ga_hbm)
    for k in ORDER:
        r = red.rows(k)
        resid = hid_ref[r].astype(single) + red.final(k)
        resid_ref[r] = resid
        moe_ref[me, r] = rms(resid, gain2_ref[...]).astype(brain)
        if k != ORDER[0]:
            moe_g.start_own(ORDER[ORDER.index(k) - 1])
    save(resid_ref, resid_hbm)
    moe_g.start_own(ORDER[-1])

    def moe_rows(block_at):
        p = block_at // 2

        def one(i, carry):
            take(place, moe_ref[2 * p + i], x_rows, 2 * p + i, cap)
            return carry

        lax.fori_loop(0, 2, one, 0)

    moe_g.pair(me)
    moe_rows(me)
    for i in range(CHUNKS):
        moe_g.relay(i)
    moe_g.pair(moe_g.across)
    moe_rows(moe_g.across)
    for i in range(CHUNKS // 2):
        moe_g.relay_far(i)
    moe_g.pair(moe_g.along)
    moe_rows(moe_g.along)
    moe_g.pair(moe_g.far)
    moe_rows(moe_g.far)
    save(x_rows, x_hbm)
    for mover in (seq_g, top_g, red, moe_g):
        mover.drain()
    for copy in saves:
        copy.wait()


def front(ids, hid, top, routes, gates, gain, gain2, w, a, b, wo, pa, pb, dn, da, db, n, cap, cid=0):
    toks, width = hid.shape
    span = w.shape[2]
    length = toks * n
    experts, hidden = dn.shape[0], dn.shape[1]
    rows = n * cap
    vm = pl.BlockSpec(memory_space=pltpu.VMEM)
    sm = pl.BlockSpec(memory_space=pltpu.SMEM)
    hb = pl.BlockSpec(memory_space=pl.ANY)
    f = lambda *s: jax.ShapeDtypeStruct(s, single)
    h = lambda *s: jax.ShapeDtypeStruct(s, brain)
    bv = lambda *s: pltpu.VMEM(s, brain)
    fv = lambda *s: pltpu.VMEM(s, single)
    whole = bv(n, toks, width)
    return pl.pallas_call(
        functools.partial(front_kernel, cap),
        out_shape=(
            h(length, 48), f(length, span // HEAD), h(length, 16), h(experts, rows, 16), f(n * experts, toks),
            f(experts, rows, 1),
            h(n, toks, width), h(3, length, span), h(length, span), f(toks, width),
            h(experts, rows, width), h(experts, rows, width), h(experts, rows, hidden),
        ),
        in_specs=[sm] + [vm] * 6 + [hb] * 9,
        out_specs=[vm] * 6 + [hb] * 7,
        scratch_shapes=[
            whole, whole, bv(3, length, span), bv(length, span), whole, fv(toks, width), whole,
            bv(experts, rows, width), bv(experts, rows, width), bv(experts, rows, hidden),
        ]
        + [pltpu.VMEM(v.shape, brain) for v in (w, a, b, wo, pa, pb, dn, da, db)]
        + [
            bv(48, width), bv(3, 48, span), fv(experts * n, toks), fv(n * experts, toks), fv(n, experts * n, toks),
            pltpu.SemaphoreType.DMA((9,)), pltpu.SemaphoreType.DMA((7,)),
        ]
        + gather_scratch(n) + gather_scratch(n) + gather_scratch(n) + scatter_scratch(toks, width)
        + [pltpu.SemaphoreType.DMA((n,)), pltpu.SemaphoreType.DMA((n,))],
        compiler_params=pltpu.CompilerParams(collective_id=cid, has_side_effects=True, vmem_limit_bytes=VMEM_ALL),
        name="front",
    )(ids, hid, top, routes, gates, gain, gain2, w, a, b, wo, pa, pb, dn, da, db)


def moe_kernel(
    cap, replicas, ids_ref, place, weight, gdr_ref, x_hbm, g_hbm, ga_hbm, gu_hbm, ha_hbm, hb_hbm, da_hbm,
    drank_ref, gina_ref, gmidb_ref, gdna_ref, gdnb_ref, gpart_hbm, act_hbm,
    gu, x_rows, g_rows, ga, s_rows, act, gg, uu, irank, girank, ha_ref, hb_ref, da_ref,
    out_stage, pick_sem, x_sem, g_sem, ga_sem, gu_sem, act_sem, out_sem,
):
    experts, width, hidden = gu.shape[0], gu.shape[2], gu.shape[3]
    blocks = place.shape[0] // experts
    rows = x_rows.shape[1]
    tiles = hidden // TILE
    which = ids_ref[lax.axis_index("dp")]
    picked = []
    for e in range(experts):
        for i in range(2):
            picked.append((ha_hbm.at[e, i, which], ha_ref.at[e, pl.ds(16 * i, 16)]))
            picked.append((hb_hbm.at[e, i, which], hb_ref.at[e, i]))
        picked.append((da_hbm.at[e, which], da_ref.at[e]))

    def cols(f):
        return pl.ds(pl.multiple_of(f * TILE, TILE), TILE)

    x_copy = lambda e: pltpu.make_async_copy(x_hbm.at[e], x_rows.at[e], x_sem.at[e])
    g_copy = lambda e: pltpu.make_async_copy(g_hbm.at[e], g_rows.at[e], g_sem.at[e])
    ga_copy = lambda e: pltpu.make_async_copy(ga_hbm.at[e], ga.at[e], ga_sem.at[e])
    gu_copy = lambda e, f: pltpu.make_async_copy(
        gu_hbm.at[e, :, :, cols(f)], gu.at[e, :, :, cols(f)], gu_sem.at[e, f]
    )
    act_copy = lambda e: pltpu.make_async_copy(act.at[e], act_hbm.at[e], act_sem.at[e])
    x_copy(0).start()
    picked = [fetch(s, d, pick_sem.at[i]) for i, (s, d) in enumerate(picked)]
    for e in range(experts):
        for f in range(tiles):
            gu_copy(e, f).start()
            if f == 0:
                ga_copy(e).start()
        if e + 1 < experts:
            x_copy(e + 1).start()
        g_copy(e).start()
    for copy in picked:
        copy.wait()

    def expert(e, carry):
        x_copy(e).wait()
        irank[...] = dot(x_rows[e], ha_ref[e], 1, 1).astype(brain)
        ga_copy(e).wait()

        def tile(f, c):
            at = cols(f)
            gu_copy(e, f).wait()
            gate = dot(x_rows[e], gu[e, 0, :, at]) + dot(irank[:, :16], hb_ref[e, 0, :, at])
            up = dot(x_rows[e], gu[e, 1, :, at]) + dot(irank[:, 16:], hb_ref[e, 1, :, at])
            back = ga[e, :, at].astype(single)
            sig = jax.nn.sigmoid(gate)
            swish = gate * sig
            act[e, :, at] = (swish * up).astype(brain)
            gg[:, at] = (back * up * sig * (1.0 + gate * (1.0 - sig))).astype(brain)
            uu[:, at] = (back * swish).astype(brain)
            return c

        lax.fori_loop(0, tiles, tile, 0)
        act_copy(e).start()
        drank_ref[e] = dot(act[e], da_ref[e], 1, 1).astype(brain)
        girank[:, :16] = dot(gg[...], hb_ref[e, 0], 1, 1).astype(brain)
        girank[:, 16:] = dot(uu[...], hb_ref[e, 1], 1, 1).astype(brain)

        def deal(ref, row, value):
            piece = value.shape[1] // replicas
            at = pl.ds(pl.multiple_of(row, 16), value.shape[0])
            for d in range(replicas):
                ref[d, at, :] = value[:, d * piece : (d + 1) * piece].astype(brain)

        deal(gdna_ref, e * 16, dot(gdr_ref[e], act[e], 0, 0))
        deal(gmidb_ref, e * 32, dot(irank[:, :16], gg[...], 0, 0))
        deal(gmidb_ref, e * 32 + 16, dot(irank[:, 16:], uu[...], 0, 0))
        deal(gina_ref, e * 32, dot(girank[...], x_rows[e], 0, 0))
        g_copy(e).wait()
        deal(gdnb_ref, e * 16, dot((drank_ref[e].astype(single) * weight[e]).astype(brain), g_rows[e], 0, 0))

        def slots(d, c):
            at = cols(d)
            s = dot(gg[...], gu[e, 0, at, :], 1, 1) + dot(uu[...], gu[e, 1, at, :], 1, 1)
            s_rows[pl.ds(pl.multiple_of(e * rows, 16), rows), at] = (s + dot(girank[...], ha_ref[e, :, at])).astype(brain)
            return c

        lax.fori_loop(0, width // TILE, slots, 0)
        return carry

    lax.fori_loop(0, experts, expert, 0)
    out_copy = lambda b: pltpu.make_async_copy(out_stage.at[b % 2], gpart_hbm.at[b], out_sem.at[b % 2])

    def combine(b, carry):
        @pl.when(b >= 2)
        def _():
            out_copy(b - 2).wait()

        out_stage[b % 2] = combined(place, s_rows, b, cap, rows)
        out_copy(b).start()
        return carry

    lax.fori_loop(0, blocks, combine, 0)
    for b in (blocks - 2, blocks - 1):
        out_copy(b).wait()
    for e in range(experts):
        act_copy(e).wait()


def moe(ids, place, weight, gdr, x, g, ga, gu, ha, hb, da, cap, replicas):
    experts, rows, width = x.shape
    blocks, toks = place.shape[0] // experts, place.shape[1]
    hidden = gu.shape[3]
    rank = da.shape[2]
    vm = pl.BlockSpec(memory_space=pltpu.VMEM)
    sm = pl.BlockSpec(memory_space=pltpu.SMEM)
    hb_ = pl.BlockSpec(memory_space=pl.ANY)
    h = lambda *s: jax.ShapeDtypeStruct(s, brain)
    bv = lambda *s: pltpu.VMEM(s, brain)
    fv = lambda *s: pltpu.VMEM(s, single)
    dma = pltpu.SemaphoreType.DMA
    return pl.pallas_call(
        functools.partial(moe_kernel, cap, replicas),
        out_shape=(
            h(experts, rows, rank),
            h(replicas, experts * 2 * rank, width // replicas), h(replicas, experts * 2 * rank, hidden // replicas),
            h(replicas, experts * rank, hidden // replicas), h(replicas, experts * rank, width // replicas),
            h(blocks, toks, width), h(experts, rows, hidden),
        ),
        in_specs=[sm, vm, vm, vm] + [hb_] * 7,
        out_specs=[vm] * 5 + [hb_] * 2,
        scratch_shapes=[
            bv(*gu.shape), bv(*x.shape), bv(*x.shape), bv(*ga.shape), bv(experts * rows, width), bv(*ga.shape),
            bv(rows, hidden), bv(rows, hidden), bv(rows, 2 * rank), bv(rows, 2 * rank), bv(experts, 2 * rank, width),
            bv(experts, 2, rank, hidden), bv(experts, rank, hidden), bv(2, toks, width),
            dma((5 * experts,)), dma((experts,)), dma((experts,)), dma((experts,)), dma((experts, hidden // TILE)),
            dma((experts,)), dma((2,)),
        ],
        compiler_params=pltpu.CompilerParams(vmem_limit_bytes=VMEM_ALL),
        name="moe",
    )(ids, place, weight, gdr, x, g, ga, gu, ha, hb, da)


ADAPTERS = 8
RANK = 16
CLIP = 256.0
beta_one = 0.9
beta_two = 0.95
learn_rate = 0.02
weight_decay = 0.1
adam_eps = 1e-08


def norm_back(values, gain, grad):
    inverse = lax.rsqrt(jnp.mean(values * values, axis=-1, keepdims=True) + norm_eps)
    scaled = grad * gain
    return inverse * scaled - values * (
        inverse * inverse * inverse * jnp.mean(scaled * values, axis=-1, keepdims=True)
    )


def back_kernel(
    cap, replicas,
    ids_ref, hid_ref, top_ref, gain_ref, gain2_ref, low_ref, lse_ref, orank_ref, place, weight, drank_ref,
    resid_hbm, seq_hbm, proj_hbm, mixed_hbm, gpart_hbm, act_hbm, dn_hbm, db_hbm,
    w_hbm, a_hbm, b_hbm, wo_hbm, pa_hbm, pb_hbm, gina_hbm, gmidb_hbm, gdna_hbm, gdnb_hbm,
    out_ref, gh_ref, norm_ref, shared_got, got_qb, got_oa, got_ina, got_midb, got_dna, got_dnb,
    resid_ref, proj_ref, mixed_ref, own_g, ypart, act, dn, db_all, part,
    w_ref, a_all, b_all, wo_ref, pa_all, pb_all, a_ref,
    bf, gres, gmix, grank, gproj, glow, gk, gv,
    gqb_ref, goa_ref, shared_ref, shared_in, shared_mid, tot_e, tot_d, mine, load_sem, own_sem,
    sh_send, sh_recv, mid_send, mid_recv, p_send, p_recv, t_send, t_recv, *sems,
):
    toks, width = hid_ref.shape
    span = w_ref.shape[2]
    heads = span // HEAD
    experts = dn.shape[0]
    n = place.shape[0] // experts
    length = toks * n
    red = Scatter(gpart_hbm, *sems[0:7], own=own_g)
    redy = Scatter(ypart, *sems[7:14])
    redn = Scatter(part, *sems[14:21])
    bf_g = Gather(bf, *sems[21:23])
    me = red.me
    rep = lax.axis_index("dp")
    slot = ids_ref[rep]
    owns = [fetch(gpart_hbm.at[red.order[i]], own_g.at[i], own_sem.at[i]) for i in range(4)]
    loads = {}
    for i, (name, src, dst) in enumerate(
        (
            ("act", act_hbm, act), ("db", db_hbm, db_all), ("dn", dn_hbm, dn), ("resid", resid_hbm, resid_ref), ("wo", wo_hbm, wo_ref), ("pb", pb_hbm, pb_all), ("pa", pa_hbm, pa_all),
            ("mixed", mixed_hbm, mixed_ref), ("proj", proj_hbm, proj_ref), ("b", b_hbm, b_all), ("a", a_hbm, a_all),
            ("w", w_hbm, w_ref), ("ina", gina_hbm.at[rep], got_ina.at[rep]),
            ("midb", gmidb_hbm.at[rep], got_midb.at[rep]), ("dna", gdna_hbm.at[rep], got_dna.at[rep]),
            ("dnb", gdnb_hbm.at[rep], got_dnb.at[rep]),
        )
    ):
        loads[name] = fetch(src, dst, load_sem.at[i])

    def need(*names):
        for name in names:
            loads.pop(name).wait()

    meet(n, replicas, True)
    for i in range(4):
        red.give(i)
    pending = []

    def go(src, dst, send_sem, recv_sem, where):
        copy = pltpu.make_async_remote_copy(
            src_ref=src, dst_ref=dst, send_sem=send_sem, recv_sem=recv_sem, device_id=where
        )
        copy.start()
        pending.append(copy)

    def wait(view, recv_sem):
        pltpu.make_async_remote_copy(
            src_ref=view, dst_ref=view, send_sem=t_send.at[0], recv_sem=recv_sem, device_id={"expert": (me + 1) % n}
        ).wait_recv()

    got = (got_qb, got_oa, got_ina, got_midb, got_dna, got_dnb)

    def swap(i, source):
        for j in range(1, replicas):
            peer = (rep + j) % replicas
            go(
                source.at[peer], got[i].at[rep], p_send.at[i * replicas + j], p_recv.at[i * replicas + rep],
                {"dp": peer},
            )

    def swapped(i):
        for j in range(1, replicas):
            src = (rep + j) % replicas
            wait(got[i].at[src], p_recv.at[i * replicas + src])

    for copy in owns:
        copy.wait()
    steps = red.steps()
    for step in steps[:4]:
        step()
    for i, source in enumerate((gina_hbm, gmidb_hbm, gdna_hbm, gdnb_hbm)):
        swap(i + 2, source)
    red.flush()
    need("act", "db", "dn")
    tiles = width // TILE

    def y_tile(t):
        e = t // tiles
        s = pl.ds(pl.multiple_of(t % tiles * TILE, TILE), TILE)
        y = dot(act[e], dn[e, :, s]) + dot(drank_ref[e], db_all[e, slot, :, s])
        part[pl.ds(pl.multiple_of(e * n * cap, 16), n * cap), s] = (y * weight[e]).astype(brain)

    drive(experts * tiles, y_tile, {2: steps[4:5], 4: steps[5:6], 5: steps[6:7]})
    seq_ref = dn.at[0]
    loads["seq"] = fetch(seq_hbm, seq_ref, load_sem.at[len(loads) + 4])
    need("resid")
    for k in ORDER:
        r = red.rows(k)
        grad = top_ref[r].astype(single) + norm_back(resid_ref[r], gain2_ref[...], red.final(k))
        gres[r] = grad
        bf[me, r] = grad.astype(brain)
        if k != ORDER[0]:
            bf_g.start_own(ORDER[ORDER.index(k) - 1])
    bf_g.start_own(ORDER[-1])
    need("wo", "pb", "pa", "mixed")

    def mixed_grad(block):
        p = block // 2
        both = bf[pl.ds(2 * p, 2)].reshape(2 * toks, width)
        at = two(p, toks)
        rank = dot(both, pb_all[slot], 1, 1).astype(brain)
        grank[at, :] = rank
        gmix[at, :] = (dot(both, wo_ref[...], 1, 1) + dot(rank, pa_all[slot])).astype(brain)

    def y_block(block_at):
        ypart[block_at] = combined(place, part, block_at, cap, n * cap)

    bf_g.pair(me)
    mixed_grad(me)
    drive(
        n, y_block, {2: [functools.partial(bf_g.relay, 0)], 6: [functools.partial(bf_g.relay, 1)]},
    )
    for i in range(4):
        redy.give(i)
    for i in range(2, CHUNKS):
        bf_g.relay(i)
    ysteps = redy.steps()
    for step in ysteps[:4]:
        step()
    bf_g.pair(bf_g.across)
    mixed_grad(bf_g.across)
    redy.flush()
    bf_g.relay_far(0)
    bf_g.pair(bf_g.along)
    mixed_grad(bf_g.along)
    for i in range(1, CHUNKS // 2):
        bf_g.relay_far(i)
    bf_g.pair(bf_g.far)
    mixed_grad(bf_g.far)

    piece = span // replicas
    goa = dot(grank[...], mixed_ref[...], 0, 0)
    for d in range(replicas):
        goa_ref[d] = goa[:, d * piece : (d + 1) * piece].astype(brain)
    got_oa[rep] = goa_ref[rep]
    swap(1, goa_ref)

    need("proj")
    scale = HEAD ** (-0.5)
    block = 256
    for h in range(heads):
        at = slice(h * HEAD, (h + 1) * HEAD)
        gk[...] = jnp.zeros_like(gk)
        gv[...] = jnp.zeros_like(gv)

        def attend(i, h=h, at=at):
            r = pl.ds(pl.multiple_of(i * block, block), block)
            q, do = proj_ref[0, r, at], gmix[r, at]
            delta = jnp.sum(do.astype(single) * mixed_ref[r, at].astype(single), axis=-1, keepdims=True)
            probs = jnp.exp(dot(q, proj_ref[1, :, at], 1, 1) * scale - lse_ref[r, h : h + 1])
            gp = dot(do, proj_ref[2, :, at], 1, 1)
            gs = (probs * (gp - delta)).astype(brain)
            gproj[0, r, at] = (dot(gs, proj_ref[1, :, at]) * scale).astype(brain)
            gk[...] += dot(gs, q, 0, 0)
            gv[...] += dot(probs.astype(brain), do, 0, 0)

        drive(length // block, attend, {0: ysteps[4:5], 1: ysteps[5:6], 2: ysteps[6:]} if h == 0 else {})
        gproj[1, :, at] = (gk[...] * scale).astype(brain)
        gproj[2, :, at] = gv[...].astype(brain)

    need("a", "b", "w")
    for j in range(3):
        a_ref[16 * j : 16 * j + 16, :] = a_all[j, slot]
    nsteps = redn.steps()
    for i in range(4):
        p = redn.order[i] // 2
        at = two(p, toks)
        for j in range(3):
            glow[at, 16 * j : 16 * j + 16] = dot(gproj[j, at, :], b_all[j, slot], 1, 1).astype(brain)
        wide = min(1024, width)

        def normed_grad(c, carry, p=p, at=at):
            s = pl.ds(pl.multiple_of(c * wide, wide), wide)
            out = dot(glow[at, :], a_ref[:, s])
            for j in range(3):
                out = out + dot(gproj[j, at, :], w_ref[j, s, :], 1, 1)
            part[at, s] = out.astype(brain)
            return carry

        lax.fori_loop(0, width // wide, normed_grad, 0)
        if i:
            redn.give(i - 1)
        if i == 2:
            for step in nsteps[:2]:
                step()
    redn.give(3)
    for step in nsteps[2:4]:
        step()
    del nsteps[:4]

    thin = width // (n * replicas)

    def share(row, value, base):
        for c in range(value.shape[1] // thin):
            d, e = (base + c) // n, (base + c) % n
            shared_ref[e, row : row + value.shape[0], d * thin : (d + 1) * thin] = value[
                :, c * thin : (c + 1) * thin
            ].astype(brain)

    def advance():
        if nsteps:
            nsteps.pop(0)()

    for j in range(3):
        gqb = dot(low_ref[:, 16 * j : 16 * j + 16], gproj[j], 0, 0)
        for d in range(replicas):
            gqb_ref[d, 16 * j : 16 * j + 16, :] = gqb[:, d * piece : (d + 1) * piece].astype(brain)
    redn.flush()
    got_qb[rep] = gqb_ref[rep]
    swap(0, gqb_ref)
    need("seq")
    cols = 512
    for c in range(width // cols):
        s = slice(c * cols, (c + 1) * cols)
        share(0, dot(glow[...], seq_ref[:, s], 0, 0), c * cols // thin)
        share(48, dot(orank_ref[...], bf[:, :, s].reshape(length, cols), 0, 0), c * cols // thin)
        advance()
    shared_in[me] = shared_ref[me]
    for j in range(1, n):
        peer = (me + j) % n
        go(shared_ref.at[peer], shared_in.at[me], sh_send.at[j - 1], sh_recv.at[me], {"expert": peer})
    while nsteps:
        advance()

    def squares(i, source):
        rows = source.shape[1] // RANK

        def body(t, acc):
            at = pl.ds(pl.multiple_of(t // ADAPTERS * RANK, RANK), RANK)
            value = jnp.zeros((RANK, source.shape[2]), single)
            for s in range(replicas):
                value = value + source[s, at, :].astype(single) * jnp.where(ids_ref[s] == t % ADAPTERS, 1.0, 0.0)
            return acc + value * value

        return jnp.sum(
            lax.fori_loop(0, rows * ADAPTERS, body, jnp.zeros((RANK, source.shape[2]), single))
        )

    need("ina", "midb", "dna", "dnb")
    total = jnp.zeros((), single)
    for i in range(2, 6):
        swapped(i)
        total = total + squares(i, got[i])
    for j in range(1, n):
        src = (me + j) % n
        wait(shared_in.at[src], sh_recv.at[src])
    summed = shared_in[0].astype(single)
    for e in range(1, n):
        summed = summed + shared_in[e].astype(single)
    for d in range(replicas):
        shared_mid[d] = summed[:, d * thin : (d + 1) * thin].astype(brain)
    shared_got[rep] = shared_mid[rep]
    for j in range(1, replicas):
        peer = (rep + j) % replicas
        go(shared_mid.at[peer], shared_got.at[rep], mid_send.at[j], mid_recv.at[rep], {"dp": peer})
    for k in ORDER:
        r = redy.rows(k)
        out_ref[r] = (resid_ref[r] + redy.final(k)).astype(brain)
    for i in range(2):
        swapped(i)
        total = total + squares(i, got[i])
    for j in range(1, replicas):
        src = (rep + j) % replicas
        wait(shared_got.at[src], mid_recv.at[src])
    total = total + squares(0, shared_got)

    mine[0] = jnp.full(mine.shape[1:], total, single)
    tot_e[me] = mine[0]
    for j in range(1, n):
        go(mine.at[0], tot_e.at[me], t_send.at[j], t_recv.at[me], {"expert": (me + j) % n})
    for j in range(1, n):
        src = (me + j) % n
        wait(tot_e.at[src], t_recv.at[src])
    total = tot_e[0]
    for e in range(1, n):
        total = total + tot_e[e]
    mine[1] = total
    tot_d[rep] = mine[1]
    for j in range(1, replicas):
        go(mine.at[1], tot_d.at[rep], t_send.at[n + j], t_recv.at[n + rep], {"dp": (rep + j) % replicas})
    for k in ORDER:
        r = redn.rows(k)
        gh_ref[r] = gres[r] + norm_back(hid_ref[r].astype(single), gain_ref[...], redn.final(k))
    for j in range(1, replicas):
        src = (rep + j) % replicas
        wait(tot_d.at[src], t_recv.at[n + src])
    total = tot_d[0]
    for d in range(1, replicas):
        total = total + tot_d[d]
    norm_ref[...] = jnp.sqrt(total)
    for mover in (red, redy, redn, bf_g):
        mover.drain()
    for copy in pending:
        copy.wait_send()


def back(
    ids, hid, top, gain, gain2, low, lse, orank, place, weight, drank, resid, seq, proj, mixed, gpart, act, dn, db,
    w, a, b, wo, pa, pb, pieces, cap, replicas, cid=1,
):
    n, toks, width = seq.shape
    seq = seq.reshape(n * toks, width)
    experts, rows = act.shape[:2]
    span = w.shape[2]
    length = toks * n
    vm = pl.BlockSpec(memory_space=pltpu.VMEM)
    sm = pl.BlockSpec(memory_space=pltpu.SMEM)
    hb = pl.BlockSpec(memory_space=pl.ANY)
    f = lambda *s: jax.ShapeDtypeStruct(s, single)
    h = lambda *s: jax.ShapeDtypeStruct(s, brain)
    bv = lambda *s: pltpu.VMEM(s, brain)
    fv = lambda *s: pltpu.VMEM(s, single)
    dma = pltpu.SemaphoreType.DMA
    thin = width // (n * replicas)
    piece = span // replicas
    return pl.pallas_call(
        functools.partial(back_kernel, cap, replicas),
        out_shape=(
            h(toks, width), f(toks, width), f(8, 128), h(replicas, 64, thin), h(replicas, 48, piece),
            h(replicas, 16, piece),
        ) + tuple(h(*p.shape) for p in pieces),
        in_specs=[sm] + [vm] * 10 + [hb] * 18,
        out_specs=[vm] * 10,
        scratch_shapes=[
            fv(toks, width), bv(3, length, span), bv(length, span), bv(4, toks, width), bv(n, toks, width),
            bv(*act.shape), bv(*dn.shape), bv(*db.shape), bv(experts * rows, width),
        ]
        + [pltpu.VMEM(v.shape, brain) for v in (w, a, b, wo, pa, pb)]
        + [
            bv(48, width), bv(n, toks, width), fv(toks, width), bv(length, span), bv(length, 16),
            bv(3, length, span), bv(length, 48), fv(length, HEAD), fv(length, HEAD),
            bv(replicas, 48, piece), bv(replicas, 16, piece), bv(n, 64, replicas * thin), bv(n, 64, replicas * thin),
            bv(replicas, 64, thin), fv(n, 8, 128), fv(replicas, 8, 128), fv(2, 8, 128), dma((20,)), dma((4,)),
            dma((n,)), dma((n,)), dma((replicas,)), dma((replicas,)), dma((6 * replicas,)), dma((6 * replicas,)),
            dma((n + replicas,)), dma((n + replicas,)),
        ]
        + scatter_scratch(toks, width) * 3 + gather_scratch(n),
        compiler_params=pltpu.CompilerParams(collective_id=cid, has_side_effects=True, vmem_limit_bytes=VMEM_ALL),
        name="back",
    )(
        ids, hid, top, gain, gain2, low, lse, orank, place, weight, drank, resid, seq, proj, mixed, gpart, act, dn, db,
        w, a, b, wo, pa, pb, *pieces,
    )


def adam_kernel(n, replicas, groups, spans, adapter_ref, step_ref, norm_in, out_in, gh_in, *refs):
    got, refs = refs[:7], refs[7:]
    weight_hbm, first_hbm, second_hbm, refs = refs[:8], refs[8:16], refs[16:24], refs[24:]
    out_hbm, gh_hbm, norm_ref, result, refs = refs[0], refs[1], refs[2], refs[3:35], refs[35:]
    weight, first, second, kept, refs = refs[:8], refs[8:16], refs[16:24], refs[24:56], refs[56:]
    load_sem, save_sem = refs
    me, rep = lax.axis_index("expert"), lax.axis_index("dp")
    common = rep * n + me
    loads, saves = [], []
    for a in range(8):
        size, pieces = spans[a]
        index = common if pieces == n * replicas else rep
        start = index * size // weight[a].shape[1] * weight[a].shape[1]
        view = weight_hbm[a].at[:, pl.ds(pl.multiple_of(start, 128), weight[a].shape[1])]
        loads.append(
            [
                fetch(src, dst, load_sem.at[3 * a + k])
                for k, (src, dst) in enumerate(((view, weight[a]), (first_hbm[a], first[a]), (second_hbm[a], second[a])))
            ]
        )
    saves.append(fetch(out_in, out_hbm, save_sem.at[32]))
    saves.append(fetch(gh_in, gh_hbm, save_sem.at[33]))
    norm_ref[0] = norm_in[0, 0]
    factor = jnp.minimum(1.0, CLIP / norm_in[...])[0:1, 0:1]
    steps = jnp.full((8, 128), step_ref[0].astype(single), single)
    fix_first = (1.0 / (1.0 - jnp.exp(steps * jnp.log(jnp.full((8, 128), beta_one, single)))))[0:1, 0:1]
    fix_second = (1.0 / (1.0 - jnp.exp(steps * jnp.log(jnp.full((8, 128), beta_two, single)))))[0:1, 0:1]
    for a in (4, 7, 5, 6, 0, 2, 1, 3):
        for copy in loads[a]:
            copy.wait()
        source = got[max(a - 1, 0)]
        base = groups[0] if a == 1 else 0
        size, pieces = spans[a]
        window = weight[a].shape[1]
        index = common if pieces == n * replicas else rep

        def body(t, carry, a=a, source=source, base=base, size=size, window=window, index=index):
            rows = pl.ds(pl.multiple_of((base + t) * RANK, RANK), RANK)
            parts = [source[s, rows, :].astype(single) for s in range(replicas)]
            for adapter in range(ADAPTERS):
                at = pl.ds(pl.multiple_of((t * ADAPTERS + adapter) * RANK, RANK), RANK)
                grad = jnp.zeros((RANK, size), single)
                for s in range(replicas):
                    grad = grad + parts[s] * jnp.where(adapter_ref[s] == adapter, 1.0, 0.0)
                held = weight[a][at, :].astype(single)
                w = held[:, :size]
                for c in range(1, window // size):
                    w = jnp.where(index % (window // size) == c, held[:, c * size : (c + 1) * size], w)
                clipped = grad * factor
                f = beta_one * first[a][at, :] + (1.0 - beta_one) * clipped
                s = beta_two * second[a][at, :] + (1.0 - beta_two) * clipped * clipped
                kept[4 * a][at, :] = grad
                kept[4 * a + 1][at, :] = f
                kept[4 * a + 2][at, :] = s
                kept[4 * a + 3][at, :] = -learn_rate * (
                    f * fix_first / (jnp.sqrt(s * fix_second) + adam_eps) + weight_decay * w
                )
            return carry

        lax.fori_loop(0, groups[a], body, 0)
        for k in range(4):
            saves.append(fetch(kept[4 * a + k], result[4 * a + k], save_sem.at[4 * a + k]))
    for copy in saves:
        copy.wait()


def adam(adapters, steps, norm, block_out, gh, got, weight, pieces, first, second, n, replicas):
    spans = tuple((f.shape[1], p) for f, p in zip(first, pieces))
    groups = tuple(f.shape[0] // (ADAPTERS * RANK) for f in first)
    vm = pl.BlockSpec(memory_space=pltpu.VMEM)
    sm = pl.BlockSpec(memory_space=pltpu.SMEM)
    hb = pl.BlockSpec(memory_space=pl.ANY)
    f = lambda s: jax.ShapeDtypeStruct(s, single)
    dma = pltpu.SemaphoreType.DMA
    shapes = [t.shape for t in first]
    return pl.pallas_call(
        functools.partial(adam_kernel, n, replicas, groups, spans),
        out_shape=(jax.ShapeDtypeStruct(block_out.shape, brain), f(gh.shape), f((1,)))
        + tuple(f(s) for s in shapes for _ in range(4)),
        in_specs=[sm, sm, vm, vm, vm] + [vm] * 7 + [hb] * 24,
        out_specs=[hb, hb, sm] + [hb] * 32,
        scratch_shapes=[pltpu.VMEM((s[0], max(s[1], 128)), brain) for s in shapes]
        + [pltpu.VMEM(s, single) for s in shapes] * 2
        + [pltpu.VMEM(s, single) for s in shapes for _ in range(4)]
        + [dma((24,)), dma((34,))],
        compiler_params=pltpu.CompilerParams(vmem_limit_bytes=VMEM_ALL),
        name="adam",
    )(adapters, steps, norm, block_out, gh, *got, *weight, *first, *second)


def per_device(
    hidden,
    output_cotangent,
    attention_gain,
    expert_norm_gain,
    query_key_value_weight,
    output_weight,
    gate_up_weight,
    down_weight,
    token_experts,
    expert_gate_weight,
    sequence_adapter,
    optimizer_steps,
    adapter_attention_input,
    adapter_attention_output,
    adapter_projection_input,
    adapter_projection_output,
    adapter_hidden_input,
    adapter_hidden_output,
    adapter_down_input,
    adapter_down_output,
    moment_attention_input,
    moment_attention_output,
    moment_projection_input,
    moment_projection_output,
    moment_hidden_input,
    moment_hidden_output,
    moment_down_input,
    moment_down_output,
    squared_attention_input,
    squared_attention_output,
    squared_projection_input,
    squared_projection_output,
    squared_hidden_input,
    squared_hidden_output,
    squared_down_input,
    squared_down_output,
):
    n = lax.axis_size("expert")
    replicas = lax.axis_size("dp")
    toks, width = hidden.shape[1:]
    here = down_weight.shape[0]
    cap = min(toks, toks * token_experts.shape[2] * 5 // (4 * here * n))
    gain = attention_gain[None]
    gain2 = expert_norm_gain[None]
    hid, cot = hidden[0], output_cotangent[0]
    low, lse, orank, gdr, place, weight, seq, proj, mixed, resid, x_rows, g_rows, ga = front(
        sequence_adapter, hid, cot, token_experts[0].T, expert_gate_weight[0].T, gain, gain2, query_key_value_weight,
        adapter_attention_input, adapter_attention_output, output_weight, adapter_projection_input,
        adapter_projection_output, down_weight, adapter_down_input, adapter_down_output, n, cap,
    )
    drank, *pieces, gpart, act = moe(
        sequence_adapter, place, weight, gdr, x_rows, g_rows, ga, gate_up_weight, adapter_hidden_input,
        adapter_hidden_output, adapter_down_input, cap, replicas,
    )
    block_out, grad_hidden, norm, *got = back(
        sequence_adapter, hid, cot, gain, gain2, low, lse, orank, place, weight, drank, resid, seq, proj, mixed, gpart,
        act, down_weight, adapter_down_output,
        query_key_value_weight, adapter_attention_input, adapter_attention_output, output_weight,
        adapter_projection_input, adapter_projection_output, tuple(pieces), cap, replicas,
    )

    def flat(array):
        return array.reshape(-1, array.shape[-1])

    weights = (
        adapter_attention_input, adapter_projection_output, adapter_attention_output, adapter_projection_input,
        adapter_hidden_input, adapter_hidden_output, adapter_down_input, adapter_down_output,
    )
    first = (
        moment_attention_input, moment_projection_output, moment_attention_output, moment_projection_input,
        moment_hidden_input, moment_hidden_output, moment_down_input, moment_down_output,
    )
    second = (
        squared_attention_input, squared_projection_output, squared_attention_output, squared_projection_input,
        squared_hidden_input, squared_hidden_output, squared_down_input, squared_down_output,
    )
    outs = adam(
        sequence_adapter, optimizer_steps, norm, block_out, grad_hidden, got, tuple(flat(w) for w in weights),
        (n * replicas,) * 2 + (replicas,) * 6, tuple(flat(m) for m in first), tuple(flat(s) for s in second),
        n, replicas,
    )
    results = [outs[0][None], outs[1][None], outs[2]]
    for a in (0, 2, 3, 1, 4, 5, 6, 7):
        for kind in range(4):
            results.append(outs[3 + 4 * a + kind].reshape(first[a].shape))
    return tuple(results)


def solution(mesh):
    return jax.shard_map(
        per_device,
        mesh=mesh,
        in_specs=(
            P("dp", "expert", None),
            P("dp", "expert", None),
            P(),
            P(),
            P(None, None, "expert"),
            P("expert", None),
            P("expert", None, None, None),
            P("expert", None, None),
            P("dp", "expert", None),
            P("dp", "expert", None),
            P(),
            P(),
            P(),
            P(None, None, None, "expert"),
            P(None, None, "expert"),
            P(),
            P("expert", None, None, None, None),
            P("expert", None, None, None, None),
            P("expert", None, None, None),
            P("expert", None, None, None),
            P(None, None, None, ("dp", "expert")),
            P(None, None, None, ("expert", "dp")),
            P(None, None, ("expert", "dp")),
            P(None, None, ("dp", "expert")),
            P("expert", None, None, None, "dp"),
            P("expert", None, None, None, "dp"),
            P("expert", None, None, "dp"),
            P("expert", None, None, "dp"),
            P(None, None, None, ("dp", "expert")),
            P(None, None, None, ("expert", "dp")),
            P(None, None, ("expert", "dp")),
            P(None, None, ("dp", "expert")),
            P("expert", None, None, None, "dp"),
            P("expert", None, None, None, "dp"),
            P("expert", None, None, "dp"),
            P("expert", None, None, "dp"),
        ),
        out_specs=(
            P("dp", "expert", None),
            P("dp", "expert", None),
            P(),
            P(None, None, None, ("dp", "expert")),
            P(None, None, None, ("dp", "expert")),
            P(None, None, None, ("dp", "expert")),
            P(None, None, None, ("dp", "expert")),
            P(None, None, None, ("expert", "dp")),
            P(None, None, None, ("expert", "dp")),
            P(None, None, None, ("expert", "dp")),
            P(None, None, None, ("expert", "dp")),
            P(None, None, ("expert", "dp")),
            P(None, None, ("expert", "dp")),
            P(None, None, ("expert", "dp")),
            P(None, None, ("expert", "dp")),
            P(None, None, ("dp", "expert")),
            P(None, None, ("dp", "expert")),
            P(None, None, ("dp", "expert")),
            P(None, None, ("dp", "expert")),
            P("expert", None, None, None, "dp"),
            P("expert", None, None, None, "dp"),
            P("expert", None, None, None, "dp"),
            P("expert", None, None, None, "dp"),
            P("expert", None, None, None, "dp"),
            P("expert", None, None, None, "dp"),
            P("expert", None, None, None, "dp"),
            P("expert", None, None, None, "dp"),
            P("expert", None, None, "dp"),
            P("expert", None, None, "dp"),
            P("expert", None, None, "dp"),
            P("expert", None, None, "dp"),
            P("expert", None, None, "dp"),
            P("expert", None, None, "dp"),
            P("expert", None, None, "dp"),
            P("expert", None, None, "dp"),
        ),
        check_vma=False,
    )
```

```python
import functools

import jax
import jax.numpy as jnp
from jax import lax
from jax.experimental import pallas as pl
from jax.experimental.pallas import tpu as pltpu
from jax.sharding import PartitionSpec as P


single = jnp.float32
brain = jnp.bfloat16
HEAD = 128
TILE = 256
CHUNKS = 4
ORDER = [k + j * (CHUNKS // 2) for k in range(CHUNKS // 2) for j in range(2)]
GATHER_SENDS = CHUNKS * 7
SCATTER_SEMS = CHUNKS * 7
norm_eps = 1e-05
VMEM_ALL = 67043328


def dot(a, b, left=1, right=0):
    return lax.dot_general(a, b, (((left,), (right,)), ((), ())), preferred_element_type=single)


def peers():
    me = lax.axis_index("expert")
    core = me + 1 - 2 * (me % 2)
    across = me + 2 - 4 * ((me // 2) % 2)
    along = me + 4 - 8 * (me // 4)
    return me, core, across, along


def greet():
    me, core, across, along = peers()
    barrier = pltpu.get_barrier_semaphore()
    for peer in (core, across, along):
        pl.semaphore_signal(barrier, inc=1, device_id={"expert": peer})
    pl.semaphore_wait(barrier, 3)


class Mover:
    def __init__(self, send_sem, recv_sem):
        self.send_sem, self.recv_sem = send_sem, recv_sem
        self.me, self.core, self.across, self.along = peers()
        self.far = self.across + self.along - self.me
        self.count = 0
        self.waiting = []

    def go(self, src, dst, recv, peer):
        pltpu.make_async_remote_copy(
            src_ref=src, dst_ref=dst, send_sem=self.send_sem.at[self.count],
            recv_sem=self.recv_sem.at[recv], device_id={"expert": peer},
        ).start()
        self.count += 1

    def later(self, args):
        self.waiting.append(args)
        if len(self.waiting) > 1:
            self.waiting.pop(0)()

    def flush(self):
        while self.waiting:
            self.waiting.pop(0)()

    def got(self, view, recv):
        pltpu.make_async_remote_copy(
            src_ref=view, dst_ref=view, send_sem=self.send_sem.at[0], recv_sem=self.recv_sem.at[recv],
            device_id={"expert": self.core},
        ).wait_recv()

    def drain(self):
        view = self.sample()
        for i in range(self.count):
            pltpu.make_async_remote_copy(
                src_ref=view, dst_ref=view, send_sem=self.send_sem.at[i], recv_sem=self.recv_sem.at[0],
                device_id={"expert": self.core},
            ).wait_send()

    def beside(self, block):
        return block + 1 - 2 * (self.me % 2)


class Gather(Mover):
    def __init__(self, out, send_sem, recv_sem):
        super().__init__(send_sem, recv_sem)
        self.out = out
        self.size = out.shape[1] // CHUNKS

    def sample(self):
        return self.out.at[0, pl.ds(0, self.size)]

    def move(self, block, k, peer):
        view = self.out.at[block, pl.ds(k * self.size, self.size)]
        self.go(view, view, block * CHUNKS + k, peer)

    def arrive(self, block, k):
        self.got(self.out.at[block, pl.ds(k * self.size, self.size)], block * CHUNKS + k)

    def start_own(self, k):
        for peer in (self.across, self.along, self.core):
            self.move(self.me, k, peer)

    def start(self):
        for k in ORDER:
            self.start_own(k)

    def relay(self, i):
        k = ORDER[i]
        first_half = k < CHUNKS // 2
        self.arrive(self.across, k)
        if first_half:
            self.move(self.across, k, self.along)
        self.move(self.across, k, self.core)
        self.arrive(self.along, k)
        if not first_half:
            self.move(self.along, k, self.across)
        self.move(self.along, k, self.core)

    def relay_far(self, i):
        half = CHUNKS // 2
        for k in (i, i + half):
            self.arrive(self.far, k)
            self.move(self.far, k, self.core)

    def pair(self, block):
        for k in range(CHUNKS):
            self.arrive(self.beside(block), k)


class Scatter(Mover):
    def __init__(self, part, pair, half_x, half_y, from_x, from_y, send_sem, recv_sem, own=None):
        super().__init__(send_sem, recv_sem)
        self.part, self.pair, self.own = part, pair, own
        self.half_x, self.half_y, self.from_x, self.from_y = half_x, half_y, from_x, from_y
        self.order = (self.far, self.across, self.along, self.me)
        self.toks = pair.shape[1]
        self.size = self.toks // CHUNKS
        half = CHUNKS // 2
        self.hx = 4 * CHUNKS
        self.hy = self.hx + half
        self.fx = self.hy + half
        self.fy = self.fx + CHUNKS

    def sample(self):
        return self.pair.at[0, self.rows(0)]

    def rows(self, k):
        return pl.ds(k * self.size, self.size)

    def chunk(self, block, k):
        if len(self.part.shape) == 3:
            return self.part.at[block, self.rows(k)]
        return self.part.at[pl.ds(pl.multiple_of(block * self.toks + k * self.size, self.size), self.size)]

    def mine(self, i, k):
        view = self.chunk(self.order[i], k) if self.own is None else self.own.at[i, self.rows(k)]
        return view[...].astype(single)

    def give(self, i):
        other = self.beside(self.order[i])
        for k in range(CHUNKS):
            r = self.rows(k)
            self.go(self.chunk(other, k), self.pair.at[i, r], i * CHUNKS + k, self.core)

    def add(self, i, k, extra=None):
        r = self.rows(k)
        self.got(self.pair.at[i, r], i * CHUNKS + k)
        total = self.mine(i, k) + self.pair[i, r].astype(single)
        if extra is not None:
            ref, recv, k2 = extra
            r2 = self.rows(k2)
            self.got(ref.at[r2], recv)
            total = total + ref[r2].astype(single)
        self.pair[i, r] = total.astype(brain)

    def steps(self):
        half = CHUNKS // 2
        out = []

        def relay(i, k, to, row, recv, peer):
            self.later(lambda: self.go(self.pair.at[i, self.rows(k)], to.at[self.rows(row)], recv, peer))

        def one(k):
            self.add(0, k)
            relay(0, k, self.half_x, k, self.hx + k, self.across)
            self.add(0, k + half)
            relay(0, k + half, self.half_y, k, self.hy + k, self.along)

        def two(k):
            self.add(1, k)
            relay(1, k, self.from_x, k, self.fx + k, self.across)
            self.add(2, k + half)
            relay(2, k + half, self.from_y, k + half, self.fy + k + half, self.along)

        def three(k):
            self.add(1, k + half, (self.half_y, self.hy + k, k))
            relay(1, k + half, self.from_x, k + half, self.fx + k + half, self.across)
            self.add(2, k, (self.half_x, self.hx + k, k))
            relay(2, k, self.from_y, k, self.fy + k, self.along)

        for fn in (one, two, three):
            for k in range(half):
                out.append(functools.partial(fn, k))
        out.append(self.flush)
        return out

    def final(self, k):
        r = self.rows(k)
        self.got(self.pair.at[3, r], 3 * CHUNKS + k)
        total = self.mine(3, k) + self.pair[3, r].astype(single)
        self.got(self.from_x.at[r], self.fx + k)
        total = total + self.from_x[r].astype(single)
        self.got(self.from_y.at[r], self.fy + k)
        return total + self.from_y[r].astype(single)


def scatter_scratch(rows, cols):
    return [
        pltpu.VMEM((4, rows, cols), brain),
        pltpu.VMEM((rows // 2, cols), brain),
        pltpu.VMEM((rows // 2, cols), brain),
        pltpu.VMEM((rows, cols), brain),
        pltpu.VMEM((rows, cols), brain),
        pltpu.SemaphoreType.DMA((SCATTER_SEMS,)),
        pltpu.SemaphoreType.DMA((SCATTER_SEMS,)),
    ]


def gather_scratch(n):
    return [pltpu.SemaphoreType.DMA((GATHER_SENDS,)), pltpu.SemaphoreType.DMA((n * CHUNKS,))]


def rms(values, gain):
    return values * lax.rsqrt(jnp.mean(values * values, axis=-1, keepdims=True) + norm_eps) * gain


def fetch(src, dst, sem):
    copy = pltpu.make_async_copy(src, dst, sem)
    copy.start()
    return copy


def drive(count, body, events):
    def step(i, carry):
        body(i)
        for at, actions in events.items():

            @pl.when(i == at)
            def _(actions=actions):
                for action in actions:
                    action()

        return carry

    lax.fori_loop(0, count, step, 0)


def slots_of(denseall_ref, me, experts, dense, place):
    blocks, toks = denseall_ref.shape[0], denseall_ref.shape[2]
    for b in range(blocks):
        for e in range(experts):
            at = experts * b + e
            dense[at : at + 1, :] = denseall_ref[b, pl.ds(experts * me + e, 1), :]
    upper = (
        lax.broadcasted_iota(jnp.int32, (toks, toks), 0) < lax.broadcasted_iota(jnp.int32, (toks, toks), 1)
    ).astype(single).astype(brain)
    chosen = dense[...] > 0.0
    before = dot(chosen.astype(single).astype(brain), upper)
    place[...] = jnp.where(chosen, before, -1.0)


def picks(place, b, cap, experts):
    rows = lax.broadcasted_iota(jnp.int32, (cap, place.shape[1]), 0).astype(single)
    return [(place[pl.ds(experts * b + e, 1), :] == rows).astype(single) for e in range(experts)]


def weigh(place, dense, weight, b, cap, experts):
    for e, sel in enumerate(picks(place, b, cap, experts)):
        w = jnp.sum(sel * dense[pl.ds(experts * b + e, 1), :], axis=1, keepdims=True)
        weight[e, pl.ds(pl.multiple_of(b * cap, 16), cap), :] = w


def take(place, block, rows, b, cap):
    experts = rows.shape[0]
    both = jnp.concatenate([s.astype(brain) for s in picks(place, b, cap, experts)], axis=0)
    got = dot(both, block).astype(brain)
    at = pl.ds(pl.multiple_of(b * cap, 16), cap)
    for e in range(experts):
        rows[e, at, :] = got[e * cap : (e + 1) * cap]


def combined(place, rows, b, cap, apart):
    experts = rows.shape[0] // apart
    both = jnp.concatenate([s.astype(brain) for s in picks(place, b, cap, experts)], axis=0)
    parts = [rows[pl.ds(pl.multiple_of(e * apart + b * cap, 16), cap), :] for e in range(experts)]
    return dot(both, jnp.concatenate(parts, axis=0), 0, 0).astype(brain)


def two(p, toks):
    return pl.ds(pl.multiple_of(p * 2 * toks, 2 * toks), 2 * toks)


def meet(n, replicas, with_dp):
    me, rep = lax.axis_index("expert"), lax.axis_index("dp")
    barrier = pltpu.get_barrier_semaphore()
    for j in range(1, n):
        pl.semaphore_signal(barrier, inc=1, device_id={"expert": (me + j) % n})
    if with_dp:
        for j in range(1, replicas):
            pl.semaphore_signal(barrier, inc=1, device_id={"dp": (rep + j) % replicas})
    pl.semaphore_wait(barrier, n - 1 + (replicas - 1 if with_dp else 0))


def front_kernel(
    cap, ids_ref, hid_ref, top_ref, routes_ref, gates_ref, gain_ref, gain2_ref,
    w_hbm, a_hbm, b_hbm, wo_hbm, pa_hbm, pb_hbm, dn_hbm, da_hbm, db_hbm,
    low_ref, lse_ref, orank_ref, gdr_ref, place, weight, seq_hbm, proj_hbm, mixed_hbm, resid_hbm, x_hbm, g_hbm, ga_hbm,
    part, seq_ref, proj_ref, mixed_ref, topseq_ref, resid_ref, moe_ref, x_rows, g_rows, ga,
    w_ref, a_all, b_all, wo_ref, pa_all, pb_all, dn, da_all, db_all, a_ref, b_ref, mydense, dense, denseall_ref,
    load_sem, save_sem, *sems,
):
    toks, width = hid_ref.shape
    span = w_ref.shape[2]
    heads = span // HEAD
    n = seq_ref.shape[0]
    length = toks * n
    experts, hidden = dn.shape[0], dn.shape[1]
    loads = [
        fetch(src, dst, load_sem.at[i])
        for i, (src, dst) in enumerate(
            (
                (w_hbm, w_ref), (a_hbm, a_all), (b_hbm, b_all), (pa_hbm, pa_all), (pb_hbm, pb_all), (wo_hbm, wo_ref),
                (da_hbm, da_all), (db_hbm, db_all), (dn_hbm, dn),
            )
        )
    ]
    seq_g = Gather(seq_ref, sems[0], sems[1])
    top_g = Gather(topseq_ref, sems[2], sems[3])
    moe_g = Gather(moe_ref, sems[4], sems[5])
    red = Scatter(part, *sems[6:13])
    dsend, drecv = sems[13:15]
    me = seq_g.me
    slot = ids_ref[lax.axis_index("dp")]
    saves = []

    def save(src, dst):
        saves.append(fetch(src, dst, save_sem.at[len(saves)]))

    seq_ref[me] = rms(hid_ref[...].astype(single), gain_ref[...]).astype(brain)
    topseq_ref[me] = top_ref[...]
    choices = lax.broadcasted_iota(jnp.int32, (mydense.shape[0], toks), 0)
    table = jnp.zeros(mydense.shape, single)
    for k in range(routes_ref.shape[0]):
        table = table + jnp.where(routes_ref[k : k + 1, :] == choices, gates_ref[k : k + 1, :], 0.0)
    mydense[...] = table
    denseall_ref[me] = table
    meet(n, 1, False)
    seq_g.start()

    def dense_copy(j):
        return pltpu.make_async_remote_copy(
            src_ref=mydense, dst_ref=denseall_ref.at[me], send_sem=dsend.at[j - 1], recv_sem=drecv.at[me],
            device_id={"expert": (me + j) % n},
        )

    for j in range(1, n):
        dense_copy(j).start()
    for copy in loads[:3]:
        copy.wait()
    b_ref[...] = jnp.zeros_like(b_ref)
    for j in range(3):
        a_ref[16 * j : 16 * j + 16, :] = a_all[j, slot]
        b_ref[j, 16 * j : 16 * j + 16, :] = b_all[j, slot]

    def qkv(block):
        p = block // 2
        at = two(p, toks)
        low_ref[at, :] = dot(seq_ref[pl.ds(2 * p, 2)].reshape(2 * toks, width), a_ref[...], 1, 1).astype(brain)

        def third(j, carry):
            both = seq_ref[pl.ds(2 * p, 2)].reshape(2 * toks, width)
            proj_ref[j, at, :] = (dot(both, w_ref[j]) + dot(low_ref[at, :], b_ref[j])).astype(brain)
            return carry

        lax.fori_loop(0, 3, third, 0)

    seq_g.pair(me)
    qkv(me)
    for i in range(CHUNKS):
        seq_g.relay(i)
    top_g.start()
    seq_g.pair(seq_g.across)
    qkv(seq_g.across)
    seq_g.relay_far(0)
    seq_g.pair(seq_g.along)
    qkv(seq_g.along)
    for i in range(1, CHUNKS // 2):
        seq_g.relay_far(i)
    seq_g.pair(seq_g.far)
    qkv(seq_g.far)
    save(seq_ref, seq_hbm)
    save(proj_ref, proj_hbm)

    scale = HEAD ** (-0.5)
    block = 256
    top_steps = [functools.partial(top_g.relay, i) for i in range(CHUNKS)]
    top_steps += [functools.partial(top_g.relay_far, i) for i in range(CHUNKS // 2)]

    for h in range(heads):
        at = slice(h * HEAD, (h + 1) * HEAD)

        def attend(i, h=h, at=at):
            r = pl.ds(pl.multiple_of(i * block, block), block)
            scores = dot(proj_ref[0, r, at], proj_ref[1, :, at], 1, 1) * scale
            peak = jnp.max(scores, axis=-1, keepdims=True)
            expo = jnp.exp(scores - peak)
            total = jnp.sum(expo, axis=-1, keepdims=True)
            probs = (expo * (1.0 / total)).astype(brain)
            mixed_ref[r, at] = dot(probs, proj_ref[2, :, at]).astype(brain)
            lse_ref[r, h : h + 1] = peak + jnp.log(total)

        now, top_steps = top_steps[:3], top_steps[3:]
        last = length // block - 1
        drive(length // block, attend, {0: now[:1], last - 1: now[1:2], last: now[2:]} if h == 0 else {1: now[:1]})
        if h:
            top_steps = now[1:] + top_steps
    for copy in loads[3:6]:
        copy.wait()

    for i in range(4):
        p = red.order[i] // 2
        at = two(p, toks)
        rank = dot(mixed_ref[at, :], pa_all[slot], 1, 1).astype(brain)
        orank_ref[at, :] = rank
        cols = min(1024, width)

        def project(c, carry, p=p, at=at):
            s = pl.ds(pl.multiple_of(c * cols, cols), cols)
            out = dot(mixed_ref[at, :], wo_ref[:, s]) + dot(orank_ref[at, :], pb_all[slot, :, s])
            part[pl.ds(2 * p, 2), :, s] = out.astype(brain).reshape(2, toks, cols)
            return carry

        lax.fori_loop(0, width // cols, project, 0)
        if i:
            red.give(i - 1)
    red.give(3)
    save(mixed_ref, mixed_hbm)
    steps = red.steps()
    for step in steps[:4]:
        step()
    top_steps.pop(0)()
    red.flush()
    for step in top_steps:
        step()
    for block_at in (me, top_g.across, top_g.along, top_g.far):
        top_g.pair(block_at)
    for j in range(1, n):
        src = (me + j) % n
        view = denseall_ref.at[src]
        pltpu.make_async_remote_copy(
            src_ref=view, dst_ref=view, send_sem=dsend.at[0], recv_sem=drecv.at[src], device_id={"expert": src}
        ).wait_recv()
    for j in range(1, n):
        dense_copy(j).wait_send()
    slots_of(denseall_ref, me, experts, dense, place)

    def top_rows(b):
        weigh(place, dense, weight, b, cap, experts)
        take(place, topseq_ref[b], g_rows, b, cap)

    drive(n, top_rows, {5: steps[4:5]})
    for copy in loads[6:]:
        copy.wait()

    def top_rank(e):
        gdr_ref[e] = (dot(g_rows[e], db_all[e, slot], 1, 1) * weight[e]).astype(brain)

    drive(experts, top_rank, {})
    half = n * cap // 2
    tiles = hidden // TILE

    def top_tile(t):
        e, f, m = t // (2 * tiles), t // 2 % tiles, t % 2
        at = pl.ds(pl.multiple_of(f * TILE, TILE), TILE)
        r = pl.ds(pl.multiple_of(m * half, 16), half)
        out = dot(g_rows[e, r, :], dn[e, at, :], 1, 1) * weight[e, r, :]
        ga[e, r, at] = (out + dot(gdr_ref[e, r, :], da_all[e, slot, :, at])).astype(brain)

    drive(2 * experts * tiles, top_tile, {0: steps[5:6], 1: steps[6:7]})
    save(g_rows, g_hbm)
    save(ga, ga_hbm)
    for k in ORDER:
        r = red.rows(k)
        resid = hid_ref[r].astype(single) + red.final(k)
        resid_ref[r] = resid
        moe_ref[me, r] = rms(resid, gain2_ref[...]).astype(brain)
        if k != ORDER[0]:
            moe_g.start_own(ORDER[ORDER.index(k) - 1])
    save(resid_ref, resid_hbm)
    moe_g.start_own(ORDER[-1])

    def moe_rows(block_at):
        p = block_at // 2

        def one(i, carry):
            take(place, moe_ref[2 * p + i], x_rows, 2 * p + i, cap)
            return carry

        lax.fori_loop(0, 2, one, 0)
        at = pl.ds(pl.multiple_of(2 * p * cap, 16), 2 * cap)
        for e in range(experts):
            save(x_rows.at[e, at], x_hbm.at[e, at])

    moe_g.pair(me)
    moe_rows(me)
    for i in range(CHUNKS):
        moe_g.relay(i)
    moe_g.pair(moe_g.across)
    moe_rows(moe_g.across)
    for i in range(CHUNKS // 2):
        moe_g.relay_far(i)
    moe_g.pair(moe_g.along)
    moe_rows(moe_g.along)
    moe_g.pair(moe_g.far)
    moe_rows(moe_g.far)
    for mover in (seq_g, top_g, red, moe_g):
        mover.drain()
    for copy in saves:
        copy.wait()


def front(ids, hid, top, routes, gates, gain, gain2, w, a, b, wo, pa, pb, dn, da, db, n, cap, cid=0):
    toks, width = hid.shape
    span = w.shape[2]
    length = toks * n
    experts, hidden = dn.shape[0], dn.shape[1]
    rows = n * cap
    vm = pl.BlockSpec(memory_space=pltpu.VMEM)
    sm = pl.BlockSpec(memory_space=pltpu.SMEM)
    hb = pl.BlockSpec(memory_space=pl.ANY)
    f = lambda *s: jax.ShapeDtypeStruct(s, single)
    h = lambda *s: jax.ShapeDtypeStruct(s, brain)
    bv = lambda *s: pltpu.VMEM(s, brain)
    fv = lambda *s: pltpu.VMEM(s, single)
    whole = bv(n, toks, width)
    return pl.pallas_call(
        functools.partial(front_kernel, cap),
        out_shape=(
            h(length, 48), f(length, span // HEAD), h(length, 16), h(experts, rows, 16), f(n * experts, toks),
            f(experts, rows, 1),
            h(n, toks, width), h(3, length, span), h(length, span), f(toks, width),
            h(experts, rows, width), h(experts, rows, width), h(experts, rows, hidden),
        ),
        in_specs=[sm] + [vm] * 6 + [hb] * 9,
        out_specs=[vm] * 6 + [hb] * 7,
        scratch_shapes=[
            whole, whole, bv(3, length, span), bv(length, span), whole, fv(toks, width), whole,
            bv(experts, rows, width), bv(experts, rows, width), bv(experts, rows, hidden),
        ]
        + [pltpu.VMEM(v.shape, brain) for v in (w, a, b, wo, pa, pb, dn, da, db)]
        + [
            bv(48, width), bv(3, 48, span), fv(experts * n, toks), fv(n * experts, toks), fv(n, experts * n, toks),
            pltpu.SemaphoreType.DMA((9,)), pltpu.SemaphoreType.DMA((6 + 4 * experts,)),
        ]
        + gather_scratch(n) + gather_scratch(n) + gather_scratch(n) + scatter_scratch(toks, width)
        + [pltpu.SemaphoreType.DMA((n,)), pltpu.SemaphoreType.DMA((n,))],
        compiler_params=pltpu.CompilerParams(collective_id=cid, has_side_effects=True, vmem_limit_bytes=VMEM_ALL),
        name="front",
    )(ids, hid, top, routes, gates, gain, gain2, w, a, b, wo, pa, pb, dn, da, db)


def moe_kernel(
    cap, replicas, ids_ref, place, weight, gdr_ref, x_hbm, g_hbm, ga_hbm, gu_hbm, ha_hbm, hb_hbm, da_hbm,
    drank_ref, gina_ref, gmidb_ref, gdna_ref, gdnb_ref, gpart_hbm, act_hbm,
    gu, x_rows, g_rows, ga, s_rows, act, gg, uu, irank, girank, ha_ref, hb_ref, da_ref,
    out_stage, pick_sem, x_sem, g_sem, ga_sem, gu_sem, act_sem, out_sem,
):
    experts, width, hidden = gu.shape[0], gu.shape[2], gu.shape[3]
    blocks = place.shape[0] // experts
    rows = x_rows.shape[1]
    tiles = hidden // TILE
    which = ids_ref[lax.axis_index("dp")]
    picked = []
    for e in range(experts):
        for i in range(2):
            picked.append((ha_hbm.at[e, i, which], ha_ref.at[e, pl.ds(16 * i, 16)]))
            picked.append((hb_hbm.at[e, i, which], hb_ref.at[e, i]))
        picked.append((da_hbm.at[e, which], da_ref.at[e]))

    def cols(f):
        return pl.ds(pl.multiple_of(f * TILE, TILE), TILE)

    x_copy = lambda e: pltpu.make_async_copy(x_hbm.at[e], x_rows.at[e], x_sem.at[e])
    g_copy = lambda e: pltpu.make_async_copy(g_hbm.at[e], g_rows.at[e], g_sem.at[e])
    ga_copy = lambda e: pltpu.make_async_copy(ga_hbm.at[e], ga.at[e], ga_sem.at[e])
    gu_copy = lambda e, f: pltpu.make_async_copy(
        gu_hbm.at[e, :, :, cols(f)], gu.at[e, :, :, cols(f)], gu_sem.at[e, f]
    )
    act_copy = lambda e: pltpu.make_async_copy(act.at[e], act_hbm.at[e], act_sem.at[e])
    x_copy(0).start()
    picked = [fetch(s, d, pick_sem.at[i]) for i, (s, d) in enumerate(picked)]
    for e in range(experts):
        for f in range(tiles):
            gu_copy(e, f).start()
            if f == 0:
                ga_copy(e).start()
        if e + 1 < experts:
            x_copy(e + 1).start()
        g_copy(e).start()
    for copy in picked:
        copy.wait()

    def expert(e, carry):
        x_copy(e).wait()
        irank[...] = dot(x_rows[e], ha_ref[e], 1, 1).astype(brain)
        ga_copy(e).wait()

        def tile(f, c):
            at = cols(f)
            gu_copy(e, f).wait()
            gate = dot(x_rows[e], gu[e, 0, :, at]) + dot(irank[:, :16], hb_ref[e, 0, :, at])
            up = dot(x_rows[e], gu[e, 1, :, at]) + dot(irank[:, 16:], hb_ref[e, 1, :, at])
            back = ga[e, :, at].astype(single)
            sig = jax.nn.sigmoid(gate)
            swish = gate * sig
            act[e, :, at] = (swish * up).astype(brain)
            gg[:, at] = (back * up * sig * (1.0 + gate * (1.0 - sig))).astype(brain)
            uu[:, at] = (back * swish).astype(brain)
            return c

        lax.fori_loop(0, tiles, tile, 0)
        act_copy(e).start()
        drank_ref[e] = dot(act[e], da_ref[e], 1, 1).astype(brain)
        girank[:, :16] = dot(gg[...], hb_ref[e, 0], 1, 1).astype(brain)
        girank[:, 16:] = dot(uu[...], hb_ref[e, 1], 1, 1).astype(brain)

        def deal(ref, row, value):
            piece = value.shape[1] // replicas
            at = pl.ds(pl.multiple_of(row, 16), value.shape[0])
            for d in range(replicas):
                ref[d, at, :] = value[:, d * piece : (d + 1) * piece].astype(brain)

        deal(gdna_ref, e * 16, dot(gdr_ref[e], act[e], 0, 0))
        deal(gmidb_ref, e * 32, dot(irank[:, :16], gg[...], 0, 0))
        deal(gmidb_ref, e * 32 + 16, dot(irank[:, 16:], uu[...], 0, 0))
        deal(gina_ref, e * 32, dot(girank[...], x_rows[e], 0, 0))
        g_copy(e).wait()
        deal(gdnb_ref, e * 16, dot((drank_ref[e].astype(single) * weight[e]).astype(brain), g_rows[e], 0, 0))

        def slots(d, c):
            at = cols(d)
            s = dot(gg[...], gu[e, 0, at, :], 1, 1) + dot(uu[...], gu[e, 1, at, :], 1, 1)
            s_rows[pl.ds(pl.multiple_of(e * rows, 16), rows), at] = (s + dot(girank[...], ha_ref[e, :, at])).astype(brain)
            return c

        lax.fori_loop(0, width // TILE, slots, 0)
        return carry

    lax.fori_loop(0, experts, expert, 0)
    out_copy = lambda b: pltpu.make_async_copy(out_stage.at[b % 2], gpart_hbm.at[b], out_sem.at[b % 2])

    def combine(b, carry):
        @pl.when(b >= 2)
        def _():
            out_copy(b - 2).wait()

        out_stage[b % 2] = combined(place, s_rows, b, cap, rows)
        out_copy(b).start()
        return carry

    lax.fori_loop(0, blocks, combine, 0)
    for b in (blocks - 2, blocks - 1):
        out_copy(b).wait()
    for e in range(experts):
        act_copy(e).wait()


def moe(ids, place, weight, gdr, x, g, ga, gu, ha, hb, da, cap, replicas):
    experts, rows, width = x.shape
    blocks, toks = place.shape[0] // experts, place.shape[1]
    hidden = gu.shape[3]
    rank = da.shape[2]
    vm = pl.BlockSpec(memory_space=pltpu.VMEM)
    sm = pl.BlockSpec(memory_space=pltpu.SMEM)
    hb_ = pl.BlockSpec(memory_space=pl.ANY)
    h = lambda *s: jax.ShapeDtypeStruct(s, brain)
    bv = lambda *s: pltpu.VMEM(s, brain)
    fv = lambda *s: pltpu.VMEM(s, single)
    dma = pltpu.SemaphoreType.DMA
    return pl.pallas_call(
        functools.partial(moe_kernel, cap, replicas),
        out_shape=(
            h(experts, rows, rank),
            h(replicas, experts * 2 * rank, width // replicas), h(replicas, experts * 2 * rank, hidden // replicas),
            h(replicas, experts * rank, hidden // replicas), h(replicas, experts * rank, width // replicas),
            h(blocks, toks, width), h(experts, rows, hidden),
        ),
        in_specs=[sm, vm, vm, vm] + [hb_] * 7,
        out_specs=[vm] * 5 + [hb_] * 2,
        scratch_shapes=[
            bv(*gu.shape), bv(*x.shape), bv(*x.shape), bv(*ga.shape), bv(experts * rows, width), bv(*ga.shape),
            bv(rows, hidden), bv(rows, hidden), bv(rows, 2 * rank), bv(rows, 2 * rank), bv(experts, 2 * rank, width),
            bv(experts, 2, rank, hidden), bv(experts, rank, hidden), bv(2, toks, width),
            dma((5 * experts,)), dma((experts,)), dma((experts,)), dma((experts,)), dma((experts, hidden // TILE)),
            dma((experts,)), dma((2,)),
        ],
        compiler_params=pltpu.CompilerParams(vmem_limit_bytes=VMEM_ALL),
        name="moe",
    )(ids, place, weight, gdr, x, g, ga, gu, ha, hb, da)


ADAPTERS = 8
RANK = 16
CLIP = 256.0
beta_one = 0.9
beta_two = 0.95
learn_rate = 0.02
weight_decay = 0.1
adam_eps = 1e-08


def norm_back(values, gain, grad):
    inverse = lax.rsqrt(jnp.mean(values * values, axis=-1, keepdims=True) + norm_eps)
    scaled = grad * gain
    return inverse * scaled - values * (
        inverse * inverse * inverse * jnp.mean(scaled * values, axis=-1, keepdims=True)
    )


def back_kernel(
    cap, replicas,
    ids_ref, hid_ref, top_ref, gain_ref, gain2_ref, low_ref, lse_ref, orank_ref, place, weight, drank_ref,
    resid_hbm, seq_hbm, proj_hbm, mixed_hbm, gpart_hbm, act_hbm, dn_hbm, db_hbm,
    w_hbm, a_hbm, b_hbm, wo_hbm, pa_hbm, pb_hbm, gina_hbm, gmidb_hbm, gdna_hbm, gdnb_hbm,
    out_ref, gh_ref, norm_ref, shared_got, got_qb, got_oa, got_ina, got_midb, got_dna, got_dnb,
    resid_ref, proj_ref, mixed_ref, own_g, ypart, act, dn, db_all, part,
    w_ref, a_all, b_all, wo_ref, pa_all, pb_all, a_ref,
    bf, gres, gmix, grank, gproj, glow, gk, gv,
    gqb_ref, goa_ref, shared_ref, shared_in, shared_mid, tot_e, tot_d, mine, load_sem, own_sem,
    sh_send, sh_recv, mid_send, mid_recv, p_send, p_recv, t_send, t_recv, *sems,
):
    toks, width = hid_ref.shape
    span = w_ref.shape[2]
    heads = span // HEAD
    experts = dn.shape[0]
    n = place.shape[0] // experts
    length = toks * n
    red = Scatter(gpart_hbm, *sems[0:7], own=own_g)
    redy = Scatter(ypart, *sems[7:14])
    redn = Scatter(part, *sems[14:21])
    bf_g = Gather(bf, *sems[21:23])
    me = red.me
    rep = lax.axis_index("dp")
    slot = ids_ref[rep]
    owns = [fetch(gpart_hbm.at[red.order[i]], own_g.at[i], own_sem.at[i]) for i in range(4)]
    loads = {}
    for i, (name, src, dst) in enumerate(
        (
            ("act", act_hbm, act), ("db", db_hbm, db_all), ("dn", dn_hbm, dn), ("resid", resid_hbm, resid_ref), ("wo", wo_hbm, wo_ref), ("pb", pb_hbm, pb_all), ("pa", pa_hbm, pa_all),
            ("mixed", mixed_hbm, mixed_ref), ("proj", proj_hbm, proj_ref), ("b", b_hbm, b_all), ("a", a_hbm, a_all),
            ("w", w_hbm, w_ref), ("ina", gina_hbm.at[rep], got_ina.at[rep]),
            ("midb", gmidb_hbm.at[rep], got_midb.at[rep]), ("dna", gdna_hbm.at[rep], got_dna.at[rep]),
            ("dnb", gdnb_hbm.at[rep], got_dnb.at[rep]),
        )
    ):
        loads[name] = fetch(src, dst, load_sem.at[i])

    def need(*names):
        for name in names:
            loads.pop(name).wait()

    meet(n, replicas, True)
    for i in range(4):
        red.give(i)
    pending = []

    def go(src, dst, send_sem, recv_sem, where):
        copy = pltpu.make_async_remote_copy(
            src_ref=src, dst_ref=dst, send_sem=send_sem, recv_sem=recv_sem, device_id=where
        )
        copy.start()
        pending.append(copy)

    def wait(view, recv_sem):
        pltpu.make_async_remote_copy(
            src_ref=view, dst_ref=view, send_sem=t_send.at[0], recv_sem=recv_sem, device_id={"expert": (me + 1) % n}
        ).wait_recv()

    got = (got_qb, got_oa, got_ina, got_midb, got_dna, got_dnb)

    def swap(i, source):
        for j in range(1, replicas):
            peer = (rep + j) % replicas
            go(
                source.at[peer], got[i].at[rep], p_send.at[i * replicas + j], p_recv.at[i * replicas + rep],
                {"dp": peer},
            )

    def swapped(i):
        for j in range(1, replicas):
            src = (rep + j) % replicas
            wait(got[i].at[src], p_recv.at[i * replicas + src])

    for copy in owns:
        copy.wait()
    steps = red.steps()
    for step in steps[:4]:
        step()
    for i, source in enumerate((gina_hbm, gmidb_hbm, gdna_hbm, gdnb_hbm)):
        swap(i + 2, source)
    red.flush()
    need("act", "db", "dn")
    tiles = width // TILE

    def y_tile(t):
        e = t // tiles
        s = pl.ds(pl.multiple_of(t % tiles * TILE, TILE), TILE)
        y = dot(act[e], dn[e, :, s]) + dot(drank_ref[e], db_all[e, slot, :, s])
        part[pl.ds(pl.multiple_of(e * n * cap, 16), n * cap), s] = (y * weight[e]).astype(brain)

    drive(experts * tiles, y_tile, {2: steps[4:5], 4: steps[5:6], 5: steps[6:7]})
    seq_ref = dn.at[0]
    loads["seq"] = fetch(seq_hbm, seq_ref, load_sem.at[len(loads) + 4])
    need("resid")
    for k in ORDER:
        r = red.rows(k)
        grad = top_ref[r].astype(single) + norm_back(resid_ref[r], gain2_ref[...], red.final(k))
        gres[r] = grad
        bf[me, r] = grad.astype(brain)
        if k != ORDER[0]:
            bf_g.start_own(ORDER[ORDER.index(k) - 1])
    bf_g.start_own(ORDER[-1])
    need("wo", "pb", "pa", "mixed")

    def mixed_grad(block):
        p = block // 2
        both = bf[pl.ds(2 * p, 2)].reshape(2 * toks, width)
        at = two(p, toks)
        rank = dot(both, pb_all[slot], 1, 1).astype(brain)
        grank[at, :] = rank
        gmix[at, :] = (dot(both, wo_ref[...], 1, 1) + dot(rank, pa_all[slot])).astype(brain)

    def y_block(block_at):
        ypart[block_at] = combined(place, part, block_at, cap, n * cap)

    bf_g.pair(me)
    mixed_grad(me)
    drive(
        n, y_block, {2: [functools.partial(bf_g.relay, 0)], 6: [functools.partial(bf_g.relay, 1)]},
    )
    for i in range(4):
        redy.give(i)
    for i in range(2, CHUNKS):
        bf_g.relay(i)
    ysteps = redy.steps()
    for step in ysteps[:4]:
        step()
    bf_g.pair(bf_g.across)
    mixed_grad(bf_g.across)
    redy.flush()
    bf_g.relay_far(0)
    bf_g.pair(bf_g.along)
    mixed_grad(bf_g.along)
    for i in range(1, CHUNKS // 2):
        bf_g.relay_far(i)
    bf_g.pair(bf_g.far)
    mixed_grad(bf_g.far)

    piece = span // replicas
    goa = dot(grank[...], mixed_ref[...], 0, 0)
    for d in range(replicas):
        goa_ref[d] = goa[:, d * piece : (d + 1) * piece].astype(brain)
    got_oa[rep] = goa_ref[rep]
    swap(1, goa_ref)

    need("proj")
    scale = HEAD ** (-0.5)
    block = 256
    for h in range(heads):
        at = slice(h * HEAD, (h + 1) * HEAD)
        gk[...] = jnp.zeros_like(gk)
        gv[...] = jnp.zeros_like(gv)

        def attend(i, h=h, at=at):
            r = pl.ds(pl.multiple_of(i * block, block), block)
            q, do = proj_ref[0, r, at], gmix[r, at]
            delta = jnp.sum(do.astype(single) * mixed_ref[r, at].astype(single), axis=-1, keepdims=True)
            probs = jnp.exp(dot(q, proj_ref[1, :, at], 1, 1) * scale - lse_ref[r, h : h + 1])
            gp = dot(do, proj_ref[2, :, at], 1, 1)
            gs = (probs * (gp - delta)).astype(brain)
            gproj[0, r, at] = (dot(gs, proj_ref[1, :, at]) * scale).astype(brain)
            gk[...] += dot(gs, q, 0, 0)
            gv[...] += dot(probs.astype(brain), do, 0, 0)

        drive(length // block, attend, {0: ysteps[4:5], 1: ysteps[5:6], 2: ysteps[6:]} if h == 0 else {})
        gproj[1, :, at] = (gk[...] * scale).astype(brain)
        gproj[2, :, at] = gv[...].astype(brain)

    need("a", "b", "w")
    for j in range(3):
        a_ref[16 * j : 16 * j + 16, :] = a_all[j, slot]
    nsteps = redn.steps()
    for i in range(4):
        p = redn.order[i] // 2
        at = two(p, toks)
        for j in range(3):
            glow[at, 16 * j : 16 * j + 16] = dot(gproj[j, at, :], b_all[j, slot], 1, 1).astype(brain)
        wide = min(1024, width)

        def normed_grad(c, carry, p=p, at=at):
            s = pl.ds(pl.multiple_of(c * wide, wide), wide)
            out = dot(glow[at, :], a_ref[:, s])
            for j in range(3):
                out = out + dot(gproj[j, at, :], w_ref[j, s, :], 1, 1)
            part[at, s] = out.astype(brain)
            return carry

        lax.fori_loop(0, width // wide, normed_grad, 0)
        if i:
            redn.give(i - 1)
        if i == 2:
            for step in nsteps[:2]:
                step()
    redn.give(3)
    for step in nsteps[2:4]:
        step()
    del nsteps[:4]

    thin = width // (n * replicas)

    def share(row, value, base):
        for c in range(value.shape[1] // thin):
            d, e = (base + c) // n, (base + c) % n
            shared_ref[e, row : row + value.shape[0], d * thin : (d + 1) * thin] = value[
                :, c * thin : (c + 1) * thin
            ].astype(brain)

    def advance():
        if nsteps:
            nsteps.pop(0)()

    for j in range(3):
        gqb = dot(low_ref[:, 16 * j : 16 * j + 16], gproj[j], 0, 0)
        for d in range(replicas):
            gqb_ref[d, 16 * j : 16 * j + 16, :] = gqb[:, d * piece : (d + 1) * piece].astype(brain)
    redn.flush()
    got_qb[rep] = gqb_ref[rep]
    swap(0, gqb_ref)
    need("seq")
    cols = 512
    for c in range(width // cols):
        s = slice(c * cols, (c + 1) * cols)
        share(0, dot(glow[...], seq_ref[:, s], 0, 0), c * cols // thin)
        share(48, dot(orank_ref[...], bf[:, :, s].reshape(length, cols), 0, 0), c * cols // thin)
        advance()
    shared_in[me] = shared_ref[me]
    for j in range(1, n):
        peer = (me + j) % n
        go(shared_ref.at[peer], shared_in.at[me], sh_send.at[j - 1], sh_recv.at[me], {"expert": peer})
    while nsteps:
        advance()

    def squares(i, source):
        rows = source.shape[1] // RANK

        def body(t, acc):
            at = pl.ds(pl.multiple_of(t // ADAPTERS * RANK, RANK), RANK)
            value = jnp.zeros((RANK, source.shape[2]), single)
            for s in range(replicas):
                value = value + source[s, at, :].astype(single) * jnp.where(ids_ref[s] == t % ADAPTERS, 1.0, 0.0)
            return acc + value * value

        return jnp.sum(
            lax.fori_loop(0, rows * ADAPTERS, body, jnp.zeros((RANK, source.shape[2]), single))
        )

    need("ina", "midb", "dna", "dnb")
    total = jnp.zeros((), single)
    for i in range(2, 6):
        swapped(i)
        total = total + squares(i, got[i])
    for j in range(1, n):
        src = (me + j) % n
        wait(shared_in.at[src], sh_recv.at[src])
    summed = shared_in[0].astype(single)
    for e in range(1, n):
        summed = summed + shared_in[e].astype(single)
    for d in range(replicas):
        shared_mid[d] = summed[:, d * thin : (d + 1) * thin].astype(brain)
    shared_got[rep] = shared_mid[rep]
    for j in range(1, replicas):
        peer = (rep + j) % replicas
        go(shared_mid.at[peer], shared_got.at[rep], mid_send.at[j], mid_recv.at[rep], {"dp": peer})
    for k in ORDER:
        r = redy.rows(k)
        out_ref[r] = (resid_ref[r] + redy.final(k)).astype(brain)
    for i in range(2):
        swapped(i)
        total = total + squares(i, got[i])
    for j in range(1, replicas):
        src = (rep + j) % replicas
        wait(shared_got.at[src], mid_recv.at[src])
    total = total + squares(0, shared_got)

    mine[0] = jnp.full(mine.shape[1:], total, single)
    tot_e[me] = mine[0]
    for j in range(1, n):
        go(mine.at[0], tot_e.at[me], t_send.at[j], t_recv.at[me], {"expert": (me + j) % n})
    for j in range(1, n):
        src = (me + j) % n
        wait(tot_e.at[src], t_recv.at[src])
    total = tot_e[0]
    for e in range(1, n):
        total = total + tot_e[e]
    mine[1] = total
    tot_d[rep] = mine[1]
    for j in range(1, replicas):
        go(mine.at[1], tot_d.at[rep], t_send.at[n + j], t_recv.at[n + rep], {"dp": (rep + j) % replicas})
    for k in ORDER:
        r = redn.rows(k)
        gh_ref[r] = gres[r] + norm_back(hid_ref[r].astype(single), gain_ref[...], redn.final(k))
    for j in range(1, replicas):
        src = (rep + j) % replicas
        wait(tot_d.at[src], t_recv.at[n + src])
    total = tot_d[0]
    for d in range(1, replicas):
        total = total + tot_d[d]
    norm_ref[...] = jnp.sqrt(total)
    for mover in (red, redy, redn, bf_g):
        mover.drain()
    for copy in pending:
        copy.wait_send()


def back(
    ids, hid, top, gain, gain2, low, lse, orank, place, weight, drank, resid, seq, proj, mixed, gpart, act, dn, db,
    w, a, b, wo, pa, pb, pieces, cap, replicas, cid=1,
):
    n, toks, width = seq.shape
    seq = seq.reshape(n * toks, width)
    experts, rows = act.shape[:2]
    span = w.shape[2]
    length = toks * n
    vm = pl.BlockSpec(memory_space=pltpu.VMEM)
    sm = pl.BlockSpec(memory_space=pltpu.SMEM)
    hb = pl.BlockSpec(memory_space=pl.ANY)
    f = lambda *s: jax.ShapeDtypeStruct(s, single)
    h = lambda *s: jax.ShapeDtypeStruct(s, brain)
    bv = lambda *s: pltpu.VMEM(s, brain)
    fv = lambda *s: pltpu.VMEM(s, single)
    dma = pltpu.SemaphoreType.DMA
    thin = width // (n * replicas)
    piece = span // replicas
    return pl.pallas_call(
        functools.partial(back_kernel, cap, replicas),
        out_shape=(
            h(toks, width), f(toks, width), f(8, 128), h(replicas, 64, thin), h(replicas, 48, piece),
            h(replicas, 16, piece),
        ) + tuple(h(*p.shape) for p in pieces),
        in_specs=[sm] + [vm] * 10 + [hb] * 18,
        out_specs=[vm] * 10,
        scratch_shapes=[
            fv(toks, width), bv(3, length, span), bv(length, span), bv(4, toks, width), bv(n, toks, width),
            bv(*act.shape), bv(*dn.shape), bv(*db.shape), bv(experts * rows, width),
        ]
        + [pltpu.VMEM(v.shape, brain) for v in (w, a, b, wo, pa, pb)]
        + [
            bv(48, width), bv(n, toks, width), fv(toks, width), bv(length, span), bv(length, 16),
            bv(3, length, span), bv(length, 48), fv(length, HEAD), fv(length, HEAD),
            bv(replicas, 48, piece), bv(replicas, 16, piece), bv(n, 64, replicas * thin), bv(n, 64, replicas * thin),
            bv(replicas, 64, thin), fv(n, 8, 128), fv(replicas, 8, 128), fv(2, 8, 128), dma((20,)), dma((4,)),
            dma((n,)), dma((n,)), dma((replicas,)), dma((replicas,)), dma((6 * replicas,)), dma((6 * replicas,)),
            dma((n + replicas,)), dma((n + replicas,)),
        ]
        + scatter_scratch(toks, width) * 3 + gather_scratch(n),
        compiler_params=pltpu.CompilerParams(collective_id=cid, has_side_effects=True, vmem_limit_bytes=VMEM_ALL),
        name="back",
    )(
        ids, hid, top, gain, gain2, low, lse, orank, place, weight, drank, resid, seq, proj, mixed, gpart, act, dn, db,
        w, a, b, wo, pa, pb, *pieces,
    )


def adam_kernel(n, replicas, groups, spans, adapter_ref, step_ref, norm_in, out_in, gh_in, *refs):
    got, refs = refs[:7], refs[7:]
    weight_hbm, first_hbm, second_hbm, refs = refs[:8], refs[8:16], refs[16:24], refs[24:]
    out_hbm, gh_hbm, norm_ref, result, refs = refs[0], refs[1], refs[2], refs[3:35], refs[35:]
    weight, first, second, kept, refs = refs[:8], refs[8:16], refs[16:24], refs[24:56], refs[56:]
    load_sem, save_sem = refs
    me, rep = lax.axis_index("expert"), lax.axis_index("dp")
    common = rep * n + me
    loads, saves = {}, []
    turns = (6, 5, 4, 7, 0, 2, 1, 3)
    for a in turns:
        size, pieces = spans[a]
        index = common if pieces == n * replicas else rep
        start = index * size // weight[a].shape[1] * weight[a].shape[1]
        view = weight_hbm[a].at[:, pl.ds(pl.multiple_of(start, 128), weight[a].shape[1])]
        loads[a] = [
            fetch(src, dst, load_sem.at[3 * a + k])
            for k, (src, dst) in enumerate(((view, weight[a]), (first_hbm[a], first[a]), (second_hbm[a], second[a])))
        ]
    saves.append(fetch(out_in, out_hbm, save_sem.at[32]))
    saves.append(fetch(gh_in, gh_hbm, save_sem.at[33]))
    norm_ref[0] = norm_in[0, 0]
    factor = jnp.minimum(1.0, CLIP / norm_in[...])[0:1, 0:1]
    steps = jnp.full((8, 128), step_ref[0].astype(single), single)
    fix_first = (1.0 / (1.0 - jnp.exp(steps * jnp.log(jnp.full((8, 128), beta_one, single)))))[0:1, 0:1]
    fix_second = (1.0 / (1.0 - jnp.exp(steps * jnp.log(jnp.full((8, 128), beta_two, single)))))[0:1, 0:1]
    for a in turns:
        for copy in loads[a]:
            copy.wait()
        source = got[max(a - 1, 0)]
        base = groups[0] if a == 1 else 0
        size, pieces = spans[a]
        window = weight[a].shape[1]
        index = common if pieces == n * replicas else rep

        def body(t, carry, a=a, source=source, base=base, size=size, window=window, index=index):
            rows = pl.ds(pl.multiple_of((base + t) * RANK, RANK), RANK)
            parts = [source[s, rows, :].astype(single) for s in range(replicas)]
            for adapter in range(ADAPTERS):
                at = pl.ds(pl.multiple_of((t * ADAPTERS + adapter) * RANK, RANK), RANK)
                grad = jnp.zeros((RANK, size), single)
                for s in range(replicas):
                    grad = grad + parts[s] * jnp.where(adapter_ref[s] == adapter, 1.0, 0.0)
                held = weight[a][at, :].astype(single)
                w = held[:, :size]
                for c in range(1, window // size):
                    w = jnp.where(index % (window // size) == c, held[:, c * size : (c + 1) * size], w)
                clipped = grad * factor
                f = beta_one * first[a][at, :] + (1.0 - beta_one) * clipped
                s = beta_two * second[a][at, :] + (1.0 - beta_two) * clipped * clipped
                kept[4 * a][at, :] = grad
                kept[4 * a + 1][at, :] = f
                kept[4 * a + 2][at, :] = s
                kept[4 * a + 3][at, :] = -learn_rate * (
                    f * fix_first / (jnp.sqrt(s * fix_second) + adam_eps) + weight_decay * w
                )
            done = pl.ds(pl.multiple_of(t * ADAPTERS * RANK, ADAPTERS * RANK), ADAPTERS * RANK)
            for k in range(4 * a, 4 * a + 4):
                fetch(kept[k].at[done], result[k].at[done], save_sem.at[k])
            return carry

        lax.fori_loop(0, groups[a], body, 0)
        for k in range(4 * a, 4 * a + 4):
            saves.append(pltpu.make_async_copy(kept[k], result[k], save_sem.at[k]))
    for copy in saves:
        copy.wait()


def adam(adapters, steps, norm, block_out, gh, got, weight, pieces, first, second, n, replicas):
    spans = tuple((f.shape[1], p) for f, p in zip(first, pieces))
    groups = tuple(f.shape[0] // (ADAPTERS * RANK) for f in first)
    vm = pl.BlockSpec(memory_space=pltpu.VMEM)
    sm = pl.BlockSpec(memory_space=pltpu.SMEM)
    hb = pl.BlockSpec(memory_space=pl.ANY)
    f = lambda s: jax.ShapeDtypeStruct(s, single)
    dma = pltpu.SemaphoreType.DMA
    shapes = [t.shape for t in first]
    return pl.pallas_call(
        functools.partial(adam_kernel, n, replicas, groups, spans),
        out_shape=(jax.ShapeDtypeStruct(block_out.shape, brain), f(gh.shape), f((1,)))
        + tuple(f(s) for s in shapes for _ in range(4)),
        in_specs=[sm, sm, vm, vm, vm] + [vm] * 7 + [hb] * 24,
        out_specs=[hb, hb, sm] + [hb] * 32,
        scratch_shapes=[pltpu.VMEM((s[0], max(s[1], 128)), brain) for s in shapes]
        + [pltpu.VMEM(s, single) for s in shapes] * 2
        + [pltpu.VMEM(s, single) for s in shapes for _ in range(4)]
        + [dma((24,)), dma((34,))],
        compiler_params=pltpu.CompilerParams(vmem_limit_bytes=VMEM_ALL),
        name="adam",
    )(adapters, steps, norm, block_out, gh, *got, *weight, *first, *second)


def per_device(
    hidden,
    output_cotangent,
    attention_gain,
    expert_norm_gain,
    query_key_value_weight,
    output_weight,
    gate_up_weight,
    down_weight,
    token_experts,
    expert_gate_weight,
    sequence_adapter,
    optimizer_steps,
    adapter_attention_input,
    adapter_attention_output,
    adapter_projection_input,
    adapter_projection_output,
    adapter_hidden_input,
    adapter_hidden_output,
    adapter_down_input,
    adapter_down_output,
    moment_attention_input,
    moment_attention_output,
    moment_projection_input,
    moment_projection_output,
    moment_hidden_input,
    moment_hidden_output,
    moment_down_input,
    moment_down_output,
    squared_attention_input,
    squared_attention_output,
    squared_projection_input,
    squared_projection_output,
    squared_hidden_input,
    squared_hidden_output,
    squared_down_input,
    squared_down_output,
):
    n = lax.axis_size("expert")
    replicas = lax.axis_size("dp")
    toks, width = hidden.shape[1:]
    here = down_weight.shape[0]
    cap = min(toks, toks * token_experts.shape[2] * 5 // (4 * here * n))
    gain = attention_gain[None]
    gain2 = expert_norm_gain[None]
    hid, cot = hidden[0], output_cotangent[0]
    low, lse, orank, gdr, place, weight, seq, proj, mixed, resid, x_rows, g_rows, ga = front(
        sequence_adapter, hid, cot, token_experts[0].T, expert_gate_weight[0].T, gain, gain2, query_key_value_weight,
        adapter_attention_input, adapter_attention_output, output_weight, adapter_projection_input,
        adapter_projection_output, down_weight, adapter_down_input, adapter_down_output, n, cap,
    )
    drank, *pieces, gpart, act = moe(
        sequence_adapter, place, weight, gdr, x_rows, g_rows, ga, gate_up_weight, adapter_hidden_input,
        adapter_hidden_output, adapter_down_input, cap, replicas,
    )
    block_out, grad_hidden, norm, *got = back(
        sequence_adapter, hid, cot, gain, gain2, low, lse, orank, place, weight, drank, resid, seq, proj, mixed, gpart,
        act, down_weight, adapter_down_output,
        query_key_value_weight, adapter_attention_input, adapter_attention_output, output_weight,
        adapter_projection_input, adapter_projection_output, tuple(pieces), cap, replicas,
    )

    def flat(array):
        return array.reshape(-1, array.shape[-1])

    weights = (
        adapter_attention_input, adapter_projection_output, adapter_attention_output, adapter_projection_input,
        adapter_hidden_input, adapter_hidden_output, adapter_down_input, adapter_down_output,
    )
    first = (
        moment_attention_input, moment_projection_output, moment_attention_output, moment_projection_input,
        moment_hidden_input, moment_hidden_output, moment_down_input, moment_down_output,
    )
    second = (
        squared_attention_input, squared_projection_output, squared_attention_output, squared_projection_input,
        squared_hidden_input, squared_hidden_output, squared_down_input, squared_down_output,
    )
    outs = adam(
        sequence_adapter, optimizer_steps, norm, block_out, grad_hidden, got, tuple(flat(w) for w in weights),
        (n * replicas,) * 2 + (replicas,) * 6, tuple(flat(m) for m in first), tuple(flat(s) for s in second),
        n, replicas,
    )
    results = [outs[0][None], outs[1][None], outs[2]]
    for a in (0, 2, 3, 1, 4, 5, 6, 7):
        for kind in range(4):
            results.append(outs[3 + 4 * a + kind].reshape(first[a].shape))
    return tuple(results)


def solution(mesh):
    return jax.shard_map(
        per_device,
        mesh=mesh,
        in_specs=(
            P("dp", "expert", None),
            P("dp", "expert", None),
            P(),
            P(),
            P(None, None, "expert"),
            P("expert", None),
            P("expert", None, None, None),
            P("expert", None, None),
            P("dp", "expert", None),
            P("dp", "expert", None),
            P(),
            P(),
            P(),
            P(None, None, None, "expert"),
            P(None, None, "expert"),
            P(),
            P("expert", None, None, None, None),
            P("expert", None, None, None, None),
            P("expert", None, None, None),
            P("expert", None, None, None),
            P(None, None, None, ("dp", "expert")),
            P(None, None, None, ("expert", "dp")),
            P(None, None, ("expert", "dp")),
            P(None, None, ("dp", "expert")),
            P("expert", None, None, None, "dp"),
            P("expert", None, None, None, "dp"),
            P("expert", None, None, "dp"),
            P("expert", None, None, "dp"),
            P(None, None, None, ("dp", "expert")),
            P(None, None, None, ("expert", "dp")),
            P(None, None, ("expert", "dp")),
            P(None, None, ("dp", "expert")),
            P("expert", None, None, None, "dp"),
            P("expert", None, None, None, "dp"),
            P("expert", None, None, "dp"),
            P("expert", None, None, "dp"),
        ),
        out_specs=(
            P("dp", "expert", None),
            P("dp", "expert", None),
            P(),
            P(None, None, None, ("dp", "expert")),
            P(None, None, None, ("dp", "expert")),
            P(None, None, None, ("dp", "expert")),
            P(None, None, None, ("dp", "expert")),
            P(None, None, None, ("expert", "dp")),
            P(None, None, None, ("expert", "dp")),
            P(None, None, None, ("expert", "dp")),
            P(None, None, None, ("expert", "dp")),
            P(None, None, ("expert", "dp")),
            P(None, None, ("expert", "dp")),
            P(None, None, ("expert", "dp")),
            P(None, None, ("expert", "dp")),
            P(None, None, ("dp", "expert")),
            P(None, None, ("dp", "expert")),
            P(None, None, ("dp", "expert")),
            P(None, None, ("dp", "expert")),
            P("expert", None, None, None, "dp"),
            P("expert", None, None, None, "dp"),
            P("expert", None, None, None, "dp"),
            P("expert", None, None, None, "dp"),
            P("expert", None, None, None, "dp"),
            P("expert", None, None, None, "dp"),
            P("expert", None, None, None, "dp"),
            P("expert", None, None, None, "dp"),
            P("expert", None, None, "dp"),
            P("expert", None, None, "dp"),
            P("expert", None, None, "dp"),
            P("expert", None, None, "dp"),
            P("expert", None, None, "dp"),
            P("expert", None, None, "dp"),
            P("expert", None, None, "dp"),
            P("expert", None, None, "dp"),
        ),
        check_vma=False,
    )
```

```python
import functools

import jax
import jax.numpy as jnp
from jax import lax
from jax.experimental import pallas as pl
from jax.experimental.pallas import tpu as pltpu
from jax.sharding import PartitionSpec as P


single = jnp.float32
brain = jnp.bfloat16
HEAD = 128
TILE = 256
CHUNKS = 4
ORDER = [k + j * (CHUNKS // 2) for k in range(CHUNKS // 2) for j in range(2)]
GATHER_SENDS = CHUNKS * 7
SCATTER_SEMS = CHUNKS * 7
norm_eps = 1e-05
VMEM_ALL = 67043328


def dot(a, b, left=1, right=0):
    return lax.dot_general(a, b, (((left,), (right,)), ((), ())), preferred_element_type=single)


def peers():
    me = lax.axis_index("expert")
    core = me + 1 - 2 * (me % 2)
    across = me + 2 - 4 * ((me // 2) % 2)
    along = me + 4 - 8 * (me // 4)
    return me, core, across, along


def greet():
    me, core, across, along = peers()
    barrier = pltpu.get_barrier_semaphore()
    for peer in (core, across, along):
        pl.semaphore_signal(barrier, inc=1, device_id={"expert": peer})
    pl.semaphore_wait(barrier, 3)


class Mover:
    def __init__(self, send_sem, recv_sem):
        self.send_sem, self.recv_sem = send_sem, recv_sem
        self.me, self.core, self.across, self.along = peers()
        self.far = self.across + self.along - self.me
        self.count = 0
        self.waiting = []

    def go(self, src, dst, recv, peer):
        pltpu.make_async_remote_copy(
            src_ref=src, dst_ref=dst, send_sem=self.send_sem.at[self.count],
            recv_sem=self.recv_sem.at[recv], device_id={"expert": peer},
        ).start()
        self.count += 1

    def later(self, args):
        self.waiting.append(args)
        if len(self.waiting) > 1:
            self.waiting.pop(0)()

    def flush(self):
        while self.waiting:
            self.waiting.pop(0)()

    def got(self, view, recv):
        pltpu.make_async_remote_copy(
            src_ref=view, dst_ref=view, send_sem=self.send_sem.at[0], recv_sem=self.recv_sem.at[recv],
            device_id={"expert": self.core},
        ).wait_recv()

    def drain(self):
        view = self.sample()
        for i in range(self.count):
            pltpu.make_async_remote_copy(
                src_ref=view, dst_ref=view, send_sem=self.send_sem.at[i], recv_sem=self.recv_sem.at[0],
                device_id={"expert": self.core},
            ).wait_send()

    def beside(self, block):
        return block + 1 - 2 * (self.me % 2)


class Gather(Mover):
    def __init__(self, out, send_sem, recv_sem):
        super().__init__(send_sem, recv_sem)
        self.out = out
        self.size = out.shape[1] // CHUNKS

    def sample(self):
        return self.out.at[0, pl.ds(0, self.size)]

    def move(self, block, k, peer):
        view = self.out.at[block, pl.ds(k * self.size, self.size)]
        self.go(view, view, block * CHUNKS + k, peer)

    def arrive(self, block, k):
        self.got(self.out.at[block, pl.ds(k * self.size, self.size)], block * CHUNKS + k)

    def start_own(self, k):
        for peer in (self.across, self.along, self.core):
            self.move(self.me, k, peer)

    def start(self):
        for k in ORDER:
            self.start_own(k)

    def relay(self, i):
        k = ORDER[i]
        first_half = k < CHUNKS // 2
        self.arrive(self.across, k)
        if first_half:
            self.move(self.across, k, self.along)
        self.move(self.across, k, self.core)
        self.arrive(self.along, k)
        if not first_half:
            self.move(self.along, k, self.across)
        self.move(self.along, k, self.core)

    def relay_far(self, i):
        half = CHUNKS // 2
        for k in (i, i + half):
            self.arrive(self.far, k)
            self.move(self.far, k, self.core)

    def pair(self, block):
        for k in range(CHUNKS):
            self.arrive(self.beside(block), k)


class Scatter(Mover):
    def __init__(self, part, pair, half_x, half_y, from_x, from_y, send_sem, recv_sem, own=None):
        super().__init__(send_sem, recv_sem)
        self.part, self.pair, self.own = part, pair, own
        self.half_x, self.half_y, self.from_x, self.from_y = half_x, half_y, from_x, from_y
        self.order = (self.far, self.across, self.along, self.me)
        self.toks = pair.shape[1]
        self.size = self.toks // CHUNKS
        half = CHUNKS // 2
        self.hx = 4 * CHUNKS
        self.hy = self.hx + half
        self.fx = self.hy + half
        self.fy = self.fx + CHUNKS

    def sample(self):
        return self.pair.at[0, self.rows(0)]

    def rows(self, k):
        return pl.ds(k * self.size, self.size)

    def chunk(self, block, k):
        if len(self.part.shape) == 3:
            return self.part.at[block, self.rows(k)]
        return self.part.at[pl.ds(pl.multiple_of(block * self.toks + k * self.size, self.size), self.size)]

    def mine(self, i, k):
        view = self.chunk(self.order[i], k) if self.own is None else self.own.at[i, self.rows(k)]
        return view[...].astype(single)

    def give(self, i):
        other = self.beside(self.order[i])
        for k in range(CHUNKS):
            r = self.rows(k)
            self.go(self.chunk(other, k), self.pair.at[i, r], i * CHUNKS + k, self.core)

    def add(self, i, k, extra=None):
        r = self.rows(k)
        self.got(self.pair.at[i, r], i * CHUNKS + k)
        total = self.mine(i, k) + self.pair[i, r].astype(single)
        if extra is not None:
            ref, recv, k2 = extra
            r2 = self.rows(k2)
            self.got(ref.at[r2], recv)
            total = total + ref[r2].astype(single)
        self.pair[i, r] = total.astype(brain)

    def steps(self):
        half = CHUNKS // 2
        out = []

        def relay(i, k, to, row, recv, peer):
            self.later(lambda: self.go(self.pair.at[i, self.rows(k)], to.at[self.rows(row)], recv, peer))

        def one(k):
            self.add(0, k)
            relay(0, k, self.half_x, k, self.hx + k, self.across)
            self.add(0, k + half)
            relay(0, k + half, self.half_y, k, self.hy + k, self.along)

        def two(k):
            self.add(1, k)
            relay(1, k, self.from_x, k, self.fx + k, self.across)
            self.add(2, k + half)
            relay(2, k + half, self.from_y, k + half, self.fy + k + half, self.along)

        def three(k):
            self.add(1, k + half, (self.half_y, self.hy + k, k))
            relay(1, k + half, self.from_x, k + half, self.fx + k + half, self.across)
            self.add(2, k, (self.half_x, self.hx + k, k))
            relay(2, k, self.from_y, k, self.fy + k, self.along)

        for fn in (one, two, three):
            for k in range(half):
                out.append(functools.partial(fn, k))
        out.append(self.flush)
        return out

    def final(self, k):
        r = self.rows(k)
        self.got(self.pair.at[3, r], 3 * CHUNKS + k)
        total = self.mine(3, k) + self.pair[3, r].astype(single)
        self.got(self.from_x.at[r], self.fx + k)
        total = total + self.from_x[r].astype(single)
        self.got(self.from_y.at[r], self.fy + k)
        return total + self.from_y[r].astype(single)


def scatter_scratch(rows, cols):
    return [
        pltpu.VMEM((4, rows, cols), brain),
        pltpu.VMEM((rows // 2, cols), brain),
        pltpu.VMEM((rows // 2, cols), brain),
        pltpu.VMEM((rows, cols), brain),
        pltpu.VMEM((rows, cols), brain),
        pltpu.SemaphoreType.DMA((SCATTER_SEMS,)),
        pltpu.SemaphoreType.DMA((SCATTER_SEMS,)),
    ]


def gather_scratch(n):
    return [pltpu.SemaphoreType.DMA((GATHER_SENDS,)), pltpu.SemaphoreType.DMA((n * CHUNKS,))]


def rms(values, gain):
    return values * lax.rsqrt(jnp.mean(values * values, axis=-1, keepdims=True) + norm_eps) * gain


def fetch(src, dst, sem):
    copy = pltpu.make_async_copy(src, dst, sem)
    copy.start()
    return copy


def drive(count, body, events):
    def step(i, carry):
        body(i)
        for at, actions in events.items():

            @pl.when(i == at)
            def _(actions=actions):
                for action in actions:
                    action()

        return carry

    lax.fori_loop(0, count, step, 0)


def slots_of(denseall_ref, me, experts, dense, place):
    blocks, toks = denseall_ref.shape[0], denseall_ref.shape[2]
    for b in range(blocks):
        for e in range(experts):
            at = experts * b + e
            dense[at : at + 1, :] = denseall_ref[b, pl.ds(experts * me + e, 1), :]
    upper = (
        lax.broadcasted_iota(jnp.int32, (toks, toks), 0) < lax.broadcasted_iota(jnp.int32, (toks, toks), 1)
    ).astype(single).astype(brain)
    chosen = dense[...] > 0.0
    before = dot(chosen.astype(single).astype(brain), upper)
    place[...] = jnp.where(chosen, before, -1.0)


def picks(place, b, cap, experts):
    rows = lax.broadcasted_iota(jnp.int32, (cap, place.shape[1]), 0).astype(single)
    return [(place[pl.ds(experts * b + e, 1), :] == rows).astype(single) for e in range(experts)]


def weigh(place, dense, weight, b, cap, experts):
    for e, sel in enumerate(picks(place, b, cap, experts)):
        w = jnp.sum(sel * dense[pl.ds(experts * b + e, 1), :], axis=1, keepdims=True)
        weight[e, pl.ds(pl.multiple_of(b * cap, 16), cap), :] = w


def take(place, block, rows, b, cap):
    experts = rows.shape[0]
    both = jnp.concatenate([s.astype(brain) for s in picks(place, b, cap, experts)], axis=0)
    got = dot(both, block).astype(brain)
    at = pl.ds(pl.multiple_of(b * cap, 16), cap)
    for e in range(experts):
        rows[e, at, :] = got[e * cap : (e + 1) * cap]


def combined(place, rows, b, cap, apart):
    experts = rows.shape[0] // apart
    both = jnp.concatenate([s.astype(brain) for s in picks(place, b, cap, experts)], axis=0)
    parts = [rows[pl.ds(pl.multiple_of(e * apart + b * cap, 16), cap), :] for e in range(experts)]
    return dot(both, jnp.concatenate(parts, axis=0), 0, 0).astype(brain)


def two(p, toks):
    return pl.ds(pl.multiple_of(p * 2 * toks, 2 * toks), 2 * toks)


def meet(n, replicas, with_dp):
    me, rep = lax.axis_index("expert"), lax.axis_index("dp")
    barrier = pltpu.get_barrier_semaphore()
    for j in range(1, n):
        pl.semaphore_signal(barrier, inc=1, device_id={"expert": (me + j) % n})
    if with_dp:
        for j in range(1, replicas):
            pl.semaphore_signal(barrier, inc=1, device_id={"dp": (rep + j) % replicas})
    pl.semaphore_wait(barrier, n - 1 + (replicas - 1 if with_dp else 0))


def front_kernel(
    cap, ids_ref, hid_ref, top_ref, routes_ref, gates_ref, gain_ref, gain2_ref,
    w_hbm, a_hbm, b_hbm, wo_hbm, pa_hbm, pb_hbm, dn_hbm, da_hbm, db_hbm,
    low_ref, lse_ref, orank_ref, gdr_ref, place, weight, seq_hbm, proj_hbm, mixed_hbm, resid_hbm, x_hbm, g_hbm, ga_hbm,
    part, seq_ref, proj_ref, mixed_ref, topseq_ref, resid_ref, moe_ref, x_rows, g_rows, ga,
    w_ref, a_all, b_all, wo_ref, pa_all, pb_all, dn, da_all, db_all, a_ref, b_ref, mydense, dense, denseall_ref,
    load_sem, save_sem, *sems,
):
    toks, width = hid_ref.shape
    span = w_ref.shape[2]
    heads = span // HEAD
    n = seq_ref.shape[0]
    length = toks * n
    experts, hidden = dn.shape[0], dn.shape[1]
    loads = [
        fetch(src, dst, load_sem.at[i])
        for i, (src, dst) in enumerate(
            (
                (w_hbm, w_ref), (a_hbm, a_all), (b_hbm, b_all), (pa_hbm, pa_all), (pb_hbm, pb_all), (wo_hbm, wo_ref),
                (da_hbm, da_all), (db_hbm, db_all), (dn_hbm, dn),
            )
        )
    ]
    seq_g = Gather(seq_ref, sems[0], sems[1])
    top_g = Gather(topseq_ref, sems[2], sems[3])
    moe_g = Gather(moe_ref, sems[4], sems[5])
    red = Scatter(part, *sems[6:13])
    dsend, drecv = sems[13:15]
    me = seq_g.me
    slot = ids_ref[lax.axis_index("dp")]
    saves = []

    def save(src, dst):
        saves.append(fetch(src, dst, save_sem.at[len(saves)]))

    seq_ref[me] = rms(hid_ref[...].astype(single), gain_ref[...]).astype(brain)
    topseq_ref[me] = top_ref[...]
    choices = lax.broadcasted_iota(jnp.int32, (mydense.shape[0], toks), 0)
    table = jnp.zeros(mydense.shape, single)
    for k in range(routes_ref.shape[0]):
        table = table + jnp.where(routes_ref[k : k + 1, :] == choices, gates_ref[k : k + 1, :], 0.0)
    mydense[...] = table
    denseall_ref[me] = table
    meet(n, 1, False)
    seq_g.start()

    def dense_copy(j):
        return pltpu.make_async_remote_copy(
            src_ref=mydense, dst_ref=denseall_ref.at[me], send_sem=dsend.at[j - 1], recv_sem=drecv.at[me],
            device_id={"expert": (me + j) % n},
        )

    for j in range(1, n):
        dense_copy(j).start()
    for copy in loads[:3]:
        copy.wait()
    b_ref[...] = jnp.zeros_like(b_ref)
    for j in range(3):
        a_ref[16 * j : 16 * j + 16, :] = a_all[j, slot]
        b_ref[j, 16 * j : 16 * j + 16, :] = b_all[j, slot]

    def qkv(block):
        p = block // 2
        at = two(p, toks)
        low_ref[at, :] = dot(seq_ref[pl.ds(2 * p, 2)].reshape(2 * toks, width), a_ref[...], 1, 1).astype(brain)

        def third(j, carry):
            both = seq_ref[pl.ds(2 * p, 2)].reshape(2 * toks, width)
            proj_ref[j, at, :] = (dot(both, w_ref[j]) + dot(low_ref[at, :], b_ref[j])).astype(brain)
            return carry

        lax.fori_loop(0, 3, third, 0)

    seq_g.pair(me)
    qkv(me)
    for i in range(CHUNKS):
        seq_g.relay(i)
    top_g.start()
    seq_g.pair(seq_g.across)
    qkv(seq_g.across)
    seq_g.relay_far(0)
    seq_g.pair(seq_g.along)
    qkv(seq_g.along)
    for i in range(1, CHUNKS // 2):
        seq_g.relay_far(i)
    seq_g.pair(seq_g.far)
    qkv(seq_g.far)
    save(seq_ref, seq_hbm)
    save(proj_ref, proj_hbm)

    scale = HEAD ** (-0.5)
    block = 256
    top_steps = [functools.partial(top_g.relay, i) for i in range(CHUNKS)]
    top_steps += [functools.partial(top_g.relay_far, i) for i in range(CHUNKS // 2)]

    for h in range(heads):
        at = slice(h * HEAD, (h + 1) * HEAD)

        def attend(i, h=h, at=at):
            r = pl.ds(pl.multiple_of(i * block, block), block)
            scores = dot(proj_ref[0, r, at], proj_ref[1, :, at], 1, 1) * scale
            peak = jnp.max(scores, axis=-1, keepdims=True)
            expo = jnp.exp(scores - peak)
            total = jnp.sum(expo, axis=-1, keepdims=True)
            probs = (expo * (1.0 / total)).astype(brain)
            mixed_ref[r, at] = dot(probs, proj_ref[2, :, at]).astype(brain)
            lse_ref[r, h : h + 1] = peak + jnp.log(total)

        now, top_steps = top_steps[:3], top_steps[3:]
        last = length // block - 1
        drive(length // block, attend, {0: now[:1], last - 1: now[1:2], last: now[2:]} if h == 0 else {1: now[:1]})
        if h:
            top_steps = now[1:] + top_steps
    for copy in loads[3:6]:
        copy.wait()

    for i in range(4):
        p = red.order[i] // 2
        at = two(p, toks)
        rank = dot(mixed_ref[at, :], pa_all[slot], 1, 1).astype(brain)
        orank_ref[at, :] = rank
        cols = min(1024, width)

        def project(c, carry, p=p, at=at):
            s = pl.ds(pl.multiple_of(c * cols, cols), cols)
            out = dot(mixed_ref[at, :], wo_ref[:, s]) + dot(orank_ref[at, :], pb_all[slot, :, s])
            part[pl.ds(2 * p, 2), :, s] = out.astype(brain).reshape(2, toks, cols)
            return carry

        lax.fori_loop(0, width // cols, project, 0)
        if i:
            red.give(i - 1)
    red.give(3)
    save(mixed_ref, mixed_hbm)
    steps = red.steps()
    for step in steps[:4]:
        step()
    top_steps.pop(0)()
    red.flush()
    for step in top_steps:
        step()
    for block_at in (me, top_g.across, top_g.along, top_g.far):
        top_g.pair(block_at)
    for j in range(1, n):
        src = (me + j) % n
        view = denseall_ref.at[src]
        pltpu.make_async_remote_copy(
            src_ref=view, dst_ref=view, send_sem=dsend.at[0], recv_sem=drecv.at[src], device_id={"expert": src}
        ).wait_recv()
    for j in range(1, n):
        dense_copy(j).wait_send()
    slots_of(denseall_ref, me, experts, dense, place)

    def top_rows(b):
        weigh(place, dense, weight, b, cap, experts)
        take(place, topseq_ref[b], g_rows, b, cap)

    drive(n, top_rows, {5: steps[4:5]})
    for copy in loads[6:]:
        copy.wait()

    def top_rank(e):
        gdr_ref[e] = (dot(g_rows[e], db_all[e, slot], 1, 1) * weight[e]).astype(brain)

    drive(experts, top_rank, {})
    half = n * cap // 2
    tiles = hidden // TILE

    def top_tile(t):
        e, f, m = t // (2 * tiles), t // 2 % tiles, t % 2
        at = pl.ds(pl.multiple_of(f * TILE, TILE), TILE)
        r = pl.ds(pl.multiple_of(m * half, 16), half)
        out = dot(g_rows[e, r, :], dn[e, at, :], 1, 1) * weight[e, r, :]
        ga[e, r, at] = (out + dot(gdr_ref[e, r, :], da_all[e, slot, :, at])).astype(brain)

    drive(2 * experts * tiles, top_tile, {0: steps[5:6], 1: steps[6:7]})
    save(g_rows, g_hbm)
    save(ga, ga_hbm)
    for k in ORDER:
        r = red.rows(k)
        resid = hid_ref[r].astype(single) + red.final(k)
        resid_ref[r] = resid
        moe_ref[me, r] = rms(resid, gain2_ref[...]).astype(brain)
        if k != ORDER[0]:
            moe_g.start_own(ORDER[ORDER.index(k) - 1])
    save(resid_ref, resid_hbm)
    moe_g.start_own(ORDER[-1])

    def moe_rows(block_at):
        p = block_at // 2

        def one(i, carry):
            take(place, moe_ref[2 * p + i], x_rows, 2 * p + i, cap)
            return carry

        lax.fori_loop(0, 2, one, 0)
        at = pl.ds(pl.multiple_of(2 * p * cap, 16), 2 * cap)
        for e in range(experts):
            save(x_rows.at[e, at], x_hbm.at[e, at])

    moe_g.pair(me)
    moe_rows(me)
    for i in range(CHUNKS):
        moe_g.relay(i)
    moe_g.pair(moe_g.across)
    moe_rows(moe_g.across)
    for i in range(CHUNKS // 2):
        moe_g.relay_far(i)
    moe_g.pair(moe_g.along)
    moe_rows(moe_g.along)
    moe_g.pair(moe_g.far)
    moe_rows(moe_g.far)
    for mover in (seq_g, top_g, red, moe_g):
        mover.drain()
    for copy in saves:
        copy.wait()


def front(ids, hid, top, routes, gates, gain, gain2, w, a, b, wo, pa, pb, dn, da, db, n, cap, cid=0):
    toks, width = hid.shape
    span = w.shape[2]
    length = toks * n
    experts, hidden = dn.shape[0], dn.shape[1]
    rows = n * cap
    vm = pl.BlockSpec(memory_space=pltpu.VMEM)
    sm = pl.BlockSpec(memory_space=pltpu.SMEM)
    hb = pl.BlockSpec(memory_space=pl.ANY)
    f = lambda *s: jax.ShapeDtypeStruct(s, single)
    h = lambda *s: jax.ShapeDtypeStruct(s, brain)
    bv = lambda *s: pltpu.VMEM(s, brain)
    fv = lambda *s: pltpu.VMEM(s, single)
    whole = bv(n, toks, width)
    return pl.pallas_call(
        functools.partial(front_kernel, cap),
        out_shape=(
            h(length, 48), f(length, span // HEAD), h(length, 16), h(experts, rows, 16), f(n * experts, toks),
            f(experts, rows, 1),
            h(n, toks, width), h(3, length, span), h(length, span), f(toks, width),
            h(experts, rows, width), h(experts, rows, width), h(experts, rows, hidden),
        ),
        in_specs=[sm] + [vm] * 6 + [hb] * 9,
        out_specs=[vm] * 6 + [hb] * 7,
        scratch_shapes=[
            whole, whole, bv(3, length, span), bv(length, span), whole, fv(toks, width), whole,
            bv(experts, rows, width), bv(experts, rows, width), bv(experts, rows, hidden),
        ]
        + [pltpu.VMEM(v.shape, brain) for v in (w, a, b, wo, pa, pb, dn, da, db)]
        + [
            bv(48, width), bv(3, 48, span), fv(experts * n, toks), fv(n * experts, toks), fv(n, experts * n, toks),
            pltpu.SemaphoreType.DMA((9,)), pltpu.SemaphoreType.DMA((6 + 4 * experts,)),
        ]
        + gather_scratch(n) + gather_scratch(n) + gather_scratch(n) + scatter_scratch(toks, width)
        + [pltpu.SemaphoreType.DMA((n,)), pltpu.SemaphoreType.DMA((n,))],
        compiler_params=pltpu.CompilerParams(collective_id=cid, has_side_effects=True, vmem_limit_bytes=VMEM_ALL),
        name="front",
    )(ids, hid, top, routes, gates, gain, gain2, w, a, b, wo, pa, pb, dn, da, db)


def moe_kernel(
    cap, replicas, ids_ref, place, weight, gdr_ref, x_hbm, g_hbm, ga_hbm, gu_hbm, ha_hbm, hb_hbm, da_hbm,
    drank_ref, gina_ref, gmidb_ref, gdna_ref, gdnb_ref, gpart_hbm, act_hbm,
    gu, x_rows, g_rows, ga, s_rows, act, gg, uu, irank, girank, ha_ref, hb_ref, da_ref,
    out_stage, pick_sem, x_sem, g_sem, ga_sem, gu_sem, act_sem, out_sem,
):
    experts, width, hidden = gu.shape[0], gu.shape[2], gu.shape[3]
    blocks = place.shape[0] // experts
    rows = x_rows.shape[1]
    tiles = hidden // TILE
    which = ids_ref[lax.axis_index("dp")]
    picked = []
    for e in range(experts):
        for i in range(2):
            picked.append((ha_hbm.at[e, i, which], ha_ref.at[e, pl.ds(16 * i, 16)]))
            picked.append((hb_hbm.at[e, i, which], hb_ref.at[e, i]))
        picked.append((da_hbm.at[e, which], da_ref.at[e]))

    def cols(f):
        return pl.ds(pl.multiple_of(f * TILE, TILE), TILE)

    x_copy = lambda e: pltpu.make_async_copy(x_hbm.at[e], x_rows.at[e], x_sem.at[e])
    g_copy = lambda e: pltpu.make_async_copy(g_hbm.at[e], g_rows.at[e], g_sem.at[e])
    ga_copy = lambda e: pltpu.make_async_copy(ga_hbm.at[e], ga.at[e], ga_sem.at[e])
    gu_copy = lambda e, f: pltpu.make_async_copy(
        gu_hbm.at[e, :, :, cols(f)], gu.at[e, :, :, cols(f)], gu_sem.at[e, f]
    )
    act_copy = lambda e: pltpu.make_async_copy(act.at[e], act_hbm.at[e], act_sem.at[e])
    x_copy(0).start()
    picked = [fetch(s, d, pick_sem.at[i]) for i, (s, d) in enumerate(picked)]
    for e in range(experts):
        for f in range(tiles):
            gu_copy(e, f).start()
            if f == 0:
                ga_copy(e).start()
        if e + 1 < experts:
            x_copy(e + 1).start()
        g_copy(e).start()
    for copy in picked:
        copy.wait()

    def expert(e, carry):
        x_copy(e).wait()
        irank[...] = dot(x_rows[e], ha_ref[e], 1, 1).astype(brain)
        ga_copy(e).wait()

        def tile(f, c):
            at = cols(f)
            gu_copy(e, f).wait()
            gate = dot(x_rows[e], gu[e, 0, :, at]) + dot(irank[:, :16], hb_ref[e, 0, :, at])
            up = dot(x_rows[e], gu[e, 1, :, at]) + dot(irank[:, 16:], hb_ref[e, 1, :, at])
            back = ga[e, :, at].astype(single)
            sig = jax.nn.sigmoid(gate)
            swish = gate * sig
            act[e, :, at] = (swish * up).astype(brain)
            gg[:, at] = (back * up * sig * (1.0 + gate * (1.0 - sig))).astype(brain)
            uu[:, at] = (back * swish).astype(brain)
            return c

        lax.fori_loop(0, tiles, tile, 0)
        act_copy(e).start()
        drank_ref[e] = dot(act[e], da_ref[e], 1, 1).astype(brain)
        girank[:, :16] = dot(gg[...], hb_ref[e, 0], 1, 1).astype(brain)
        girank[:, 16:] = dot(uu[...], hb_ref[e, 1], 1, 1).astype(brain)

        def deal(ref, row, value):
            piece = value.shape[1] // replicas
            at = pl.ds(pl.multiple_of(row, 16), value.shape[0])
            for d in range(replicas):
                ref[d, at, :] = value[:, d * piece : (d + 1) * piece].astype(brain)

        deal(gdna_ref, e * 16, dot(gdr_ref[e], act[e], 0, 0))
        deal(gmidb_ref, e * 32, dot(irank[:, :16], gg[...], 0, 0))
        deal(gmidb_ref, e * 32 + 16, dot(irank[:, 16:], uu[...], 0, 0))
        deal(gina_ref, e * 32, dot(girank[...], x_rows[e], 0, 0))
        g_copy(e).wait()
        deal(gdnb_ref, e * 16, dot((drank_ref[e].astype(single) * weight[e]).astype(brain), g_rows[e], 0, 0))

        wide = min(2 * TILE, width)

        def slots(d, c):
            at = pl.ds(pl.multiple_of(d * wide, wide), wide)
            s = dot(gg[...], gu[e, 0, at, :], 1, 1) + dot(uu[...], gu[e, 1, at, :], 1, 1)
            s_rows[pl.ds(pl.multiple_of(e * rows, 16), rows), at] = (s + dot(girank[...], ha_ref[e, :, at])).astype(brain)
            return c

        lax.fori_loop(0, width // wide, slots, 0)
        return carry

    lax.fori_loop(0, experts, expert, 0)
    out_copy = lambda b: pltpu.make_async_copy(out_stage.at[b % 2], gpart_hbm.at[b], out_sem.at[b % 2])

    def combine(b, carry):
        @pl.when(b >= 2)
        def _():
            out_copy(b - 2).wait()

        out_stage[b % 2] = combined(place, s_rows, b, cap, rows)
        out_copy(b).start()
        return carry

    lax.fori_loop(0, blocks, combine, 0)
    for b in (blocks - 2, blocks - 1):
        out_copy(b).wait()
    for e in range(experts):
        act_copy(e).wait()


def moe(ids, place, weight, gdr, x, g, ga, gu, ha, hb, da, cap, replicas):
    experts, rows, width = x.shape
    blocks, toks = place.shape[0] // experts, place.shape[1]
    hidden = gu.shape[3]
    rank = da.shape[2]
    vm = pl.BlockSpec(memory_space=pltpu.VMEM)
    sm = pl.BlockSpec(memory_space=pltpu.SMEM)
    hb_ = pl.BlockSpec(memory_space=pl.ANY)
    h = lambda *s: jax.ShapeDtypeStruct(s, brain)
    bv = lambda *s: pltpu.VMEM(s, brain)
    fv = lambda *s: pltpu.VMEM(s, single)
    dma = pltpu.SemaphoreType.DMA
    return pl.pallas_call(
        functools.partial(moe_kernel, cap, replicas),
        out_shape=(
            h(experts, rows, rank),
            h(replicas, experts * 2 * rank, width // replicas), h(replicas, experts * 2 * rank, hidden // replicas),
            h(replicas, experts * rank, hidden // replicas), h(replicas, experts * rank, width // replicas),
            h(blocks, toks, width), h(experts, rows, hidden),
        ),
        in_specs=[sm, vm, vm, vm] + [hb_] * 7,
        out_specs=[vm] * 5 + [hb_] * 2,
        scratch_shapes=[
            bv(*gu.shape), bv(*x.shape), bv(*x.shape), bv(*ga.shape), bv(experts * rows, width), bv(*ga.shape),
            bv(rows, hidden), bv(rows, hidden), bv(rows, 2 * rank), bv(rows, 2 * rank), bv(experts, 2 * rank, width),
            bv(experts, 2, rank, hidden), bv(experts, rank, hidden), bv(2, toks, width),
            dma((5 * experts,)), dma((experts,)), dma((experts,)), dma((experts,)), dma((experts, hidden // TILE)),
            dma((experts,)), dma((2,)),
        ],
        compiler_params=pltpu.CompilerParams(vmem_limit_bytes=VMEM_ALL),
        name="moe",
    )(ids, place, weight, gdr, x, g, ga, gu, ha, hb, da)


ADAPTERS = 8
RANK = 16
CLIP = 256.0
beta_one = 0.9
beta_two = 0.95
learn_rate = 0.02
weight_decay = 0.1
adam_eps = 1e-08


def norm_back(values, gain, grad):
    inverse = lax.rsqrt(jnp.mean(values * values, axis=-1, keepdims=True) + norm_eps)
    scaled = grad * gain
    return inverse * scaled - values * (
        inverse * inverse * inverse * jnp.mean(scaled * values, axis=-1, keepdims=True)
    )


def back_kernel(
    cap, replicas,
    ids_ref, hid_ref, top_ref, gain_ref, gain2_ref, low_ref, lse_ref, orank_ref, place, weight, drank_ref,
    resid_hbm, seq_hbm, proj_hbm, mixed_hbm, gpart_hbm, act_hbm, dn_hbm, db_hbm,
    w_hbm, a_hbm, b_hbm, wo_hbm, pa_hbm, pb_hbm, gina_hbm, gmidb_hbm, gdna_hbm, gdnb_hbm,
    out_ref, gh_ref, norm_ref, shared_got, got_qb, got_oa, got_ina, got_midb, got_dna, got_dnb,
    resid_ref, proj_ref, mixed_ref, own_g, ypart, act, dn, db_all, part,
    w_ref, a_all, b_all, wo_ref, pa_all, pb_all, a_ref,
    bf, gres, gmix, grank, gproj, glow, gk, gv,
    gqb_ref, goa_ref, shared_ref, shared_in, shared_mid, tot_e, tot_d, mine, load_sem, own_sem,
    sh_send, sh_recv, mid_send, mid_recv, p_send, p_recv, t_send, t_recv, *sems,
):
    toks, width = hid_ref.shape
    span = w_ref.shape[2]
    heads = span // HEAD
    experts = dn.shape[0]
    n = place.shape[0] // experts
    length = toks * n
    red = Scatter(gpart_hbm, *sems[0:7], own=own_g)
    redy = Scatter(ypart, *sems[7:14])
    redn = Scatter(part, *sems[14:21])
    bf_g = Gather(bf, *sems[21:23])
    me = red.me
    rep = lax.axis_index("dp")
    slot = ids_ref[rep]
    owns = [fetch(gpart_hbm.at[red.order[i]], own_g.at[i], own_sem.at[i]) for i in range(4)]
    loads = {}
    for i, (name, src, dst) in enumerate(
        (
            ("act", act_hbm, act), ("db", db_hbm, db_all), ("dn", dn_hbm, dn), ("resid", resid_hbm, resid_ref), ("wo", wo_hbm, wo_ref), ("pb", pb_hbm, pb_all), ("pa", pa_hbm, pa_all),
            ("mixed", mixed_hbm, mixed_ref), ("proj", proj_hbm, proj_ref), ("b", b_hbm, b_all), ("a", a_hbm, a_all),
            ("w", w_hbm, w_ref), ("ina", gina_hbm.at[rep], got_ina.at[rep]),
            ("midb", gmidb_hbm.at[rep], got_midb.at[rep]), ("dna", gdna_hbm.at[rep], got_dna.at[rep]),
            ("dnb", gdnb_hbm.at[rep], got_dnb.at[rep]),
        )
    ):
        loads[name] = fetch(src, dst, load_sem.at[i])

    def need(*names):
        for name in names:
            loads.pop(name).wait()

    meet(n, replicas, True)
    for i in range(4):
        red.give(i)
    pending = []

    def go(src, dst, send_sem, recv_sem, where):
        copy = pltpu.make_async_remote_copy(
            src_ref=src, dst_ref=dst, send_sem=send_sem, recv_sem=recv_sem, device_id=where
        )
        copy.start()
        pending.append(copy)

    def wait(view, recv_sem):
        pltpu.make_async_remote_copy(
            src_ref=view, dst_ref=view, send_sem=t_send.at[0], recv_sem=recv_sem, device_id={"expert": (me + 1) % n}
        ).wait_recv()

    got = (got_qb, got_oa, got_ina, got_midb, got_dna, got_dnb)

    def swap(i, source):
        for j in range(1, replicas):
            peer = (rep + j) % replicas
            go(
                source.at[peer], got[i].at[rep], p_send.at[i * replicas + j], p_recv.at[i * replicas + rep],
                {"dp": peer},
            )

    def swapped(i):
        for j in range(1, replicas):
            src = (rep + j) % replicas
            wait(got[i].at[src], p_recv.at[i * replicas + src])

    for copy in owns:
        copy.wait()
    steps = red.steps()
    for step in steps[:4]:
        step()
    for i, source in enumerate((gina_hbm, gmidb_hbm, gdna_hbm, gdnb_hbm)):
        swap(i + 2, source)
    red.flush()
    need("act", "db", "dn")
    tiles = width // TILE

    def y_tile(t):
        e = t // tiles
        s = pl.ds(pl.multiple_of(t % tiles * TILE, TILE), TILE)
        y = dot(act[e], dn[e, :, s]) + dot(drank_ref[e], db_all[e, slot, :, s])
        part[pl.ds(pl.multiple_of(e * n * cap, 16), n * cap), s] = (y * weight[e]).astype(brain)

    drive(experts * tiles, y_tile, {2: steps[4:5], 4: steps[5:6], 5: steps[6:7]})
    seq_ref = dn.at[0]
    loads["seq"] = fetch(seq_hbm, seq_ref, load_sem.at[len(loads) + 4])
    need("resid")
    for k in ORDER:
        r = red.rows(k)
        grad = top_ref[r].astype(single) + norm_back(resid_ref[r], gain2_ref[...], red.final(k))
        gres[r] = grad
        bf[me, r] = grad.astype(brain)
        if k != ORDER[0]:
            bf_g.start_own(ORDER[ORDER.index(k) - 1])
    bf_g.start_own(ORDER[-1])
    need("wo", "pb", "pa", "mixed")

    def mixed_grad(block):
        p = block // 2
        both = bf[pl.ds(2 * p, 2)].reshape(2 * toks, width)
        at = two(p, toks)
        rank = dot(both, pb_all[slot], 1, 1).astype(brain)
        grank[at, :] = rank
        gmix[at, :] = (dot(both, wo_ref[...], 1, 1) + dot(rank, pa_all[slot])).astype(brain)

    def y_block(block_at):
        ypart[block_at] = combined(place, part, block_at, cap, n * cap)

    bf_g.pair(me)
    mixed_grad(me)
    drive(
        n, y_block, {2: [functools.partial(bf_g.relay, 0)], 6: [functools.partial(bf_g.relay, 1)]},
    )
    for i in range(4):
        redy.give(i)
    for i in range(2, CHUNKS):
        bf_g.relay(i)
    ysteps = redy.steps()
    for step in ysteps[:4]:
        step()
    bf_g.pair(bf_g.across)
    mixed_grad(bf_g.across)
    redy.flush()
    bf_g.relay_far(0)
    bf_g.pair(bf_g.along)
    mixed_grad(bf_g.along)
    for i in range(1, CHUNKS // 2):
        bf_g.relay_far(i)
    bf_g.pair(bf_g.far)
    mixed_grad(bf_g.far)

    piece = span // replicas
    goa = dot(grank[...], mixed_ref[...], 0, 0)
    for d in range(replicas):
        goa_ref[d] = goa[:, d * piece : (d + 1) * piece].astype(brain)
    got_oa[rep] = goa_ref[rep]
    swap(1, goa_ref)

    need("proj")
    scale = HEAD ** (-0.5)
    block = 256
    for h in range(heads):
        at = slice(h * HEAD, (h + 1) * HEAD)
        gk[...] = jnp.zeros_like(gk)
        gv[...] = jnp.zeros_like(gv)

        def attend(i, h=h, at=at):
            r = pl.ds(pl.multiple_of(i * block, block), block)
            q, do = proj_ref[0, r, at], gmix[r, at]
            delta = jnp.sum(do.astype(single) * mixed_ref[r, at].astype(single), axis=-1, keepdims=True)
            probs = jnp.exp(dot(q, proj_ref[1, :, at], 1, 1) * scale - lse_ref[r, h : h + 1])
            gp = dot(do, proj_ref[2, :, at], 1, 1)
            gs = (probs * (gp - delta)).astype(brain)
            gproj[0, r, at] = (dot(gs, proj_ref[1, :, at]) * scale).astype(brain)
            gk[...] += dot(gs, q, 0, 0)
            gv[...] += dot(probs.astype(brain), do, 0, 0)

        drive(length // block, attend, {0: ysteps[4:5], 1: ysteps[5:6], 2: ysteps[6:]} if h == 0 else {})
        gproj[1, :, at] = (gk[...] * scale).astype(brain)
        gproj[2, :, at] = gv[...].astype(brain)

    need("a", "b", "w")
    for j in range(3):
        a_ref[16 * j : 16 * j + 16, :] = a_all[j, slot]
    nsteps = redn.steps()
    for i in range(4):
        p = redn.order[i] // 2
        at = two(p, toks)
        for j in range(3):
            glow[at, 16 * j : 16 * j + 16] = dot(gproj[j, at, :], b_all[j, slot], 1, 1).astype(brain)
        wide = min(1024, width)

        def normed_grad(c, carry, p=p, at=at):
            s = pl.ds(pl.multiple_of(c * wide, wide), wide)
            out = dot(glow[at, :], a_ref[:, s])
            for j in range(3):
                out = out + dot(gproj[j, at, :], w_ref[j, s, :], 1, 1)
            part[at, s] = out.astype(brain)
            return carry

        lax.fori_loop(0, width // wide, normed_grad, 0)
        if i:
            redn.give(i - 1)
        if i == 2:
            for step in nsteps[:2]:
                step()
    redn.give(3)
    for step in nsteps[2:4]:
        step()
    del nsteps[:4]

    thin = width // (n * replicas)

    def share(row, value, base):
        for c in range(value.shape[1] // thin):
            d, e = (base + c) // n, (base + c) % n
            shared_ref[e, row : row + value.shape[0], d * thin : (d + 1) * thin] = value[
                :, c * thin : (c + 1) * thin
            ].astype(brain)

    def advance():
        if nsteps:
            nsteps.pop(0)()

    for j in range(3):
        gqb = dot(low_ref[:, 16 * j : 16 * j + 16], gproj[j], 0, 0)
        for d in range(replicas):
            gqb_ref[d, 16 * j : 16 * j + 16, :] = gqb[:, d * piece : (d + 1) * piece].astype(brain)
    redn.flush()
    got_qb[rep] = gqb_ref[rep]
    swap(0, gqb_ref)
    need("seq")
    cols = 512
    for c in range(width // cols):
        s = slice(c * cols, (c + 1) * cols)
        share(0, dot(glow[...], seq_ref[:, s], 0, 0), c * cols // thin)
        share(48, dot(orank_ref[...], bf[:, :, s].reshape(length, cols), 0, 0), c * cols // thin)
        advance()
    shared_in[me] = shared_ref[me]
    for j in range(1, n):
        peer = (me + j) % n
        go(shared_ref.at[peer], shared_in.at[me], sh_send.at[j - 1], sh_recv.at[me], {"expert": peer})
    while nsteps:
        advance()

    def squares(i, source):
        rows = source.shape[1] // RANK

        def body(t, acc):
            at = pl.ds(pl.multiple_of(t // ADAPTERS * RANK, RANK), RANK)
            value = jnp.zeros((RANK, source.shape[2]), single)
            for s in range(replicas):
                value = value + source[s, at, :].astype(single) * jnp.where(ids_ref[s] == t % ADAPTERS, 1.0, 0.0)
            return acc + value * value

        return jnp.sum(
            lax.fori_loop(0, rows * ADAPTERS, body, jnp.zeros((RANK, source.shape[2]), single))
        )

    need("ina", "midb", "dna", "dnb")
    total = jnp.zeros((), single)
    for i in range(2, 6):
        swapped(i)
        total = total + squares(i, got[i])
    for j in range(1, n):
        src = (me + j) % n
        wait(shared_in.at[src], sh_recv.at[src])
    summed = shared_in[0].astype(single)
    for e in range(1, n):
        summed = summed + shared_in[e].astype(single)
    for d in range(replicas):
        shared_mid[d] = summed[:, d * thin : (d + 1) * thin].astype(brain)
    shared_got[rep] = shared_mid[rep]
    for j in range(1, replicas):
        peer = (rep + j) % replicas
        go(shared_mid.at[peer], shared_got.at[rep], mid_send.at[j], mid_recv.at[rep], {"dp": peer})
    for k in ORDER:
        r = redy.rows(k)
        out_ref[r] = (resid_ref[r] + redy.final(k)).astype(brain)
    for i in range(2):
        swapped(i)
        total = total + squares(i, got[i])
    for j in range(1, replicas):
        src = (rep + j) % replicas
        wait(shared_got.at[src], mid_recv.at[src])
    total = total + squares(0, shared_got)

    mine[0] = jnp.full(mine.shape[1:], total, single)
    tot_e[me] = mine[0]
    for j in range(1, n):
        go(mine.at[0], tot_e.at[me], t_send.at[j], t_recv.at[me], {"expert": (me + j) % n})
    for j in range(1, n):
        src = (me + j) % n
        wait(tot_e.at[src], t_recv.at[src])
    total = tot_e[0]
    for e in range(1, n):
        total = total + tot_e[e]
    mine[1] = total
    tot_d[rep] = mine[1]
    for j in range(1, replicas):
        go(mine.at[1], tot_d.at[rep], t_send.at[n + j], t_recv.at[n + rep], {"dp": (rep + j) % replicas})
    for k in ORDER:
        r = redn.rows(k)
        gh_ref[r] = gres[r] + norm_back(hid_ref[r].astype(single), gain_ref[...], redn.final(k))
    for j in range(1, replicas):
        src = (rep + j) % replicas
        wait(tot_d.at[src], t_recv.at[n + src])
    total = tot_d[0]
    for d in range(1, replicas):
        total = total + tot_d[d]
    norm_ref[...] = jnp.sqrt(total)
    for mover in (red, redy, redn, bf_g):
        mover.drain()
    for copy in pending:
        copy.wait_send()


def back(
    ids, hid, top, gain, gain2, low, lse, orank, place, weight, drank, resid, seq, proj, mixed, gpart, act, dn, db,
    w, a, b, wo, pa, pb, pieces, cap, replicas, cid=1,
):
    n, toks, width = seq.shape
    seq = seq.reshape(n * toks, width)
    experts, rows = act.shape[:2]
    span = w.shape[2]
    length = toks * n
    vm = pl.BlockSpec(memory_space=pltpu.VMEM)
    sm = pl.BlockSpec(memory_space=pltpu.SMEM)
    hb = pl.BlockSpec(memory_space=pl.ANY)
    f = lambda *s: jax.ShapeDtypeStruct(s, single)
    h = lambda *s: jax.ShapeDtypeStruct(s, brain)
    bv = lambda *s: pltpu.VMEM(s, brain)
    fv = lambda *s: pltpu.VMEM(s, single)
    dma = pltpu.SemaphoreType.DMA
    thin = width // (n * replicas)
    piece = span // replicas
    return pl.pallas_call(
        functools.partial(back_kernel, cap, replicas),
        out_shape=(
            h(toks, width), f(toks, width), f(8, 128), h(replicas, 64, thin), h(replicas, 48, piece),
            h(replicas, 16, piece),
        ) + tuple(h(*p.shape) for p in pieces),
        in_specs=[sm] + [vm] * 10 + [hb] * 18,
        out_specs=[vm] * 10,
        scratch_shapes=[
            fv(toks, width), bv(3, length, span), bv(length, span), bv(4, toks, width), bv(n, toks, width),
            bv(*act.shape), bv(*dn.shape), bv(*db.shape), bv(experts * rows, width),
        ]
        + [pltpu.VMEM(v.shape, brain) for v in (w, a, b, wo, pa, pb)]
        + [
            bv(48, width), bv(n, toks, width), fv(toks, width), bv(length, span), bv(length, 16),
            bv(3, length, span), bv(length, 48), fv(length, HEAD), fv(length, HEAD),
            bv(replicas, 48, piece), bv(replicas, 16, piece), bv(n, 64, replicas * thin), bv(n, 64, replicas * thin),
            bv(replicas, 64, thin), fv(n, 8, 128), fv(replicas, 8, 128), fv(2, 8, 128), dma((20,)), dma((4,)),
            dma((n,)), dma((n,)), dma((replicas,)), dma((replicas,)), dma((6 * replicas,)), dma((6 * replicas,)),
            dma((n + replicas,)), dma((n + replicas,)),
        ]
        + scatter_scratch(toks, width) * 3 + gather_scratch(n),
        compiler_params=pltpu.CompilerParams(collective_id=cid, has_side_effects=True, vmem_limit_bytes=VMEM_ALL),
        name="back",
    )(
        ids, hid, top, gain, gain2, low, lse, orank, place, weight, drank, resid, seq, proj, mixed, gpart, act, dn, db,
        w, a, b, wo, pa, pb, *pieces,
    )


def adam_kernel(n, replicas, groups, spans, adapter_ref, step_ref, norm_in, out_in, gh_in, *refs):
    got, refs = refs[:7], refs[7:]
    weight_hbm, first_hbm, second_hbm, refs = refs[:8], refs[8:16], refs[16:24], refs[24:]
    out_hbm, gh_hbm, norm_ref, result, refs = refs[0], refs[1], refs[2], refs[3:35], refs[35:]
    weight, first, second, kept, refs = refs[:8], refs[8:16], refs[16:24], refs[24:56], refs[56:]
    load_sem, save_sem = refs
    me, rep = lax.axis_index("expert"), lax.axis_index("dp")
    common = rep * n + me
    loads, saves = {}, []
    turns = (6, 5, 4, 7, 0, 2, 1, 3)
    for a in turns:
        size, pieces = spans[a]
        index = common if pieces == n * replicas else rep
        start = index * size // weight[a].shape[1] * weight[a].shape[1]
        view = weight_hbm[a].at[:, pl.ds(pl.multiple_of(start, 128), weight[a].shape[1])]
        loads[a] = [
            fetch(src, dst, load_sem.at[3 * a + k])
            for k, (src, dst) in enumerate(((view, weight[a]), (first_hbm[a], first[a]), (second_hbm[a], second[a])))
        ]
    saves.append(fetch(out_in, out_hbm, save_sem.at[32]))
    saves.append(fetch(gh_in, gh_hbm, save_sem.at[33]))
    norm_ref[0] = norm_in[0, 0]
    factor = jnp.minimum(1.0, CLIP / norm_in[...])[0:1, 0:1]
    steps = jnp.full((8, 128), step_ref[0].astype(single), single)
    fix_first = (1.0 / (1.0 - jnp.exp(steps * jnp.log(jnp.full((8, 128), beta_one, single)))))[0:1, 0:1]
    fix_second = (1.0 / (1.0 - jnp.exp(steps * jnp.log(jnp.full((8, 128), beta_two, single)))))[0:1, 0:1]
    for a in turns:
        for copy in loads[a]:
            copy.wait()
        source = got[max(a - 1, 0)]
        base = groups[0] if a == 1 else 0
        size, pieces = spans[a]
        window = weight[a].shape[1]
        index = common if pieces == n * replicas else rep

        def body(t, carry, a=a, source=source, base=base, size=size, window=window, index=index):
            rows = pl.ds(pl.multiple_of((base + t) * RANK, RANK), RANK)
            parts = [source[s, rows, :].astype(single) for s in range(replicas)]
            for adapter in range(ADAPTERS):
                at = pl.ds(pl.multiple_of((t * ADAPTERS + adapter) * RANK, RANK), RANK)
                grad = jnp.zeros((RANK, size), single)
                for s in range(replicas):
                    grad = grad + parts[s] * jnp.where(adapter_ref[s] == adapter, 1.0, 0.0)
                held = weight[a][at, :].astype(single)
                w = held[:, :size]
                for c in range(1, window // size):
                    w = jnp.where(index % (window // size) == c, held[:, c * size : (c + 1) * size], w)
                clipped = grad * factor
                f = beta_one * first[a][at, :] + (1.0 - beta_one) * clipped
                s = beta_two * second[a][at, :] + (1.0 - beta_two) * clipped * clipped
                kept[4 * a][at, :] = grad
                kept[4 * a + 1][at, :] = f
                kept[4 * a + 2][at, :] = s
                kept[4 * a + 3][at, :] = -learn_rate * (
                    f * fix_first / (jnp.sqrt(s * fix_second) + adam_eps) + weight_decay * w
                )
            done = pl.ds(pl.multiple_of(t * ADAPTERS * RANK, ADAPTERS * RANK), ADAPTERS * RANK)
            for k in range(4 * a, 4 * a + 4):
                fetch(kept[k].at[done], result[k].at[done], save_sem.at[k])
            return carry

        lax.fori_loop(0, groups[a], body, 0)
        for k in range(4 * a, 4 * a + 4):
            saves.append(pltpu.make_async_copy(kept[k], result[k], save_sem.at[k]))
    for copy in saves:
        copy.wait()


def adam(adapters, steps, norm, block_out, gh, got, weight, pieces, first, second, n, replicas):
    spans = tuple((f.shape[1], p) for f, p in zip(first, pieces))
    groups = tuple(f.shape[0] // (ADAPTERS * RANK) for f in first)
    vm = pl.BlockSpec(memory_space=pltpu.VMEM)
    sm = pl.BlockSpec(memory_space=pltpu.SMEM)
    hb = pl.BlockSpec(memory_space=pl.ANY)
    f = lambda s: jax.ShapeDtypeStruct(s, single)
    dma = pltpu.SemaphoreType.DMA
    shapes = [t.shape for t in first]
    return pl.pallas_call(
        functools.partial(adam_kernel, n, replicas, groups, spans),
        out_shape=(jax.ShapeDtypeStruct(block_out.shape, brain), f(gh.shape), f((1,)))
        + tuple(f(s) for s in shapes for _ in range(4)),
        in_specs=[sm, sm, vm, vm, vm] + [vm] * 7 + [hb] * 24,
        out_specs=[hb, hb, sm] + [hb] * 32,
        scratch_shapes=[pltpu.VMEM((s[0], max(s[1], 128)), brain) for s in shapes]
        + [pltpu.VMEM(s, single) for s in shapes] * 2
        + [pltpu.VMEM(s, single) for s in shapes for _ in range(4)]
        + [dma((24,)), dma((34,))],
        compiler_params=pltpu.CompilerParams(vmem_limit_bytes=VMEM_ALL),
        name="adam",
    )(adapters, steps, norm, block_out, gh, *got, *weight, *first, *second)


def per_device(
    hidden,
    output_cotangent,
    attention_gain,
    expert_norm_gain,
    query_key_value_weight,
    output_weight,
    gate_up_weight,
    down_weight,
    token_experts,
    expert_gate_weight,
    sequence_adapter,
    optimizer_steps,
    adapter_attention_input,
    adapter_attention_output,
    adapter_projection_input,
    adapter_projection_output,
    adapter_hidden_input,
    adapter_hidden_output,
    adapter_down_input,
    adapter_down_output,
    moment_attention_input,
    moment_attention_output,
    moment_projection_input,
    moment_projection_output,
    moment_hidden_input,
    moment_hidden_output,
    moment_down_input,
    moment_down_output,
    squared_attention_input,
    squared_attention_output,
    squared_projection_input,
    squared_projection_output,
    squared_hidden_input,
    squared_hidden_output,
    squared_down_input,
    squared_down_output,
):
    n = lax.axis_size("expert")
    replicas = lax.axis_size("dp")
    toks, width = hidden.shape[1:]
    here = down_weight.shape[0]
    cap = min(toks, toks * token_experts.shape[2] * 5 // (4 * here * n))
    gain = attention_gain[None]
    gain2 = expert_norm_gain[None]
    hid, cot = hidden[0], output_cotangent[0]
    low, lse, orank, gdr, place, weight, seq, proj, mixed, resid, x_rows, g_rows, ga = front(
        sequence_adapter, hid, cot, token_experts[0].T, expert_gate_weight[0].T, gain, gain2, query_key_value_weight,
        adapter_attention_input, adapter_attention_output, output_weight, adapter_projection_input,
        adapter_projection_output, down_weight, adapter_down_input, adapter_down_output, n, cap,
    )
    drank, *pieces, gpart, act = moe(
        sequence_adapter, place, weight, gdr, x_rows, g_rows, ga, gate_up_weight, adapter_hidden_input,
        adapter_hidden_output, adapter_down_input, cap, replicas,
    )
    block_out, grad_hidden, norm, *got = back(
        sequence_adapter, hid, cot, gain, gain2, low, lse, orank, place, weight, drank, resid, seq, proj, mixed, gpart,
        act, down_weight, adapter_down_output,
        query_key_value_weight, adapter_attention_input, adapter_attention_output, output_weight,
        adapter_projection_input, adapter_projection_output, tuple(pieces), cap, replicas,
    )

    def flat(array):
        return array.reshape(-1, array.shape[-1])

    weights = (
        adapter_attention_input, adapter_projection_output, adapter_attention_output, adapter_projection_input,
        adapter_hidden_input, adapter_hidden_output, adapter_down_input, adapter_down_output,
    )
    first = (
        moment_attention_input, moment_projection_output, moment_attention_output, moment_projection_input,
        moment_hidden_input, moment_hidden_output, moment_down_input, moment_down_output,
    )
    second = (
        squared_attention_input, squared_projection_output, squared_attention_output, squared_projection_input,
        squared_hidden_input, squared_hidden_output, squared_down_input, squared_down_output,
    )
    outs = adam(
        sequence_adapter, optimizer_steps, norm, block_out, grad_hidden, got, tuple(flat(w) for w in weights),
        (n * replicas,) * 2 + (replicas,) * 6, tuple(flat(m) for m in first), tuple(flat(s) for s in second),
        n, replicas,
    )
    results = [outs[0][None], outs[1][None], outs[2]]
    for a in (0, 2, 3, 1, 4, 5, 6, 7):
        for kind in range(4):
            results.append(outs[3 + 4 * a + kind].reshape(first[a].shape))
    return tuple(results)


def solution(mesh):
    return jax.shard_map(
        per_device,
        mesh=mesh,
        in_specs=(
            P("dp", "expert", None),
            P("dp", "expert", None),
            P(),
            P(),
            P(None, None, "expert"),
            P("expert", None),
            P("expert", None, None, None),
            P("expert", None, None),
            P("dp", "expert", None),
            P("dp", "expert", None),
            P(),
            P(),
            P(),
            P(None, None, None, "expert"),
            P(None, None, "expert"),
            P(),
            P("expert", None, None, None, None),
            P("expert", None, None, None, None),
            P("expert", None, None, None),
            P("expert", None, None, None),
            P(None, None, None, ("dp", "expert")),
            P(None, None, None, ("expert", "dp")),
            P(None, None, ("expert", "dp")),
            P(None, None, ("dp", "expert")),
            P("expert", None, None, None, "dp"),
            P("expert", None, None, None, "dp"),
            P("expert", None, None, "dp"),
            P("expert", None, None, "dp"),
            P(None, None, None, ("dp", "expert")),
            P(None, None, None, ("expert", "dp")),
            P(None, None, ("expert", "dp")),
            P(None, None, ("dp", "expert")),
            P("expert", None, None, None, "dp"),
            P("expert", None, None, None, "dp"),
            P("expert", None, None, "dp"),
            P("expert", None, None, "dp"),
        ),
        out_specs=(
            P("dp", "expert", None),
            P("dp", "expert", None),
            P(),
            P(None, None, None, ("dp", "expert")),
            P(None, None, None, ("dp", "expert")),
            P(None, None, None, ("dp", "expert")),
            P(None, None, None, ("dp", "expert")),
            P(None, None, None, ("expert", "dp")),
            P(None, None, None, ("expert", "dp")),
            P(None, None, None, ("expert", "dp")),
            P(None, None, None, ("expert", "dp")),
            P(None, None, ("expert", "dp")),
            P(None, None, ("expert", "dp")),
            P(None, None, ("expert", "dp")),
            P(None, None, ("expert", "dp")),
            P(None, None, ("dp", "expert")),
            P(None, None, ("dp", "expert")),
            P(None, None, ("dp", "expert")),
            P(None, None, ("dp", "expert")),
            P("expert", None, None, None, "dp"),
            P("expert", None, None, None, "dp"),
            P("expert", None, None, None, "dp"),
            P("expert", None, None, None, "dp"),
            P("expert", None, None, None, "dp"),
            P("expert", None, None, None, "dp"),
            P("expert", None, None, None, "dp"),
            P("expert", None, None, None, "dp"),
            P("expert", None, None, "dp"),
            P("expert", None, None, "dp"),
            P("expert", None, None, "dp"),
            P("expert", None, None, "dp"),
            P("expert", None, None, "dp"),
            P("expert", None, None, "dp"),
            P("expert", None, None, "dp"),
            P("expert", None, None, "dp"),
        ),
        check_vma=False,
    )
```
